32 devices in a mesh: groups: 2 (over x), cols: 4 (over y, core), rows: 4 (over z).
Axes of the slice: x: 2, y: 2, z: 4, core: 2. Of those that a mesh axis runs over, the one named last changes fastest.
Arguments:
- camera_tokens: bfloat16 [1024, 6144], P(('groups', 'rows'), 'cols'), parts along dimension 0, may hold values from -150 to 150, as said below
- norm_gain: float32 [6144], P('cols'), may hold values from 0.25 to 1.75
- query_weight: bfloat16 [6144, 6144], P('cols', 'rows'), may hold values from -0.078125 to 0.078125
- key_weight: bfloat16 [6144, 6144], P('cols', 'rows'), may hold values from -0.078125 to 0.078125
- value_weight: bfloat16 [6144, 6144], P('cols', 'rows'), may hold values from -0.078125 to 0.078125
- query_gain: float32 [6144], P('rows'), may hold values from 0.5 to 14, as said below
- key_gain: float32 [6144], P('rows'), may hold values from 0.5 to 14, as said below
- out_weight: bfloat16 [6144, 6144], P('rows', 'cols'), may hold values from -0.078125 to 0.078125
- up_weight: bfloat16 [6144, 24576], P('cols', 'rows'), may hold values from -0.078125 to 0.078125
- up_bias: float32 [24576], P('rows'), may hold values from -3 to 3
- down_weight: bfloat16 [24576, 6144], P('rows', 'cols'), may hold values from -0.0390625 to 0.0390625
- down_bias: float32 [6144], P('cols'), may hold values from -3 to 3
- join_gain: float32 [6144], P('cols'), may hold values from 0.25 to 1.75
- join_query: bfloat16 [6144, 6144], P('cols', 'rows'), may hold values from -0.078125 to 0.078125
- join_key: bfloat16 [6144, 6144], P('cols', 'rows'), may hold values from -0.078125 to 0.078125
- join_value: bfloat16 [6144, 6144], P('cols', 'rows'), may hold values from -0.078125 to 0.078125
- join_query_gain: float32 [6144], P('rows'), may hold values from 0.5 to 14, as said below
- join_key_gain: float32 [6144], P('rows'), may hold values from 0.5 to 14, as said below
- join_out: bfloat16 [6144, 6144], P('rows', 'cols'), may hold values from -0.078125 to 0.078125
Outputs:
- joined_tokens: bfloat16 [1024, 6144], P(('groups', 'rows'), 'cols'), parts along dimension 0
The draws below stay inside these ranges and needn't reach their ends.
There are 2 independent parts, one for each index of `groups`. The reference program is written for one: setup_inputs(seed, part) draws one part's arguments, and reference() takes and returns one part's arrays. A program takes and returns all parts, laid end to end along the dimension named above; an argument that names none is the same for every part. Nothing has to cross between parts.
Inputs may be any that keep to these rules, and one draw needn't show every extreme that they name: `camera_tokens`: real valued tokens. `query_gain`: Positive. `key_gain`: Positive. `join_query_gain`: Positive. `join_key_gain`: Positive.
All inputs are finite; a program needn't handle non-finite values.
Results may differ from the reference program's by a relative error of at most 0.012.
Values may be sent and summed in bfloat16 or wider, within the bound.
A program may use at most 192 MiB of HBM per device.

```python
import math
import jax
import jax.numpy as jnp
from jax import lax

HEADS = 48
HEAD_DIM = 128
FF = 24576
CAMERAS = 8
TOK_CAM = 64
D = 6144
TOKENS = 512


def head_scales(key):
    subkeys = jax.random.split(key, 2)
    per_head = jnp.exp(jax.random.uniform(subkeys[0], (HEADS, 1), jnp.float32, math.log(1.2), math.log(3.5)))
    jitter = jax.random.uniform(subkeys[1], (HEADS, HEAD_DIM), jnp.float32, 0.8, 1.25)
    return (per_head * jitter).reshape(HEADS * HEAD_DIM)


def draw_query_gain(key, part):
    return head_scales(jax.random.fold_in(key, 11))


def draw_key_gain(key, part):
    return head_scales(jax.random.fold_in(key, 23))


def draw_join_query_gain(key, part):
    return head_scales(jax.random.fold_in(key, 37))


def draw_join_key_gain(key, part):
    return head_scales(jax.random.fold_in(key, 41))


def draw_camera_tokens(key, part):
    subkeys = jax.random.split(jax.random.fold_in(key, 5), 3)
    width = HEADS * HEAD_DIM
    gaussian = jax.random.truncated_normal(subkeys[0], -4.0, 4.0, (TOKENS, width), jnp.float32)
    rising = 3.0 ** (jnp.arange(width, dtype=jnp.float32) / width)
    row_scale = jnp.exp(jax.random.uniform(subkeys[1], (TOKENS, 1), jnp.float32, math.log(0.5), math.log(2.0)))
    col_scale = jnp.exp(jax.random.uniform(subkeys[2], (1, width), jnp.float32, math.log(0.6), math.log(1.6))) * rising
    return (gaussian * row_scale * col_scale).astype(jnp.bfloat16)


def levels(own_key, shape, shards, low, top_value):
    loudness = 1.0
    for dim, shards_of in shards:
        steps = jax.random.uniform(jax.random.fold_in(jax.random.fold_in(own_key, 6), dim), (shards_of,), jnp.float32, low / len(shards), top_value / len(shards))
        loudness = loudness * jnp.repeat(jnp.exp(steps), shape[dim] // shards_of).reshape((-1,) + (1,) * (len(shape) - 1 - dim))
    return loudness


def noise(own_key, extent, scale, most, cuts=(), kind=jnp.bfloat16):
    drawn = scale * jax.random.normal(own_key, extent, jnp.float32)
    if cuts:
        drawn = drawn * levels(own_key, extent, cuts, -0.22, 0.18)
    return jnp.clip(drawn, -most, most).astype(kind)


def setup_inputs(seed: int = 0, part: int = 0) -> dict:
    arg_keys = jax.random.split(jax.random.key(seed), 20)
    part_keys = jax.random.split(jax.random.fold_in(arg_keys[19], part), 20)
    return {
        "camera_tokens": draw_camera_tokens(jax.random.fold_in(jax.random.fold_in(arg_keys[19], part), 71), part),
        "norm_gain": jnp.clip(1.0 + 0.15 * jax.random.normal(arg_keys[1], (D,), jnp.float32), 0.25, 1.75),
        "query_weight": noise(arg_keys[2], (D, D), D ** -0.5, 0.078125, ((0, 4), (1, 4))),
        "key_weight": noise(arg_keys[3], (D, D), D ** -0.5, 0.078125, ((0, 4), (1, 4))),
        "value_weight": noise(arg_keys[4], (D, D), D ** -0.5, 0.078125, ((0, 4), (1, 4))),
        "query_gain": draw_query_gain(jax.random.fold_in(arg_keys[19], 71), part),
        "key_gain": draw_key_gain(jax.random.fold_in(arg_keys[19], 71), part),
        "out_weight": noise(arg_keys[7], (D, D), D ** -0.5, 0.078125, ((0, 4), (1, 4))),
        "up_weight": noise(arg_keys[8], (D, FF), D ** -0.5, 0.078125, ((0, 4), (1, 4))),
        "up_bias": noise(arg_keys[9], (FF,), 0.5, 3.0, ((0, 4),), jnp.float32),
        "down_weight": noise(arg_keys[10], (FF, D), FF ** -0.5, 0.0390625, ((0, 4), (1, 4))),
        "down_bias": noise(arg_keys[11], (D,), 0.5, 3.0, ((0, 4),), jnp.float32),
        "join_gain": jnp.clip(1.0 + 0.15 * jax.random.normal(arg_keys[12], (D,), jnp.float32), 0.25, 1.75),
        "join_query": noise(arg_keys[13], (D, D), D ** -0.5, 0.078125, ((0, 4), (1, 4))),
        "join_key": noise(arg_keys[14], (D, D), D ** -0.5, 0.078125, ((0, 4), (1, 4))),
        "join_value": noise(arg_keys[15], (D, D), D ** -0.5, 0.078125, ((0, 4), (1, 4))),
        "join_query_gain": draw_join_query_gain(jax.random.fold_in(arg_keys[19], 71), part),
        "join_key_gain": draw_join_key_gain(jax.random.fold_in(arg_keys[19], 71), part),
        "join_out": noise(arg_keys[18], (D, D), D ** -0.5, 0.078125, ((0, 4), (1, 4))),
    }


EPS = 1e-06

def layer_norm(values, scales):
    row_mean = lax.optimization_barrier(jnp.mean(values, -1, keepdims=True))
    row_var = lax.optimization_barrier(jnp.mean(values * values, -1, keepdims=True)) - row_mean * row_mean
    return ((values - row_mean) * lax.rsqrt(row_var + EPS) * scales).astype(jnp.bfloat16)

def head_norm(values, scales):
    row_count = values.shape[0]
    grouped = values.reshape(row_count, -1, HEAD_DIM)
    row_mean = lax.optimization_barrier(jnp.mean(grouped, -1, keepdims=True))
    row_var = lax.optimization_barrier(jnp.mean(grouped * grouped, -1, keepdims=True)) - row_mean * row_mean
    normed = (grouped - row_mean) * lax.rsqrt(row_var + EPS)
    return (normed.reshape(row_count, -1) * scales).astype(jnp.bfloat16)

def attend(queries, key_rows, val_rows):
    inv_root = 1.0 / math.sqrt(HEAD_DIM)
    scores = jnp.einsum('bqhd,bkhd->bhqk', queries.astype(jnp.float32), key_rows.astype(jnp.float32)) * inv_root
    row_max = lax.optimization_barrier(jnp.max(scores, -1, keepdims=True))
    weights = jnp.exp(scores - row_max)
    row_sum = lax.optimization_barrier(jnp.sum(weights, -1))
    rounded = lax.optimization_barrier(weights.astype(jnp.bfloat16)).astype(jnp.float32)
    blended = jnp.einsum('bhqk,bkhd->bqhd', rounded, val_rows.astype(jnp.float32))
    return blended / jnp.transpose(row_sum, (0, 2, 1))[..., None]

def reference(camera_tokens, norm_gain, query_weight, key_weight, value_weight, query_gain, key_gain, out_weight, up_weight, up_bias, down_weight, down_bias, join_gain, join_query, join_key, join_value, join_query_gain, join_key_gain, join_out):
    start_f32 = camera_tokens.astype(jnp.float32)
    normed = layer_norm(start_f32, norm_gain)
    query_raw = jnp.dot(normed, query_weight, preferred_element_type=jnp.float32)
    key_raw = jnp.dot(normed, key_weight, preferred_element_type=jnp.float32)
    value_raw = jnp.dot(normed, value_weight, preferred_element_type=jnp.float32)
    up_raw = jnp.dot(normed, up_weight, preferred_element_type=jnp.float32)
    query_normed = head_norm(query_raw, query_gain)
    key_normed = head_norm(key_raw, key_gain)
    value_rounded = value_raw.astype(jnp.bfloat16)
    cam_shape = (CAMERAS, TOK_CAM, HEADS, HEAD_DIM)
    attended = attend(query_normed.reshape(cam_shape), key_normed.reshape(cam_shape), value_rounded.reshape(cam_shape))
    attended = attended.reshape(TOKENS, D).astype(jnp.bfloat16)
    hidden = jax.nn.gelu(up_raw + up_bias, approximate=False).astype(jnp.bfloat16)
    mixed = jnp.dot(attended, out_weight, preferred_element_type=jnp.float32) + jnp.dot(hidden, down_weight, preferred_element_type=jnp.float32)
    camera_out = (start_f32 + mixed + down_bias).astype(jnp.bfloat16)
    layer_f32 = camera_out.astype(jnp.float32)
    join_normed = layer_norm(layer_f32, join_gain)
    join_q = head_norm(jnp.dot(join_normed, join_query, preferred_element_type=jnp.float32), join_query_gain)
    join_k = head_norm(jnp.dot(join_normed, join_key, preferred_element_type=jnp.float32), join_key_gain)
    join_v = jnp.dot(join_normed, join_value, preferred_element_type=jnp.float32).astype(jnp.bfloat16)
    all_shape = (1, TOKENS, HEADS, HEAD_DIM)
    join_attended = attend(join_q.reshape(all_shape), join_k.reshape(all_shape), join_v.reshape(all_shape))
    join_attended = join_attended.reshape(TOKENS, D).astype(jnp.bfloat16)
    return (layer_f32 + jnp.dot(join_attended, join_out, preferred_element_type=jnp.float32)).astype(jnp.bfloat16)
```

```python
import functools
import math
import types

import jax
import jax.numpy as jnp
from jax import lax
from jax.experimental import pallas as pl
from jax.experimental.pallas import tpu as pltpu
from jax.sharding import PartitionSpec as P

HEAD_DIM = 128
TOK_CAM = 64
D = 6144


EPS = 1e-06


def partner_2(array, axis, bit):
    return lax.ppermute(array, axis, [(i, i ^ 1 << bit) for i in range(lax.axis_size(axis))])


def normalize(values, scales, moments):
    row_mean = moments[0] / D
    row_var = moments[1] / D - row_mean * row_mean
    return ((values - row_mean[:, None]) * lax.rsqrt(row_var[:, None] + EPS) * scales).astype(
        jnp.bfloat16
    )


def shard_moments(values):
    return lax.psum((jnp.sum(values, 1), jnp.sum(values * values, 1)), "cols")


def head_norm(values, scales):
    row_count = values.shape[0]
    grouped = values.reshape(row_count, -1, HEAD_DIM)
    row_mean = jnp.mean(grouped, -1, keepdims=True)
    row_var = jnp.mean(grouped * grouped, -1, keepdims=True) - row_mean * row_mean
    normed = (grouped - row_mean) * lax.rsqrt(row_var + EPS)
    return (normed.reshape(row_count, -1) * scales).astype(jnp.bfloat16)


def attend(queries, key_rows, val_rows):
    inv_root = 1.0 / math.sqrt(HEAD_DIM)
    scores = (
        jnp.einsum("bqhd,bkhd->bhqk", queries, key_rows, preferred_element_type=jnp.float32)
        * inv_root
    )
    row_max = jnp.max(scores, -1, keepdims=True)
    weights = jnp.exp(scores - row_max)
    row_sum = jnp.sum(weights, -1)
    blended = jnp.einsum(
        "bhqk,bkhd->bqhd",
        weights.astype(jnp.bfloat16),
        val_rows,
        preferred_element_type=jnp.float32,
    )
    return blended / jnp.transpose(row_sum, (0, 2, 1))[..., None]


def to_heads(matrix, blocks):
    return matrix.reshape(blocks, -1, matrix.shape[1] // HEAD_DIM, HEAD_DIM)


def camera_attention(queries, key_rows, val_rows):
    local_rows = queries.shape[0]
    if local_rows >= TOK_CAM:
        blocks = local_rows // TOK_CAM
        result = attend(
            to_heads(queries, blocks), to_heads(key_rows, blocks), to_heads(val_rows, blocks)
        )
    else:
        cam_span = TOK_CAM // local_rows
        position = lax.axis_index("cols")
        key_value = jnp.stack((key_rows, val_rows))
        for which_bit in range(cam_span.bit_length() - 1):
            partner = partner_2(key_value, "cols", which_bit)
            is_lower = position >> which_bit & 1 == 0
            key_value = jnp.where(
                is_lower,
                jnp.concatenate((key_value, partner), 1),
                jnp.concatenate((partner, key_value), 1),
            )
        result = attend(to_heads(queries, 1), to_heads(key_value[0], 1), to_heads(key_value[1], 1))
    return result.reshape(local_rows, -1).astype(jnp.bfloat16)


def plain_body(
    camera_tokens,
    norm_gain,
    query_weight,
    key_weight,
    value_weight,
    query_gain,
    key_gain,
    out_weight,
    up_weight,
    up_bias,
    down_weight,
    down_bias,
    join_gain,
    join_query,
    join_key,
    join_value,
    join_query_gain,
    join_key_gain,
    join_out,
):
    own_rows = camera_tokens.shape[0]
    all_rows = own_rows * lax.axis_size("rows")
    col_rows = all_rows // lax.axis_size("cols")
    attn_width = query_weight.shape[1]
    start_f32 = camera_tokens.astype(jnp.float32)
    normed_all = lax.all_gather(
        normalize(start_f32, norm_gain, shard_moments(start_f32)), "rows", axis=0, tiled=True
    )
    joint_weight = jnp.concatenate((query_weight, key_weight, value_weight, up_weight), 1)
    joint = lax.psum_scatter(
        jnp.dot(normed_all, joint_weight, preferred_element_type=jnp.float32),
        "cols",
        scatter_dimension=0,
        tiled=True,
    )
    up_sum = joint[:, 3 * attn_width :]
    hidden = jax.nn.gelu(up_sum + up_bias, approximate=False).astype(jnp.bfloat16)
    attended = camera_attention(
        head_norm(joint[:, :attn_width], query_gain),
        head_norm(joint[:, attn_width : 2 * attn_width], key_gain),
        joint[:, 2 * attn_width : 3 * attn_width].astype(jnp.bfloat16),
    )
    attn_all, hidden_all = (
        lax.all_gather(attended, "cols", axis=0, tiled=True),
        lax.all_gather(hidden, "cols", axis=0, tiled=True),
    )
    mixed = lax.psum_scatter(
        jnp.dot(attn_all, out_weight, preferred_element_type=jnp.float32)
        + jnp.dot(hidden_all, down_weight, preferred_element_type=jnp.float32),
        "rows",
        scatter_dimension=0,
        tiled=True,
    )
    layer_own = (start_f32 + mixed + down_bias).astype(jnp.bfloat16)
    layer_f32 = layer_own.astype(jnp.float32)
    join_in = lax.all_gather(
        normalize(layer_f32, join_gain, shard_moments(layer_f32)), "rows", axis=0, tiled=True
    )
    join_weight = jnp.concatenate((join_query, join_key, join_value), 1)
    join_joint = lax.psum_scatter(
        jnp.dot(join_in, join_weight, preferred_element_type=jnp.float32),
        "cols",
        scatter_dimension=0,
        tiled=True,
    )
    join_q = head_norm(join_joint[:, :attn_width], join_query_gain)
    join_k = head_norm(join_joint[:, attn_width : 2 * attn_width], join_key_gain)
    join_v = join_joint[:, 2 * attn_width :].astype(jnp.bfloat16)
    heads_here = attn_width // HEAD_DIM
    query_heads = join_q.reshape(col_rows, heads_here, HEAD_DIM)
    inv_root = 1.0 / math.sqrt(HEAD_DIM)
    run_max = jnp.full((heads_here, col_rows), -jnp.inf, jnp.float32)
    run_sum = jnp.zeros((heads_here, col_rows), jnp.float32)
    accum = jnp.zeros((col_rows, heads_here, HEAD_DIM), jnp.float32)
    key_part = lax.all_gather(join_k, "cols", axis=0, tiled=True)
    val_part = lax.all_gather(join_v, "cols", axis=0, tiled=True)
    row_count = key_part.shape[0]
    key_heads = key_part.reshape(row_count, heads_here, HEAD_DIM)
    val_heads = val_part.reshape(row_count, heads_here, HEAD_DIM)
    scores = (
        jnp.einsum("qhd,khd->hqk", query_heads, key_heads, preferred_element_type=jnp.float32)
        * inv_root
    )
    new_max = jnp.max(scores, -1)
    factor = jnp.exp(run_max - new_max)
    weights = jnp.exp(scores - new_max[..., None])
    run_sum = run_sum * factor + jnp.sum(weights, -1)
    accum = accum * jnp.transpose(factor)[..., None] + jnp.einsum(
        "hqk,khd->qhd", weights.astype(jnp.bfloat16), val_heads, preferred_element_type=jnp.float32
    )
    run_max, run_sum, accum = (new_max, run_sum, accum)
    joined_attn = (
        (accum / jnp.transpose(run_sum)[..., None])
        .reshape(col_rows, attn_width)
        .astype(jnp.bfloat16)
    )
    joined_all = lax.all_gather(joined_attn, "cols", axis=0, tiled=True)
    result = lax.psum_scatter(
        jnp.dot(joined_all, join_out, preferred_element_type=jnp.float32),
        "rows",
        scatter_dimension=0,
        tiled=True,
    )
    return (layer_own.astype(jnp.float32) + result).astype(jnp.bfloat16)


F32 = jnp.float32
BF16 = jnp.bfloat16
MESH = pl.DeviceIdType.MESH
VMEM_LIMIT = 66 * 1024 * 1024 - 3 * 1024 * 1024


def each(count, step):
    lax.fori_loop(0, count, lambda i, carry: (step(i), carry)[1], None)


def remote(src, dst, send, recv, device):
    return pltpu.make_async_remote_copy(
        src_ref=src,
        dst_ref=dst,
        send_sem=send,
        recv_sem=recv,
        device_id=device,
        device_id_type=MESH,
    )


def places():
    col = lax.axis_index("cols")
    core = lax.rem(col, 2)
    return col, col + 1 - 2 * core, lax.rem(col + 2, 4)


def greet(cols_away):
    col, row, row_count = lax.axis_index("cols"), lax.axis_index("rows"), lax.axis_size("rows")
    barrier = pltpu.get_barrier_semaphore()
    _, mate, across = places()
    others = {1: mate, 2: across}
    if cols_away == 3:
        others[3] = mate + across - col
    for other in others.values():
        pl.semaphore_signal(barrier, inc=1, device_id={"cols": other}, device_id_type=MESH)

    @pl.when(row > 0)
    def _():
        pl.semaphore_signal(barrier, inc=1, device_id={"rows": row - 1}, device_id_type=MESH)

    @pl.when(row < row_count - 1)
    def _():
        pl.semaphore_signal(barrier, inc=1, device_id={"rows": row + 1}, device_id_type=MESH)

    inner = (row > 0) & (row < row_count - 1)

    @pl.when(inner)
    def _():
        pl.semaphore_wait(barrier, len(others) + 2)

    @pl.when(jnp.logical_not(inner))
    def _():
        pl.semaphore_wait(barrier, len(others) + 1)


def norm_heads(values, scales):
    parts = []
    for start in range(0, values.shape[1], HEAD_DIM):
        part = values[:, start : start + HEAD_DIM]
        mean = jnp.mean(part, -1, keepdims=True)
        var = jnp.mean(part * part, -1, keepdims=True) - mean * mean
        parts.append((part - mean) * lax.rsqrt(var + EPS))
    return (jnp.concatenate(parts, 1) * scales).astype(BF16)


def soft_blend(query, keys, values):
    scores = lax.dot_general(
        query, keys, (((1,), (1,)), ((), ())), preferred_element_type=F32
    ) * (1.0 / math.sqrt(HEAD_DIM))
    weights = jnp.exp(scores - jnp.max(scores, -1, keepdims=True))
    total = jnp.sum(weights, -1, keepdims=True)
    blended = jnp.dot(weights.astype(BF16), values, preferred_element_type=F32)
    return (blended / total).astype(BF16)


def layer_kernel(names, width, *refs):
    r = types.SimpleNamespace(**dict(zip(names, refs)))
    normed, accum, pool, pool_sem = r.normed, r.accum, r.pool, r.pool_sem
    col, mate, across = places()
    diagonal = mate + across - col
    owners = (col, mate, across, diagonal)
    row, rows = lax.axis_index("rows"), lax.axis_size("rows")
    chunks, _, piece, depth = normed.shape
    half = chunks // 2
    ups = r.f_send1.shape[0]
    tile = pool.shape[1]
    wide = r.hid0.shape[-1]
    out_pieces = accum.shape[-1] // tile
    in_pieces = depth // tile
    slot_pieces = max(in_pieces, out_pieces)
    n_in, n_out = 3 + ups, 1 + ups
    last = chunks - 1
    ring = 2 * n_in
    mine = pl.ds(pl.multiple_of(col * wide, HEAD_DIM), wide)
    own_place, mate_place, across_place, diag_place = range(4)

    def load_in(source, slot, start, wid):
        first = slot * slot_pieces
        return pltpu.make_async_copy(
            source.at[:, :, pl.ds(pl.multiple_of(start, HEAD_DIM), wid)],
            pool.at[pl.ds(first, in_pieces), :, pl.ds(0, wid)],
            pool_sem.at[first],
        )

    def load_out(source, slot, start, deep):
        for j in range(out_pieces):
            place = slot * slot_pieces + j
            pltpu.make_async_copy(
                source.at[pl.ds(pl.multiple_of(start, HEAD_DIM), deep), pl.ds(j * tile, tile)],
                pool.at[place, pl.ds(0, deep)],
                pool_sem.at[place],
            ).start()

    def load_camera_in(owner, slot):
        for which, source in enumerate((r.wq, r.wk, r.wv)):
            load_in(source, slot + which, owner * wide, wide).start()
        each(
            ups,
            lambda unit: load_in(
                r.w_up, slot + 3 + unit, owner * (ups * tile) + unit * tile, tile
            ).start(),
        )

    def load_join_in(owner, slot):
        for which, source in enumerate((r.jq, r.jk, r.jv)):
            load_in(source, slot + which, owner * wide, wide).start()

    def load_camera_out(owner, slot):
        load_out(r.w_out, slot, owner * wide, wide)
        each(ups, lambda unit: load_out(r.w_down, slot + 1 + unit, (owner * ups + unit) * tile, tile))

    def in_weight(slot, wid):
        first = slot * slot_pieces
        return pool.at[pl.ds(first, in_pieces), :, pl.ds(0, wid)], pool_sem.at[first]

    def wait_in(slot, wid):
        part, sem = in_weight(slot, wid)
        pltpu.make_async_copy(part, part, sem).wait()

    def wait_out(slot, deep):
        for j in range(out_pieces):
            place = slot * slot_pieces + j
            part = pool.at[place, pl.ds(0, deep)]
            pltpu.make_async_copy(part, part, pool_sem.at[place]).wait()

    def product(slot, left, wid):
        part, _ = in_weight(slot, wid)
        return jnp.dot(left, part[...].reshape(depth, wid), preferred_element_type=F32)

    def add_tile(span, value, slot, begin=False):
        start, count = span
        deep = value.shape[1]
        for j in range(out_pieces):
            part = jnp.dot(
                value, pool[slot * slot_pieces + j, pl.ds(0, deep)], preferred_element_type=F32
            ).reshape(count, rows, piece, tile)
            at = (pl.ds(start, count), slice(None), slice(None), slice(j * tile, (j + 1) * tile))
            if begin:
                accum[at] = part
            else:
                accum[at] += part

    def gather_copy(stage, span, block, right):
        rel = lax.rem(block - row + rows, rows)
        away = lax.rem(rel + (rows - 1 if right else 1), rows)
        part = pl.ds(*span)
        return remote(
            normed.at[part, rel],
            normed.at[part, away],
            (r.g_right if right else r.g_left).at[stage, block],
            r.g_arrive.at[stage, block],
            {"rows": row + 1 if right else row - 1},
        )

    def arrival(stage, span, block):
        rel = lax.rem(block - row + rows, rows)
        part = normed.at[pl.ds(*span), rel]
        pltpu.make_async_copy(part, part, r.g_arrive.at[stage, block]).wait()

    def pass_on(stage, span, block, right):
        @pl.when((row < rows - 1) if right else (row > 0))
        def _():
            gather_copy(stage, span, block, right).start()

    def spread(stage, span):
        pass_on(stage, span, row, True)
        pass_on(stage, span, row, False)

    def take(stage, span, away):
        @pl.when(row >= away)
        def _():
            arrival(stage, span, row - away)
            pass_on(stage, span, row - away, True)

        @pl.when(row + away < rows)
        def _():
            arrival(stage, span, row + away)
            pass_on(stage, span, row + away, False)

    def spread_done(stage, span):
        def done(block):
            @pl.when((row >= block) & (row < rows - 1))
            def _():
                gather_copy(stage, span, block, True).wait_send()

            @pl.when((row <= block) & (row > 0))
            def _():
                gather_copy(stage, span, block, False).wait_send()

        each(rows, done)

    f_send, f_recv, y_recv = (r.f_send0, r.f_send1), (r.f_recv0, r.f_recv1), (r.y_recv0, r.y_recv1)
    p_send, p_recv = (r.p_send0, r.p_send1), (r.p_recv0, r.p_recv1)
    first_sems = ((r.fs0, r.fr0, r.ys0, r.yr0), (r.fs1, r.fr1, r.ys1, r.yr1))
    second_sems = ((r.ps0, r.pr0), (r.ps1, r.pr1))
    counts, wides, offsets = (3, ups), (wide, tile), (0, 3)

    def left_of(region):
        c0, nc, r0, nr = region
        return normed[pl.ds(c0, nc), pl.ds(r0, nr)].reshape(nc * nr * piece, depth)

    def part_of(region):
        c0, nc, r0, nr = region
        return pl.ds(c0, nc), pl.ds(r0, nr)

    def shaped(value, region):
        return value.reshape(region[1], region[3], piece, value.shape[-1])

    def f_copy(group, unit, stage, region):
        at = (unit, *part_of(region))
        fs, fr, _, _ = first_sems[group]
        return remote(
            f_send[group].at[at],
            f_recv[group].at[at],
            fs.at[unit, stage],
            fr.at[unit, stage],
            {"cols": mate},
        )

    def y_copy(group, unit, stage, region):
        at = (unit, *part_of(region))
        _, _, ys, yr = first_sems[group]
        return remote(
            f_send[group].at[at],
            y_recv[group].at[at],
            ys.at[unit, stage],
            yr.at[unit, stage],
            {"cols": across},
        )

    def p_copy(group, unit, stage, span):
        at = (unit, pl.ds(*span))
        ps, pr = second_sems[group]
        return remote(
            p_send[group].at[at],
            p_recv[group].at[at],
            ps.at[unit, stage],
            pr.at[unit, stage],
            {"cols": mate},
        )

    def give(region, stage, groups, base, fresh):
        for group in groups:
            wid = wides[group]

            def step(unit):
                slot = base + offsets[group] + unit
                if fresh:
                    wait_in(slot, wid)
                value = product(slot, left_of(region), wid).astype(BF16)
                f_send[group][(unit, *part_of(region))] = shaped(value, region)
                f_copy(group, unit, stage, region).start()

            each(counts[group], step)

    def send(region, stage, groups, base, fresh):
        for group in groups:
            wid = wides[group]

            def step(unit):
                slot = base + offsets[group] + unit
                if fresh:
                    wait_in(slot, wid)
                value = shaped(product(slot, left_of(region), wid), region)
                at = (unit, *part_of(region))
                f_copy(group, unit, stage, region).wait()
                f_send[group][at] = (value + f_recv[group][at].astype(F32)).astype(BF16)
                y_copy(group, unit, stage, region).start()

            each(counts[group], step)

    def give_second(span, stage, groups, base, fresh):
        for group in groups:
            wid = wides[group]

            def step(unit):
                slot = base + offsets[group] + unit
                if fresh is True:
                    wait_in(slot, wid)
                elif fresh is not False:

                    @pl.when(fresh)
                    def _():
                        wait_in(slot, wid)

                region = (*span, 0, rows)
                value = product(slot, left_of(region), wid).astype(BF16)
                p_send[group][unit, pl.ds(*span)] = shaped(value, region)
                p_copy(group, unit, stage, span).start()

            each(counts[group], step)

    def final(group, unit, span, slot):
        region = (*span, 0, rows)
        wid = wides[group]
        part = pl.ds(*span)
        value = product(slot, left_of(region), wid)
        height = value.shape[0]
        got = p_recv[group][unit, part].astype(F32) + y_recv[group][unit, part].astype(F32)
        return value + got.reshape(height, wid)

    def final_qkv(span, base, gains, wait):
        region = (*span, 0, rows)
        for which in range(3):
            wait(which)
            value = final(0, which, span, base + which)
            if which < 2:
                value = norm_heads(value, gains[which][mine].reshape(1, -1))
            else:
                value = value.astype(BF16)
            r.qkv[which, pl.ds(*span)] = shaped(value, region)

    def hid(place, k, span):
        if isinstance(k, int) and k == 0:
            return r.hid0.at[place, pl.ds(*span)]
        return r.hid1.at[place, k - 1, pl.ds(*span)]

    def hid_value(place, k, span):
        part = hid(place, k, span)
        return part[...].reshape(span[1] * rows * piece, part.shape[-1])

    def tile_id(phase, k):
        return n_out if phase else k

    def to_across(phase, k, c):
        i = tile_id(phase, k)
        return remote(
            hid(own_place, k, (c, 1)),
            hid(across_place, k, (c, 1)),
            r.a_send.at[i, c],
            r.a_recv.at[i, c],
            {"cols": across},
        )

    def to_mate(phase, k, c):
        i = tile_id(phase, k)
        return remote(
            hid(own_place, k, (c, 1)),
            hid(mate_place, k, (c, 1)),
            r.b_send.at[i, c],
            r.b_recv.at[i, c],
            {"cols": mate},
        )

    def forward(phase, k, c):
        i = tile_id(phase, k)
        return remote(
            hid(across_place, k, (c, 1)),
            hid(diag_place, k, (c, 1)),
            r.d_send.at[i, c],
            r.d_recv.at[i, c],
            {"cols": mate},
        )

    def z_right(phase, c, rel):
        return remote(
            r.z_send.at[c, rel],
            r.z_left.at[c, rel - 1],
            r.zr_send.at[phase, c, rel],
            r.zr_recv.at[phase, c, rel - 1],
            {"rows": row + 1},
        )

    def z_left(phase, c, rel):
        there = (rel + 1) % rows
        return remote(
            r.z_send.at[c, rel],
            r.z_right.at[c, there],
            r.zl_send.at[phase, c, rel],
            r.zl_recv.at[phase, c, there],
            {"rows": row - 1},
        )

    def sums(phase, c, step):
        @pl.when(row == step)
        def _():
            for block in range(rows - 1, step, -1):
                rel = block - step
                value = accum[c, rel]
                if step > 0:
                    z_right(phase, c, rel + 1).wait_recv()
                    value += r.z_left[c, rel].astype(F32)
                r.z_send[c, rel] = value.astype(BF16)
                z_right(phase, c, rel).start()

        here = rows - 1 - step

        @pl.when(row == here)
        def _():
            for block in range(here):
                rel = block - here + rows
                value = accum[c, rel]
                if step > 0:
                    z_left(phase, c, rel - 1).wait_recv()
                    value += r.z_right[c, rel].astype(F32)
                r.z_send[c, rel] = value.astype(BF16)
                z_left(phase, c, rel).start()

    def sums_end(phase, c):
        @pl.when(row > 0)
        def _():
            z_right(phase, c, 1).wait_recv()
            accum[c, 0] += r.z_left[c, 0].astype(F32)

        @pl.when(row < rows - 1)
        def _():
            z_left(phase, c, rows - 1).wait_recv()
            accum[c, 0] += r.z_right[c, 0].astype(F32)

    def sums_sent(phase):
        def done(c):
            for rel in range(1, rows):

                @pl.when(row + rel < rows)
                def _():
                    z_right(phase, c, rel).wait_send()

                @pl.when(row + rel >= rows)
                def _():
                    z_left(phase, c, rel).wait_send()

        each(chunks, done)

    def swap(phase, stage, slot, part):
        other = (mate, across, diagonal)[slot]
        return remote(
            r.moments.at[phase, 3, part],
            r.moments.at[phase, slot, part],
            r.m_send.at[stage, slot],
            r.m_recv.at[stage, slot],
            {"cols": other},
        )

    def moments_start(phase, stage, part, values):
        count = values.shape[0]
        flat = values.reshape(count * piece, depth)
        lane = lax.broadcasted_iota(jnp.int32, (count * piece, HEAD_DIM), 1)
        pair = jnp.where(
            lane < HEAD_DIM // 2,
            jnp.sum(flat, 1, keepdims=True),
            jnp.sum(flat * flat, 1, keepdims=True),
        )
        r.moments[phase, 3, part] = pair.reshape(count, piece, HEAD_DIM)
        for slot in range(3):
            swap(phase, stage, slot, part).start()

    def moments_end(phase, stage, part, values, gain):
        for slot in range(3):
            swap(phase, stage, slot, part).wait_recv()
        m = r.moments
        total = (m[phase, 3, part] + m[phase, 0, part]) + (m[phase, 1, part] + m[phase, 2, part])
        mean = total[:, :, :1] / width
        var = total[:, :, HEAD_DIM // 2 : HEAD_DIM // 2 + 1] / width - mean * mean
        scaled = (values - mean) * lax.rsqrt(var + EPS) * gain[...].reshape(1, 1, -1)
        normed[part, 0] = scaled.astype(BF16)

    def moments_sent(phase, stage, part):
        for slot in range(3):
            swap(phase, stage, slot, part).wait_send()

    load_camera_in(diagonal, 0)
    load_camera_in(across, n_in)
    load_camera_in(mate, ring)
    greet(3)
    every = pl.ds(0, chunks)
    halves = ((0, half), (half, half))
    own = r.tokens[...].astype(F32)
    moments_start(0, 0, every, own)
    moments_end(0, 0, every, own, r.gain)
    spread(0, halves[0])
    both = (0, 1)
    region = (0, chunks, 0, 1)
    give(region, 0, both, 0, True)
    take(0, halves[0], 1)
    send(region, 0, both, n_in, True)
    take(0, halves[0], 2)
    spread(1, halves[1])
    take(0, halves[0], 3)

    def others(h):
        rest = (h * half, half, 1, rows - 1)
        give(rest, 1 + h, both, 0, False)
        send(rest, 1 + h, both, n_in, False)

        @pl.when(h == 0)
        def _():
            take(1, halves[1], 1)

        give_second((h * half, half), h, both, ring, h == 0)

        @pl.when(h == 0)
        def _():
            take(1, halves[1], 2)
            take(1, halves[1], 3)

    each(2, others)
    load_camera_in(col, ring)
    load_camera_out(col, 0)
    load_camera_out(mate, n_out)
    load_camera_out(across, 2 * n_out)
    moments_sent(0, 0, every)
    for h in range(2):
        spread_done(h, halves[h])

    def share(phase, k, c, away):
        to_mate(phase, k, c).start()
        if away:
            to_across(phase, k, c).start()

    def finals(h):
        span = (h * half, half)
        rest = (h * half, half, 1, rows - 1)

        def arrived(group, unit):
            @pl.when(h == 0)
            def _():
                wait_in(ring + offsets[group] + unit, wides[group])
                y_copy(group, unit, 0, region).wait_recv()

            p_copy(group, unit, h, span).wait_recv()
            y_copy(group, unit, 1 + h, rest).wait_recv()

        final_qkv(span, ring, (r.q_gain, r.k_gain), lambda which: arrived(0, which))

        def camera(rel):
            for start in range(0, wide, HEAD_DIM):
                head = pl.ds(start, HEAD_DIM)
                q, k, v = (
                    r.qkv[which, pl.ds(*span), rel, :, head].reshape(half * piece, HEAD_DIM)
                    for which in range(3)
                )
                r.hid0[own_place, pl.ds(*span), rel, :, head] = soft_blend(q, k, v).reshape(
                    half, piece, HEAD_DIM
                )

        each(rows, camera)

        def ship(k):
            def one(i):
                c = h * half + i
                to_mate(0, k, c).start()

                @pl.when(h == 0)
                def _():
                    to_across(0, k, c).start()

            each(half, one)

        ship(0)

        def activate(unit):
            arrived(1, unit)
            raw = final(1, unit, span, ring + 3 + unit) + r.bias[col * ups + unit]
            value = (raw * (1.0 + lax.erf(raw * math.sqrt(0.5))) * 0.5).astype(BF16)
            r.hid1[own_place, unit, pl.ds(*span)] = shaped(value, (*span, 0, rows))
            ship(unit + 1)

        each(ups, activate)

        def fresh_out(slot, deep):
            @pl.when(h == 0)
            def _():
                wait_out(slot, deep)

        def arrived_mate(k):
            each(half, lambda i: to_mate(0, k, h * half + i).wait_recv())

        def near_up(place):
            def one(unit):
                slot = place * n_out + 1 + unit
                fresh_out(slot, tile)
                if place == mate_place:
                    arrived_mate(unit + 1)
                add_tile(span, hid_value(place, unit + 1, span), slot)

            return one

        fresh_out(0, wide)
        add_tile(span, hid_value(own_place, 0, span), 0, True)
        each(ups, near_up(own_place))
        fresh_out(n_out, wide)
        arrived_mate(0)
        add_tile(span, hid_value(mate_place, 0, span), n_out)
        each(ups, near_up(mate_place))

    each(2, finals)
    load_camera_out(diagonal, ring)
    load_join_in(diagonal, 0)
    load_join_in(across, 3)
    join_out_slots = (2 * n_out - 2, 2 * n_out - 1, ring + n_out, ring + n_out + 1)
    for place in range(4):
        load_out(r.w_join, join_out_slots[place], owners[place] * wide, wide)

    def far(c, k):
        ahead = k + AHEAD
        later, kind = c + ahead // n_out, ahead % n_out

        @pl.when((later >= half) & (later < chunks))
        def _():
            to_across(0, kind, later).start()

        to_across(0, k, c).wait_recv()
        forward(0, k, c).start()

        @pl.when(c == 0)
        def _():
            wait_out(2 * n_out + k, wide if k == 0 else tile)
            wait_out(ring + k, wide if k == 0 else tile)

        add_tile((c, 1), hid_value(across_place, k, (c, 1)), 2 * n_out + k)
        forward(0, k, c).wait_recv()
        add_tile((c, 1), hid_value(diag_place, k, (c, 1)), ring + k)

    def norm_start(c):
        sums_end(0, c)
        total = accum[c, 0] + r.tokens[c].astype(F32) + r.down_bias[...].reshape(1, -1)
        layer = total.astype(BF16)
        r.layer[c] = layer
        moments_start(1, 1 + c, pl.ds(c, 1), layer.astype(F32)[None])

    def norm_end(c):
        moments_end(1, 1 + c, pl.ds(c, 1), r.layer[pl.ds(c, 1)].astype(F32), r.join_gain)
        spread(2 + c, (c, 1))

    def steps(c):
        def before(back, action):
            @pl.when(c >= back)
            def _():
                action(c - back)

        far(c, 0)
        before(1, lambda b: sums(0, b, 1))
        far(c, 1)
        before(1, lambda b: sums(0, b, 2))
        for k in range(2, n_out):
            far(c, k)
            if k == 2:
                before(1, norm_start)
        sums(0, c, 0)
        before(1, norm_end)
        for away in range(1, rows):
            before(2, lambda b: take(2 + b, (b, 1), away))

    each(chunks, steps)
    load_join_in(mate, 2 * n_out)
    load_join_in(col, ring)

    def shared(c):
        for k in range(n_out):
            to_across(0, k, c).wait_send()
            to_mate(0, k, c).wait_send()
            forward(0, k, c).wait_send()

    each(chunks, shared)
    for group in range(2):

        def sent(unit):
            y_copy(group, unit, 0, region).wait_send()
            for h in range(2):
                y_copy(group, unit, 1 + h, (h * half, half, 1, rows - 1)).wait_send()
                p_copy(group, unit, h, (h * half, half)).wait_send()

        each(counts[group], sent)

    spans = [(last - 1, 1), (last, 1)]
    if chunks > 2:
        spans.insert(0, (0, last - 1))
    regions = [(*span, 0, rows) for span in spans]
    n_spans = len(spans)

    def join_give(i, fresh=False):
        give(regions[i], 3 + i, (0,), 0, fresh)

    def join_send(i, fresh=False):
        send(regions[i], 3 + i, (0,), 3, fresh)

    def join_second(i, fresh=False):
        give_second(spans[i], 2 + i, (0,), 2 * n_out, fresh)

    def join_final(i, fresh=False):
        def arrived(which):
            if fresh:
                wait_in(ring + which, wide)
            p_copy(0, which, 2 + i, spans[i]).wait_recv()
            y_copy(0, which, 3 + i, regions[i]).wait_recv()

        final_qkv(spans[i], ring, (r.jq_gain, r.jk_gain), arrived)

    def take_one(c, away):
        take(2 + c, (c, 1), away)

    main = n_spans == 3
    if main:
        join_give(0, True)
    sums(0, last, 1)
    take_one(last - 1, 1)
    if main:
        join_send(0, True)
    sums(0, last, 2)
    take_one(last - 1, 2)
    if main:
        join_second(0, True)
    norm_start(last)
    take_one(last - 1, 3)
    join_give(n_spans - 2, not main)
    join_send(n_spans - 2, not main)
    norm_end(last)
    join_second(n_spans - 2, not main)
    if main:
        join_final(0, True)
    take_one(last, 1)
    take_one(last, 2)
    join_final(n_spans - 2, not main)
    take_one(last, 3)
    join_give(n_spans - 1)
    join_send(n_spans - 1)
    join_second(n_spans - 1)
    sums_sent(0)
    join_final(n_spans - 1)

    def blend(c):
        for start in range(0, wide, HEAD_DIM):
            head = pl.ds(start, HEAD_DIM)
            q = r.qkv[0, c, :, :, head].reshape(rows * piece, HEAD_DIM)
            k, v = (
                r.qkv[which, :, :, :, head].reshape(chunks * rows * piece, HEAD_DIM)
                for which in (1, 2)
            )
            r.hid0[own_place, c, :, :, head] = soft_blend(q, k, v).reshape(rows, piece, HEAD_DIM)
        to_across(1, 0, c).start()
        to_mate(1, 0, c).start()

    def result_of(c):
        sums_end(1, c)
        r.result[c] = (accum[c, 0] + r.layer[c].astype(F32)).astype(BF16)

    lead = min(2, chunks)
    each(lead, blend)
    for slot in join_out_slots:
        wait_out(slot, wide)

    def join_steps(c):
        def add(place, begin=False):
            add_tile((c, 1), hid_value(place, 0, (c, 1)), join_out_slots[place], begin)

        @pl.when(c + lead < chunks)
        def _():
            blend(c + lead)

        add(own_place, True)
        to_mate(1, 0, c).wait_recv()
        add(mate_place)
        to_across(1, 0, c).wait_recv()
        forward(1, 0, c).start()
        add(across_place)
        forward(1, 0, c).wait_recv()
        add(diag_place)
        sums(1, c, 0)

        @pl.when(c >= 1)
        def _():
            sums(1, c - 1, 1)
            sums(1, c - 1, 2)

        @pl.when(c >= 2)
        def _():
            result_of(c - 2)

    each(chunks, join_steps)
    sums(1, last, 1)
    sums(1, last, 2)
    result_of(last - 1)
    result_of(last)

    sums_sent(1)

    def drained(c):
        to_across(1, 0, c).wait_send()
        to_mate(1, 0, c).wait_send()
        forward(1, 0, c).wait_send()
        moments_sent(1, 1 + c, pl.ds(c, 1))
        spread_done(2 + c, (c, 1))

    each(chunks, drained)
    for i in range(n_spans):

        def sent_join(unit):
            y_copy(0, unit, 3 + i, regions[i]).wait_send()
            p_copy(0, unit, 2 + i, spans[i]).wait_send()

        each(3, sent_join)


AHEAD = 3
CHUNKS = 4


def tile_of(depth, columns, cols):
    ups = 3
    tile = columns // cols // ups
    return ups, tile


def kernel_body(
    camera_tokens,
    norm_gain,
    query_weight,
    key_weight,
    value_weight,
    query_gain,
    key_gain,
    out_weight,
    up_weight,
    up_bias,
    down_weight,
    down_bias,
    join_gain,
    join_query,
    join_key,
    join_value,
    join_query_gain,
    join_key_gain,
    join_out,
):
    own_rows, depth = camera_tokens.shape
    rows, cols = lax.axis_size("rows"), lax.axis_size("cols")
    width = out_weight.shape[1]
    wide = query_weight.shape[1] // cols
    ups, tile = tile_of(depth, up_weight.shape[1], cols)
    chunks, piece = CHUNKS, own_rows // CHUNKS
    n_in, n_out = 3 + ups, 1 + ups
    slot_pieces = max(depth, width) // tile

    def blocked(weight):
        return weight.reshape(depth // tile, tile, weight.shape[1])

    any_spec, vmem_spec = pl.BlockSpec(memory_space=pl.ANY), pl.BlockSpec(memory_space=pltpu.VMEM)
    inputs = {
        "tokens": (camera_tokens.reshape(chunks, piece, depth), vmem_spec),
        "gain": (norm_gain, vmem_spec),
        "q_gain": (query_gain, vmem_spec),
        "k_gain": (key_gain, vmem_spec),
        "bias": (up_bias.reshape(cols * ups, 1, tile), vmem_spec),
        "down_bias": (down_bias, vmem_spec),
        "join_gain": (join_gain, vmem_spec),
        "jq_gain": (join_query_gain, vmem_spec),
        "jk_gain": (join_key_gain, vmem_spec),
        "wq": (blocked(query_weight), any_spec),
        "wk": (blocked(key_weight), any_spec),
        "wv": (blocked(value_weight), any_spec),
        "w_up": (blocked(up_weight), any_spec),
        "w_out": (out_weight, any_spec),
        "w_down": (down_weight, any_spec),
        "jq": (blocked(join_query), any_spec),
        "jk": (blocked(join_key), any_spec),
        "jv": (blocked(join_value), any_spec),
        "w_join": (join_out, any_spec),
    }
    dma, vmem = pltpu.SemaphoreType.DMA, pltpu.VMEM
    scratch = {
        "pool": vmem((3 * n_in * slot_pieces, tile, tile), BF16),
        "pool_sem": dma((3 * n_in * slot_pieces,)),
        "normed": vmem((chunks, rows, piece, depth), BF16),
        "moments": vmem((2, 4, chunks, piece, HEAD_DIM), F32),
        "m_send": dma((1 + chunks, 3)),
        "m_recv": dma((1 + chunks, 3)),
        "g_right": dma((2 + chunks, rows)),
        "g_left": dma((2 + chunks, rows)),
        "g_arrive": dma((2 + chunks, rows)),
        "qkv": vmem((3, chunks, rows, piece, wide), BF16),
        "hid0": vmem((4, chunks, rows, piece, wide), BF16),
        "hid1": vmem((4, ups, chunks, rows, piece, tile), BF16),
        "accum": vmem((chunks, rows, piece, width), F32),
        "z_send": vmem((chunks, rows, piece, width), BF16),
        "z_left": vmem((chunks, rows, piece, width), BF16),
        "z_right": vmem((chunks, rows, piece, width), BF16),
        "layer": vmem((chunks, piece, width), BF16),
    }
    for name in ("zr_send", "zr_recv", "zl_send", "zl_recv"):
        scratch[name] = dma((2, chunks, rows))
    for name in ("a_send", "a_recv", "b_send", "b_recv", "d_send", "d_recv"):
        scratch[name] = dma((n_out + 1, chunks))
    for group, (count, wid) in enumerate(((3, wide), (ups, tile))):
        for name in ("f_send", "f_recv", "y_recv", "p_send", "p_recv"):
            scratch[name + str(group)] = vmem((count, chunks, rows, piece, wid), BF16)
        for name in ("fs", "fr", "ys", "yr", "ps", "pr"):
            scratch[name + str(group)] = dma((count, 6))
    names = (*inputs, "result", *scratch)
    joined = pl.pallas_call(
        functools.partial(layer_kernel, names, float(depth * cols)),
        name="layer",
        out_shape=jax.ShapeDtypeStruct((chunks, piece, width), BF16),
        in_specs=[spec for _, spec in inputs.values()],
        out_specs=vmem_spec,
        scratch_shapes=list(scratch.values()),
        compiler_params=pltpu.CompilerParams(
            collective_id=0, has_side_effects=True, vmem_limit_bytes=VMEM_LIMIT
        ),
    )(*[value for value, _ in inputs.values()])
    return joined.reshape(own_rows, width)


def fits(mesh):
    cols, rows = mesh.shape["cols"], mesh.shape["rows"]
    return cols == 4 and rows == 4 and D % (rows * cols * HEAD_DIM) == 0


def body(*arrays):
    tokens, up_weight = arrays[0], arrays[8]
    own_rows, depth = tokens.shape
    ups, tile = tile_of(depth, up_weight.shape[1], lax.axis_size("cols"))
    wide = arrays[2].shape[1] // lax.axis_size("cols")
    good = (
        own_rows == 2 * TOK_CAM
        and tile * ups * lax.axis_size("cols") == up_weight.shape[1]
        and tile % HEAD_DIM == 0
        and depth % tile == 0
        and arrays[7].shape[1] == depth
        and wide <= tile
        and wide % HEAD_DIM == 0
    )
    return kernel_body(*arrays) if good else plain_body(*arrays)


def solution(mesh):
    in_specs = (
        P(("groups", "rows"), "cols"),
        P("cols"),
        P("cols", "rows"),
        P("cols", "rows"),
        P("cols", "rows"),
        P("rows"),
        P("rows"),
        P("rows", "cols"),
        P("cols", "rows"),
        P("rows"),
        P("rows", "cols"),
        P("cols"),
        P("cols"),
        P("cols", "rows"),
        P("cols", "rows"),
        P("cols", "rows"),
        P("rows"),
        P("rows"),
        P("rows", "cols"),
    )
    out_specs = P(("groups", "rows"), "cols")
    inner = body if fits(mesh) else plain_body
    return jax.shard_map(inner, mesh=mesh, in_specs=in_specs, out_specs=out_specs, check_vma=False)
```

```python
import functools
import math
import types

import jax
import jax.numpy as jnp
from jax import lax
from jax.experimental import pallas as pl
from jax.experimental.pallas import tpu as pltpu
from jax.sharding import PartitionSpec as P

HEAD_DIM = 128
TOK_CAM = 64
D = 6144


EPS = 1e-06


def partner_2(array, axis, bit):
    return lax.ppermute(array, axis, [(i, i ^ 1 << bit) for i in range(lax.axis_size(axis))])


def normalize(values, scales, moments):
    row_mean = moments[0] / D
    row_var = moments[1] / D - row_mean * row_mean
    return ((values - row_mean[:, None]) * lax.rsqrt(row_var[:, None] + EPS) * scales).astype(
        jnp.bfloat16
    )


def shard_moments(values):
    return lax.psum((jnp.sum(values, 1), jnp.sum(values * values, 1)), "cols")


def head_norm(values, scales):
    row_count = values.shape[0]
    grouped = values.reshape(row_count, -1, HEAD_DIM)
    row_mean = jnp.mean(grouped, -1, keepdims=True)
    row_var = jnp.mean(grouped * grouped, -1, keepdims=True) - row_mean * row_mean
    normed = (grouped - row_mean) * lax.rsqrt(row_var + EPS)
    return (normed.reshape(row_count, -1) * scales).astype(jnp.bfloat16)


def attend(queries, key_rows, val_rows):
    inv_root = 1.0 / math.sqrt(HEAD_DIM)
    scores = (
        jnp.einsum("bqhd,bkhd->bhqk", queries, key_rows, preferred_element_type=jnp.float32)
        * inv_root
    )
    row_max = jnp.max(scores, -1, keepdims=True)
    weights = jnp.exp(scores - row_max)
    row_sum = jnp.sum(weights, -1)
    blended = jnp.einsum(
        "bhqk,bkhd->bqhd",
        weights.astype(jnp.bfloat16),
        val_rows,
        preferred_element_type=jnp.float32,
    )
    return blended / jnp.transpose(row_sum, (0, 2, 1))[..., None]


def to_heads(matrix, blocks):
    return matrix.reshape(blocks, -1, matrix.shape[1] // HEAD_DIM, HEAD_DIM)


def camera_attention(queries, key_rows, val_rows):
    local_rows = queries.shape[0]
    if local_rows >= TOK_CAM:
        blocks = local_rows // TOK_CAM
        result = attend(
            to_heads(queries, blocks), to_heads(key_rows, blocks), to_heads(val_rows, blocks)
        )
    else:
        cam_span = TOK_CAM // local_rows
        position = lax.axis_index("cols")
        key_value = jnp.stack((key_rows, val_rows))
        for which_bit in range(cam_span.bit_length() - 1):
            partner = partner_2(key_value, "cols", which_bit)
            is_lower = position >> which_bit & 1 == 0
            key_value = jnp.where(
                is_lower,
                jnp.concatenate((key_value, partner), 1),
                jnp.concatenate((partner, key_value), 1),
            )
        result = attend(to_heads(queries, 1), to_heads(key_value[0], 1), to_heads(key_value[1], 1))
    return result.reshape(local_rows, -1).astype(jnp.bfloat16)


def plain_body(
    camera_tokens,
    norm_gain,
    query_weight,
    key_weight,
    value_weight,
    query_gain,
    key_gain,
    out_weight,
    up_weight,
    up_bias,
    down_weight,
    down_bias,
    join_gain,
    join_query,
    join_key,
    join_value,
    join_query_gain,
    join_key_gain,
    join_out,
):
    own_rows = camera_tokens.shape[0]
    all_rows = own_rows * lax.axis_size("rows")
    col_rows = all_rows // lax.axis_size("cols")
    attn_width = query_weight.shape[1]
    start_f32 = camera_tokens.astype(jnp.float32)
    normed_all = lax.all_gather(
        normalize(start_f32, norm_gain, shard_moments(start_f32)), "rows", axis=0, tiled=True
    )
    joint_weight = jnp.concatenate((query_weight, key_weight, value_weight, up_weight), 1)
    joint = lax.psum_scatter(
        jnp.dot(normed_all, joint_weight, preferred_element_type=jnp.float32),
        "cols",
        scatter_dimension=0,
        tiled=True,
    )
    up_sum = joint[:, 3 * attn_width :]
    hidden = jax.nn.gelu(up_sum + up_bias, approximate=False).astype(jnp.bfloat16)
    attended = camera_attention(
        head_norm(joint[:, :attn_width], query_gain),
        head_norm(joint[:, attn_width : 2 * attn_width], key_gain),
        joint[:, 2 * attn_width : 3 * attn_width].astype(jnp.bfloat16),
    )
    attn_all, hidden_all = (
        lax.all_gather(attended, "cols", axis=0, tiled=True),
        lax.all_gather(hidden, "cols", axis=0, tiled=True),
    )
    mixed = lax.psum_scatter(
        jnp.dot(attn_all, out_weight, preferred_element_type=jnp.float32)
        + jnp.dot(hidden_all, down_weight, preferred_element_type=jnp.float32),
        "rows",
        scatter_dimension=0,
        tiled=True,
    )
    layer_own = (start_f32 + mixed + down_bias).astype(jnp.bfloat16)
    layer_f32 = layer_own.astype(jnp.float32)
    join_in = lax.all_gather(
        normalize(layer_f32, join_gain, shard_moments(layer_f32)), "rows", axis=0, tiled=True
    )
    join_weight = jnp.concatenate((join_query, join_key, join_value), 1)
    join_joint = lax.psum_scatter(
        jnp.dot(join_in, join_weight, preferred_element_type=jnp.float32),
        "cols",
        scatter_dimension=0,
        tiled=True,
    )
    join_q = head_norm(join_joint[:, :attn_width], join_query_gain)
    join_k = head_norm(join_joint[:, attn_width : 2 * attn_width], join_key_gain)
    join_v = join_joint[:, 2 * attn_width :].astype(jnp.bfloat16)
    heads_here = attn_width // HEAD_DIM
    query_heads = join_q.reshape(col_rows, heads_here, HEAD_DIM)
    inv_root = 1.0 / math.sqrt(HEAD_DIM)
    run_max = jnp.full((heads_here, col_rows), -jnp.inf, jnp.float32)
    run_sum = jnp.zeros((heads_here, col_rows), jnp.float32)
    accum = jnp.zeros((col_rows, heads_here, HEAD_DIM), jnp.float32)
    key_part = lax.all_gather(join_k, "cols", axis=0, tiled=True)
    val_part = lax.all_gather(join_v, "cols", axis=0, tiled=True)
    row_count = key_part.shape[0]
    key_heads = key_part.reshape(row_count, heads_here, HEAD_DIM)
    val_heads = val_part.reshape(row_count, heads_here, HEAD_DIM)
    scores = (
        jnp.einsum("qhd,khd->hqk", query_heads, key_heads, preferred_element_type=jnp.float32)
        * inv_root
    )
    new_max = jnp.max(scores, -1)
    factor = jnp.exp(run_max - new_max)
    weights = jnp.exp(scores - new_max[..., None])
    run_sum = run_sum * factor + jnp.sum(weights, -1)
    accum = accum * jnp.transpose(factor)[..., None] + jnp.einsum(
        "hqk,khd->qhd", weights.astype(jnp.bfloat16), val_heads, preferred_element_type=jnp.float32
    )
    run_max, run_sum, accum = (new_max, run_sum, accum)
    joined_attn = (
        (accum / jnp.transpose(run_sum)[..., None])
        .reshape(col_rows, attn_width)
        .astype(jnp.bfloat16)
    )
    joined_all = lax.all_gather(joined_attn, "cols", axis=0, tiled=True)
    result = lax.psum_scatter(
        jnp.dot(joined_all, join_out, preferred_element_type=jnp.float32),
        "rows",
        scatter_dimension=0,
        tiled=True,
    )
    return (layer_own.astype(jnp.float32) + result).astype(jnp.bfloat16)


F32 = jnp.float32
BF16 = jnp.bfloat16
MESH = pl.DeviceIdType.MESH
VMEM_LIMIT = 66 * 1024 * 1024 - 3 * 1024 * 1024


def each(count, step):
    lax.fori_loop(0, count, lambda i, carry: (step(i), carry)[1], None)


def remote(src, dst, send, recv, device):
    return pltpu.make_async_remote_copy(
        src_ref=src,
        dst_ref=dst,
        send_sem=send,
        recv_sem=recv,
        device_id=device,
        device_id_type=MESH,
    )


def places():
    col = lax.axis_index("cols")
    core = lax.rem(col, 2)
    return col, col + 1 - 2 * core, lax.rem(col + 2, 4)


def greet(cols_away):
    col, row, row_count = lax.axis_index("cols"), lax.axis_index("rows"), lax.axis_size("rows")
    barrier = pltpu.get_barrier_semaphore()
    _, mate, across = places()
    others = {1: mate, 2: across}
    if cols_away == 3:
        others[3] = mate + across - col
    for other in others.values():
        pl.semaphore_signal(barrier, inc=1, device_id={"cols": other}, device_id_type=MESH)

    @pl.when(row > 0)
    def _():
        pl.semaphore_signal(barrier, inc=1, device_id={"rows": row - 1}, device_id_type=MESH)

    @pl.when(row < row_count - 1)
    def _():
        pl.semaphore_signal(barrier, inc=1, device_id={"rows": row + 1}, device_id_type=MESH)

    inner = (row > 0) & (row < row_count - 1)

    @pl.when(inner)
    def _():
        pl.semaphore_wait(barrier, len(others) + 2)

    @pl.when(jnp.logical_not(inner))
    def _():
        pl.semaphore_wait(barrier, len(others) + 1)


def norm_heads(values, scales):
    parts = []
    for start in range(0, values.shape[1], HEAD_DIM):
        part = values[:, start : start + HEAD_DIM]
        mean = jnp.mean(part, -1, keepdims=True)
        var = jnp.mean(part * part, -1, keepdims=True) - mean * mean
        parts.append((part - mean) * lax.rsqrt(var + EPS))
    return (jnp.concatenate(parts, 1) * scales).astype(BF16)


def soft_blend(query, keys, values):
    scores = lax.dot_general(
        query, keys, (((1,), (1,)), ((), ())), preferred_element_type=F32
    ) * (1.0 / math.sqrt(HEAD_DIM))
    weights = jnp.exp(scores - jnp.max(scores, -1, keepdims=True))
    total = jnp.sum(weights, -1, keepdims=True)
    blended = jnp.dot(weights.astype(BF16), values, preferred_element_type=F32)
    return (blended / total).astype(BF16)


def layer_kernel(names, width, *refs):
    r = types.SimpleNamespace(**dict(zip(names, refs)))
    normed, accum, pool, pool_sem = r.normed, r.accum, r.pool, r.pool_sem
    col, mate, across = places()
    diagonal = mate + across - col
    owners = (col, mate, across, diagonal)
    row, rows = lax.axis_index("rows"), lax.axis_size("rows")
    chunks, _, piece, depth = normed.shape
    half = chunks // 2
    ups = r.f_send1.shape[0]
    tile = pool.shape[1]
    wide = r.hid0.shape[-1]
    out_pieces = accum.shape[-1] // tile
    in_pieces = depth // tile
    slot_pieces = max(in_pieces, out_pieces)
    n_in, n_out = 3 + ups, 1 + ups
    last = chunks - 1
    ring = 2 * n_in
    mine = pl.ds(pl.multiple_of(col * wide, HEAD_DIM), wide)
    own_place, mate_place, across_place, diag_place = range(4)

    def load_in(source, slot, start, wid):
        first = slot * slot_pieces
        return pltpu.make_async_copy(
            source.at[:, :, pl.ds(pl.multiple_of(start, HEAD_DIM), wid)],
            pool.at[pl.ds(first, in_pieces), :, pl.ds(0, wid)],
            pool_sem.at[slot],
        )

    def load_out(source, slot, start, deep):
        for j in range(out_pieces):
            pltpu.make_async_copy(
                source.at[pl.ds(pl.multiple_of(start, HEAD_DIM), deep), pl.ds(j * tile, tile)],
                pool.at[slot * slot_pieces + j, pl.ds(0, deep)],
                pool_sem.at[slot],
            ).start()

    def load_camera_in(owner, slot):
        for which, source in enumerate((r.wq, r.wk, r.wv)):
            load_in(source, slot + which, owner * wide, wide).start()
        each(
            ups,
            lambda unit: load_in(
                r.w_up, slot + 3 + unit, owner * (ups * tile) + unit * tile, tile
            ).start(),
        )

    def load_join_in(owner, slot):
        for which, source in enumerate((r.jq, r.jk, r.jv)):
            load_in(source, slot + which, owner * wide, wide).start()

    def load_camera_out(owner, slot):
        load_out(r.w_out, slot, owner * wide, wide)
        each(ups, lambda unit: load_out(r.w_down, slot + 1 + unit, (owner * ups + unit) * tile, tile))

    def in_weight(slot, wid):
        return pool.at[pl.ds(slot * slot_pieces, in_pieces), :, pl.ds(0, wid)]

    def wait_in(slot, wid):
        part = in_weight(slot, wid)
        pltpu.make_async_copy(part, part, pool_sem.at[slot]).wait()

    def wait_out(slot, deep):
        part = pool.at[pl.ds(slot * slot_pieces, out_pieces), pl.ds(0, deep)]
        pltpu.make_async_copy(part, part, pool_sem.at[slot]).wait()

    def product(slot, left, wid):
        weight = in_weight(slot, wid)[...].reshape(depth, wid)
        return jnp.dot(left, weight, preferred_element_type=F32)

    def add_tile(span, value, slot, begin=False):
        start, count = span
        deep = value.shape[1]
        for j in range(out_pieces):
            part = jnp.dot(
                value, pool[slot * slot_pieces + j, pl.ds(0, deep)], preferred_element_type=F32
            ).reshape(count, rows, piece, tile)
            at = (pl.ds(start, count), slice(None), slice(None), slice(j * tile, (j + 1) * tile))
            if begin:
                accum[at] = part
            else:
                accum[at] += part

    def gather_copy(c, block, right):
        rel = lax.rem(block - row + rows, rows)
        away = lax.rem(rel + (rows - 1 if right else 1), rows)
        return remote(
            normed.at[c, rel],
            normed.at[c, away],
            r.g_send.at[int(right)],
            r.g_arrive.at[c, block],
            {"rows": row + 1 if right else row - 1},
        )

    def arrival(c, block):
        part = normed.at[c, lax.rem(block - row + rows, rows)]
        pltpu.make_async_copy(part, part, r.g_arrive.at[c, block]).wait()

    def pass_on(c, block, right):
        @pl.when((row < rows - 1) if right else (row > 0))
        def _():
            gather_copy(c, block, right).start()

    def spread(c):
        pass_on(c, row, True)
        pass_on(c, row, False)

    def take(c, away):
        @pl.when(row >= away)
        def _():
            arrival(c, row - away)
            pass_on(c, row - away, True)

        @pl.when(row + away < rows)
        def _():
            arrival(c, row + away)
            pass_on(c, row + away, False)

    def spread_done():
        for place in range(rows):

            @pl.when(row == place)
            def _():
                if place < rows - 1:
                    all_sent(normed.at[:, pl.ds(0, place + 1)], r.g_send.at[1])
                if place > 0:
                    all_sent(normed.at[:, pl.ds(0, rows - place)], r.g_send.at[0])

    f_send, f_recv, y_recv = (r.f_send0, r.f_send1), (r.f_recv0, r.f_recv1), (r.y_recv0, r.y_recv1)
    p_send, p_recv = (r.p_send0, r.p_send1), (r.p_recv0, r.p_recv1)
    first_sems = ((r.fs0, r.fr0, r.yr0), (r.fs1, r.fr1, r.yr1))
    second_recv = (r.pr0, r.pr1)
    counts, wides, offsets = (3, ups), (wide, tile), (0, 3)

    def left_of(region):
        c0, nc, r0, nr = region
        return normed[pl.ds(c0, nc), pl.ds(r0, nr)].reshape(nc * nr * piece, depth)

    def part_of(region):
        c0, nc, r0, nr = region
        return pl.ds(c0, nc), pl.ds(r0, nr)

    def shaped(value, region):
        return value.reshape(region[1], region[3], piece, value.shape[-1])

    def f_copy(group, unit, stage, region):
        at = (unit, *part_of(region))
        fs, fr, _ = first_sems[group]
        return remote(
            f_send[group].at[at], f_recv[group].at[at], fs.at[unit], fr.at[unit, stage], {"cols": mate}
        )

    def y_copy(group, unit, stage, region):
        at = (unit, *part_of(region))
        yr = first_sems[group][2]
        return remote(
            f_send[group].at[at],
            y_recv[group].at[at],
            r.ys.at[group],
            yr.at[unit, stage],
            {"cols": across},
        )

    def p_copy(group, unit, stage, span):
        at = (unit, pl.ds(*span))
        return remote(
            p_send[group].at[at],
            p_recv[group].at[at],
            r.ps.at[group],
            second_recv[group].at[unit, stage],
            {"cols": mate},
        )

    def all_sent(source, sem):
        pltpu.make_async_copy(source, source, sem).wait()

    def give(region, stage, group, base, fresh):
        wid = wides[group]

        def step(unit):
            slot = base + offsets[group] + unit
            if fresh:
                wait_in(slot, wid)
            value = product(slot, left_of(region), wid).astype(BF16)
            f_send[group][(unit, *part_of(region))] = shaped(value, region)
            f_copy(group, unit, stage, region).start()

        each(counts[group], step)

    def send(region, stage, group, base, fresh, start=True):
        wid = wides[group]

        def step(unit):
            slot = base + offsets[group] + unit
            if fresh:
                wait_in(slot, wid)
            value = shaped(product(slot, left_of(region), wid), region)
            at = (unit, *part_of(region))
            f_copy(group, unit, stage, region).wait()
            f_send[group][at] = (value + f_recv[group][at].astype(F32)).astype(BF16)
            if start:
                y_copy(group, unit, stage, region).start()

        each(counts[group], step)

    def give_second(span, stage, group, base, fresh):
        wid = wides[group]
        region = (*span, 0, rows)

        def step(unit):
            slot = base + offsets[group] + unit
            if fresh:
                wait_in(slot, wid)
            value = product(slot, left_of(region), wid).astype(BF16)
            p_send[group][unit, pl.ds(*span)] = shaped(value, region)
            p_copy(group, unit, stage, span).start()

        each(counts[group], step)

    def final(group, unit, span, slot):
        region = (*span, 0, rows)
        wid = wides[group]
        part = pl.ds(*span)
        value = product(slot, left_of(region), wid)
        height = value.shape[0]
        got = p_recv[group][unit, part].astype(F32) + y_recv[group][unit, part].astype(F32)
        return value + got.reshape(height, wid)

    def final_qkv(span, base, gains, wait):
        region = (*span, 0, rows)
        for which in range(3):
            wait(which)
            value = final(0, which, span, base + which)
            if which < 2:
                value = norm_heads(value, gains[which][mine].reshape(1, -1))
            else:
                value = value.astype(BF16)
            r.qkv[which, pl.ds(*span)] = shaped(value, region)

    def hid(place, k, span):
        if isinstance(k, int) and k == 0:
            return r.hid0.at[place, pl.ds(*span)]
        return r.hid1.at[place, k - 1, pl.ds(*span)]

    def hid_value(place, k, span):
        part = hid(place, k, span)
        return part[...].reshape(span[1] * rows * piece, part.shape[-1])

    def of(sems, phase, k, c):
        wrap = sems.shape[1]
        if phase:
            return sems.at[c // wrap, c % wrap]
        return sems.at[k, c % wrap]

    def kind(k):
        return 0 if isinstance(k, int) and k == 0 else 1

    def to_across(phase, k, c):
        return remote(
            hid(own_place, k, (c, 1)),
            hid(across_place, k, (c, 1)),
            r.a_send.at[kind(k)],
            of(r.a_recv, phase, k, c),
            {"cols": across},
        )

    def half_to_mate(k, h):
        span = (h * half, half)
        return remote(
            hid(own_place, k, span),
            hid(mate_place, k, span),
            r.b_send.at[kind(k)],
            r.b_recv.at[k, h],
            {"cols": mate},
        )

    def to_mate(c):
        return remote(
            hid(own_place, 0, (c, 1)),
            hid(mate_place, 0, (c, 1)),
            r.b_send.at[0],
            of(r.b_recv, 1, 0, c),
            {"cols": mate},
        )

    def forward(phase, k, c):
        return remote(
            hid(across_place, k, (c, 1)),
            hid(diag_place, k, (c, 1)),
            r.d_send.at[kind(k)],
            of(r.d_recv, phase, k, c),
            {"cols": mate},
        )

    def z_right(c, rel):
        return remote(
            r.z_send.at[c, rel - 1],
            r.z_in.at[c, rel - 1],
            r.z_sent.at[0],
            r.z_arrive.at[c, rel - 1],
            {"rows": row + 1},
        )

    def z_left(c, rel):
        there = (rel + 1) % rows or rows
        return remote(
            r.z_send.at[c, rel - 1],
            r.z_in.at[c, there],
            r.z_sent.at[0],
            r.z_arrive.at[c, there],
            {"rows": row - 1},
        )

    def z_wait(c, place):
        part = r.z_in.at[c, place]
        pltpu.make_async_copy(part, part, r.z_arrive.at[c, place]).wait()

    def sums(c, step):
        def go(rel, move):
            value = accum[c, rel]
            if step > 0:
                z_wait(c, rel)
                value += r.z_in[c, rel].astype(F32)
            r.z_send[c, rel - 1] = value.astype(BF16)
            move(c, rel).start()

        @pl.when(row == step)
        def _():
            for block in range(rows - 1, step, -1):
                go(block - step, z_right)

        here = rows - 1 - step

        @pl.when(row == here)
        def _():
            for block in range(here):
                go(block - here + rows, z_left)

    def sums_end(c):
        @pl.when(row > 0)
        def _():
            z_wait(c, 0)
            accum[c, 0] += r.z_in[c, 0].astype(F32)

        @pl.when(row < rows - 1)
        def _():
            z_wait(c, rows)
            accum[c, 0] += r.z_in[c, rows].astype(F32)

    others = (mate, across, diagonal)

    def pairs(flat):
        lane = lax.broadcasted_iota(jnp.int32, (flat.shape[0], HEAD_DIM), 1)
        return jnp.where(
            lane < HEAD_DIM // 2,
            jnp.sum(flat, 1, keepdims=True),
            jnp.sum(flat * flat, 1, keepdims=True),
        )

    def normal(values, mean, square, gain):
        var = square / width - mean * mean
        return ((values - mean) * lax.rsqrt(var + EPS) * gain[...].reshape(1, -1)).astype(BF16)

    def swap(c, slot):
        i = c % half
        return remote(
            r.moments.at[3, c],
            r.moments.at[slot, c],
            r.m_send.at[i, slot],
            r.m_recv.at[i, slot],
            {"cols": others[slot]},
        )

    def norm_start(c):
        sums_end(c)
        total = accum[c, 0] + r.tokens[c].astype(F32) + r.down_bias[...].reshape(1, -1)
        layer = total.astype(BF16)
        r.layer[c] = layer
        r.moments[3, c] = pairs(layer.astype(F32))
        for slot in range(3):
            swap(c, slot).start()

    def norm_end(c):
        for slot in range(3):
            swap(c, slot).wait()
        m = r.moments
        total = (m[3, c] + m[0, c]) + (m[1, c] + m[2, c])
        at = HEAD_DIM // 2
        normed[c, 0] = normal(
            r.layer[c].astype(F32), total[:, :1] / width, total[:, at : at + 1], r.join_gain
        )
        for place in range(rows):

            @pl.when(row == place)
            def _():
                for there in range(rows):
                    if abs(there - place) == 1 or (abs(there - place) == 2 and place in (0, rows - 1)):
                        cast(c, place, there, place)

    def cast(c, place, there, block):
        rel, away = (block - place) % rows, (block - there) % rows
        remote(
            normed.at[c, rel],
            normed.at[c, away],
            r.g_send.at[2],
            r.g_arrive.at[c, away],
            {"rows": there},
        ).start()

    def landed(c, rel):
        part = normed.at[c, rel]
        pltpu.make_async_copy(part, part, r.g_arrive.at[c, rel]).wait()

    def relay(c):
        for place, there, blocks in ((1, 0, (2, 3)), (2, 3, (1, 0))):

            @pl.when(row == place)
            def _():
                for block in blocks:
                    landed(c, (block - place) % rows)
                    cast(c, place, there, block)

    def gathered(c):
        for place in range(rows):

            @pl.when(row == place)
            def _():
                for block in (((1, 2, 3), (0,), (3,), (2, 1, 0))[place]):
                    landed(c, (block - place) % rows)

    load_camera_in(diagonal, 0)
    load_camera_in(across, n_in)
    load_camera_in(mate, ring)
    greet(3)
    own = r.tokens[...].reshape(chunks * piece, depth).astype(F32)
    few = r.start.shape[1]
    begin = HEAD_DIM // 2 - few // 2
    r.start[3] = jnp.transpose(pairs(own))[begin : begin + few]
    swaps = [
        remote(
            r.start.at[3],
            r.start.at[slot],
            r.m_send.at[half, slot],
            r.m_recv.at[half, slot],
            {"cols": others[slot]},
        )
        for slot in range(3)
    ]
    for move in swaps:
        move.start()
    for move in swaps:
        move.wait()
    total = (r.start[3] + r.start[0]) + (r.start[1] + r.start[2])
    total = jnp.transpose(jnp.concatenate([total] * (HEAD_DIM // few), 0))
    normed[:, 0] = normal(
        own, total[:, :1] / width, total[:, few // 2 : few // 2 + 1], r.gain
    ).reshape(chunks, piece, depth)
    first_half, second_half = (0, half), (half, half)
    each(half, spread)
    region = (0, chunks, 0, 1)
    rest = [(h * half, half, 1, rows - 1) for h in range(2)]

    def takes(h, away):
        each(half, lambda i: take(h * half + i, away))

    for group in range(2):
        give(region, 0, group, 0, True)
        send(region, 0, group, n_in, True)
    takes(0, 1)
    takes(0, 2)
    each(half, lambda i: spread(half + i))
    takes(0, 3)
    for group in range(2):
        give(rest[0], 1, group, 0, False)
        send(rest[0], 1, group, n_in, False)
        if group == 0:
            takes(1, 1)
    takes(1, 2)
    for group in range(2):
        give_second(first_half, 0, group, ring, True)
    takes(1, 3)
    for group in range(2):
        give(rest[1], 2, group, 0, False)
        send(rest[1], 2, group, n_in, False)
    load_camera_out(col, 0)
    load_camera_out(mate, n_out)
    load_camera_out(across, 2 * n_out)
    for group in range(2):
        give_second(second_half, 1, group, ring, False)
    load_camera_in(col, ring)
    spread_done()

    def finals(h):
        span = (h * half, half)

        def arrived(group, unit):
            @pl.when(h == 0)
            def _():
                wait_in(ring + offsets[group] + unit, wides[group])
                y_copy(group, unit, 0, region).wait_recv()

            p_copy(group, unit, h, span).wait_recv()
            y_copy(group, unit, 1 + h, (*span[:1], half, 1, rows - 1)).wait_recv()

        final_qkv(span, ring, (r.q_gain, r.k_gain), lambda which: arrived(0, which))

        def camera(rel):
            for start in range(0, wide, HEAD_DIM):
                head = pl.ds(start, HEAD_DIM)
                q, k, v = (
                    r.qkv[which, pl.ds(*span), rel, :, head].reshape(half * piece, HEAD_DIM)
                    for which in range(3)
                )
                r.hid0[own_place, pl.ds(*span), rel, :, head] = soft_blend(q, k, v).reshape(
                    half, piece, HEAD_DIM
                )

        each(rows, camera)
        half_to_mate(0, h).start()

        def activate(unit):
            arrived(1, unit)
            raw = final(1, unit, span, ring + 3 + unit) + r.bias[col * ups + unit]
            value = (raw * (1.0 + lax.erf(raw * math.sqrt(0.5))) * 0.5).astype(BF16)
            r.hid1[own_place, unit, pl.ds(*span)] = shaped(value, (*span, 0, rows))
            half_to_mate(unit + 1, h).start()

        each(ups, activate)

        @pl.when(h == 0)
        def _():
            def ship(c):
                to_across(0, 0, c).start()
                each(ups, lambda unit: to_across(0, unit + 1, c).start())

            each(half, ship)

        def fresh_out(slot, deep):
            @pl.when(h == 0)
            def _():
                wait_out(slot, deep)

        def near_up(place):
            def one(unit):
                slot = place * n_out + 1 + unit
                fresh_out(slot, tile)
                if place == mate_place:
                    half_to_mate(unit + 1, h).wait_recv()
                add_tile(span, hid_value(place, unit + 1, span), slot)

            return one

        fresh_out(0, wide)
        add_tile(span, hid_value(own_place, 0, span), 0, True)
        each(ups, near_up(own_place))
        fresh_out(n_out, wide)
        half_to_mate(0, h).wait_recv()
        add_tile(span, hid_value(mate_place, 0, span), n_out)
        each(ups, near_up(mate_place))

    each(2, finals)
    load_camera_out(diagonal, ring)
    load_join_in(diagonal, 0)
    load_join_in(across, 3)
    join_out_slots = (2 * n_out - 2, 2 * n_out - 1, ring + n_out, ring + n_out + 1)
    for place in range(4):
        load_out(r.w_join, join_out_slots[place], owners[place] * wide, wide)
    for group in range(2):
        all_sent(f_send[group], r.ys.at[group])
        all_sent(p_send[group], r.ps.at[group])

    def far(c, k):
        ahead = k + AHEAD
        later = c + ahead // n_out

        @pl.when((later >= half) & (later < chunks))
        def _():
            to_across(0, ahead % n_out, later).start()

        to_across(0, k, c).wait_recv()
        forward(0, k, c).start()

        @pl.when(c == 0)
        def _():
            wait_out(2 * n_out + k, wide if k == 0 else tile)

        add_tile((c, 1), hid_value(across_place, k, (c, 1)), 2 * n_out + k)

    def farther(c, k):
        @pl.when(c == 0)
        def _():
            wait_out(ring + k, wide if k == 0 else tile)

        forward(0, k, c).wait_recv()
        add_tile((c, 1), hid_value(diag_place, k, (c, 1)), ring + k)

    def steps(c, pause=lambda k: None):
        def before(back, action):
            if isinstance(c, int):
                action(c - back)
                return

            @pl.when(c >= back)
            def _():
                action(c - back)

        for k in range(n_out):
            far(c, k)
            if k > 0:
                farther(c, k - 1)
            if k == 0:
                before(3, norm_start)
                before(4, norm_end)
                before(5, relay)
            if k == 1:
                before(2, lambda b: sums(b, 2))
            if k == 2:
                before(1, lambda b: sums(b, 1))
            pause(k)
        farther(c, n_out - 1)
        sums(c, 0)

    queue = []
    spans = ((0, 2), (2, 2), (4, 2), (6, 1), (7, 1))
    second_spans = ((0, 4), (4, 2), (6, 1), (7, 1))
    final_spans = (((0, 4), (0,), (0, 1)), ((4, 2), (1,), (2,)), ((6, 2), (2, 3), (3, 4)))

    def whole(span):
        return (*span, 0, rows)

    def ready(i):
        for c in range(spans[i][0], sum(spans[i])):
            gathered(c)
        give(whole(spans[i]), i, 0, 0, i == 0)
        send(whole(spans[i]), i, 0, 3, i == 0, False)
        for unit in range(3):
            for c in range(spans[i][0], sum(spans[i])):
                queue.append((unit, i, whole((c, 1))))

    def issue(count):
        for _ in range(count):
            if queue:
                unit, i, part = queue.pop(0)
                y_copy(0, unit, i, part).start()

    def join_second(i):
        give_second(second_spans[i], i, 0, 2 * n_out, i == 0)

    def join_final(i):
        span, p_stages, y_stages = final_spans[i]

        def arrived(which):
            if i == 0:
                wait_in(ring + which, wide)
            for stage in p_stages:
                p_copy(0, which, stage, second_spans[stage]).wait_recv()
            for stage in y_stages:
                y_copy(0, which, stage, whole(spans[stage])).wait_recv()

        final_qkv(span, ring, (r.jq_gain, r.jk_gain), arrived)

    each(last, steps)
    ready(0)
    steps(last, lambda k: issue(1 if k else 0))
    load_join_in(mate, 2 * n_out)
    load_join_in(col, ring)
    norm_end(4)
    norm_start(5)
    issue(1)
    relay(3)
    sums(6, 2)
    issue(1)
    sums(7, 1)
    norm_end(5)
    issue(1)
    relay(4)
    norm_start(6)
    ready(1)
    issue(1)
    sums(7, 2)
    issue(1)
    relay(5)
    norm_end(6)
    issue(1)
    join_second(0)
    issue(1)
    norm_start(7)
    issue(2)
    ready(2)
    relay(6)
    norm_end(7)
    issue(2)
    join_final(0)
    issue(2)
    join_second(1)
    issue(2)
    ready(3)
    issue(len(queue))
    relay(7)
    join_second(2)
    all_sent(r.z_send, r.z_sent.at[0])
    for which, buffer in enumerate((r.hid0, r.hid1)):
        all_sent(buffer.at[own_place], r.a_send.at[which])
        all_sent(buffer.at[own_place], r.b_send.at[which])
        all_sent(buffer.at[own_place], r.d_send.at[which])
    ready(4)
    issue(len(queue))
    join_second(3)
    join_final(1)
    join_final(2)

    def blend(c):
        for start in range(0, wide, HEAD_DIM):
            head = pl.ds(start, HEAD_DIM)
            q = r.qkv[0, c, :, :, head].reshape(rows * piece, HEAD_DIM)
            k, v = (
                r.qkv[which, :, :, :, head].reshape(chunks * rows * piece, HEAD_DIM)
                for which in (1, 2)
            )
            r.hid0[own_place, c, :, :, head] = soft_blend(q, k, v).reshape(rows, piece, HEAD_DIM)
        to_across(1, 0, c).start()
        to_mate(c).start()

    def hand_on(c):
        to_across(1, 0, c).wait_recv()
        forward(1, 0, c).start()

    def result_of(c):
        sums_end(c)
        r.result[c] = (accum[c, 0] + r.layer[c].astype(F32)).astype(BF16)

    blend(0)
    blend(1)
    for slot in join_out_slots:
        wait_out(slot, wide)
    hand_on(0)

    def join_steps(c):
        def before(back, action):
            @pl.when(c >= back)
            def _():
                action(c - back)

        def add(place, start=False):
            add_tile((c, 1), hid_value(place, 0, (c, 1)), join_out_slots[place], start)

        add(own_place, True)
        to_mate(c).wait_recv()
        add(mate_place)
        add(across_place)
        forward(1, 0, c).wait_recv()
        add(diag_place)
        sums(c, 0)

        @pl.when(c + 2 < chunks)
        def _():
            blend(c + 2)

        before(1, lambda b: sums(b, 1))

        @pl.when(c + 1 < chunks)
        def _():
            hand_on(c + 1)

        before(2, lambda b: sums(b, 2))
        before(3, result_of)

    each(chunks, join_steps)
    sums(last - 1, 2)
    sums(last, 1)
    result_of(last - 2)
    sums(last, 2)
    result_of(last - 1)
    result_of(last)

    all_sent(r.z_send, r.z_sent.at[0])
    all_sent(r.hid0.at[own_place], r.a_send.at[0])
    all_sent(r.hid0.at[own_place], r.b_send.at[0])
    all_sent(r.hid0.at[own_place], r.d_send.at[0])
    all_sent(f_send[0], r.ys.at[0])
    all_sent(p_send[0], r.ps.at[0])
    inner = (row > 0) & (row < rows - 1)

    @pl.when(inner)
    def _():
        all_sent(normed, r.g_send.at[2])

    @pl.when(jnp.logical_not(inner))
    def _():
        all_sent(normed.at[:, pl.ds(0, 2)], r.g_send.at[2])


AHEAD = 5
CHUNKS = 8


def tile_of(depth, columns, cols):
    ups = 3
    tile = columns // cols // ups
    return ups, tile


def kernel_body(
    camera_tokens,
    norm_gain,
    query_weight,
    key_weight,
    value_weight,
    query_gain,
    key_gain,
    out_weight,
    up_weight,
    up_bias,
    down_weight,
    down_bias,
    join_gain,
    join_query,
    join_key,
    join_value,
    join_query_gain,
    join_key_gain,
    join_out,
):
    own_rows, depth = camera_tokens.shape
    rows, cols = lax.axis_size("rows"), lax.axis_size("cols")
    width = out_weight.shape[1]
    wide = query_weight.shape[1] // cols
    ups, tile = tile_of(depth, up_weight.shape[1], cols)
    chunks, piece = CHUNKS, own_rows // CHUNKS
    n_in, n_out = 3 + ups, 1 + ups
    slot_pieces = max(depth, width) // tile

    def blocked(weight):
        return weight.reshape(depth // tile, tile, weight.shape[1])

    any_spec, vmem_spec = pl.BlockSpec(memory_space=pl.ANY), pl.BlockSpec(memory_space=pltpu.VMEM)
    inputs = {
        "tokens": (camera_tokens.reshape(chunks, piece, depth), vmem_spec),
        "gain": (norm_gain, vmem_spec),
        "q_gain": (query_gain, vmem_spec),
        "k_gain": (key_gain, vmem_spec),
        "bias": (up_bias.reshape(cols * ups, 1, tile), vmem_spec),
        "down_bias": (down_bias, vmem_spec),
        "join_gain": (join_gain, vmem_spec),
        "jq_gain": (join_query_gain, vmem_spec),
        "jk_gain": (join_key_gain, vmem_spec),
        "wq": (blocked(query_weight), any_spec),
        "wk": (blocked(key_weight), any_spec),
        "wv": (blocked(value_weight), any_spec),
        "w_up": (blocked(up_weight), any_spec),
        "w_out": (out_weight, any_spec),
        "w_down": (down_weight, any_spec),
        "jq": (blocked(join_query), any_spec),
        "jk": (blocked(join_key), any_spec),
        "jv": (blocked(join_value), any_spec),
        "w_join": (join_out, any_spec),
    }
    dma, vmem = pltpu.SemaphoreType.DMA, pltpu.VMEM
    scratch = {
        "pool": vmem((3 * n_in * slot_pieces, tile, tile), BF16),
        "pool_sem": dma((3 * n_in,)),
        "normed": vmem((chunks, rows, piece, depth), BF16),
        "start": vmem((4, 16, HEAD_DIM), F32),
        "moments": vmem((4, chunks, piece, HEAD_DIM), F32),
        "m_send": dma((chunks // 2 + 1, 3)),
        "m_recv": dma((chunks // 2 + 1, 3)),
        "g_send": dma((3,)),
        "g_arrive": dma((chunks, rows)),
        "qkv": vmem((3, chunks, rows, piece, wide), BF16),
        "hid0": vmem((4, chunks, rows, piece, wide), BF16),
        "hid1": vmem((4, ups, chunks, rows, piece, tile), BF16),
        "accum": vmem((chunks, rows, piece, width), F32),
        "z_send": vmem((chunks, rows - 1, piece, width), BF16),
        "z_in": vmem((chunks, rows + 1, piece, width), BF16),
        "z_sent": dma((1,)),
        "z_arrive": dma((chunks, rows + 1)),
        "layer": vmem((chunks, piece, width), BF16),
        "a_recv": dma((n_out, chunks)),
        "b_recv": dma((n_out, 2)),
        "d_recv": dma((n_out, 2)),
        "ys": dma((2,)),
        "ps": dma((2,)),
    }
    for name in ("a_send", "b_send", "d_send"):
        scratch[name] = dma((2,))
    for group, (count, wid) in enumerate(((3, wide), (ups, tile))):
        for name in ("f_send", "f_recv", "y_recv", "p_send", "p_recv"):
            scratch[name + str(group)] = vmem((count, chunks, rows, piece, wid), BF16)
        scratch["fs" + str(group)] = dma((count,))
        for name in ("fr", "yr", "pr"):
            scratch[name + str(group)] = dma((count, 3 if group else 5))
    names = (*inputs, "result", *scratch)
    joined = pl.pallas_call(
        functools.partial(layer_kernel, names, float(depth * cols)),
        name="layer",
        out_shape=jax.ShapeDtypeStruct((chunks, piece, width), BF16),
        in_specs=[spec for _, spec in inputs.values()],
        out_specs=vmem_spec,
        scratch_shapes=list(scratch.values()),
        compiler_params=pltpu.CompilerParams(
            collective_id=0, has_side_effects=True, vmem_limit_bytes=VMEM_LIMIT
        ),
    )(*[value for value, _ in inputs.values()])
    return joined.reshape(own_rows, width)


def fits(mesh):
    cols, rows = mesh.shape["cols"], mesh.shape["rows"]
    return cols == 4 and rows == 4 and D % (rows * cols * HEAD_DIM) == 0


def body(*arrays):
    tokens, up_weight = arrays[0], arrays[8]
    own_rows, depth = tokens.shape
    ups, tile = tile_of(depth, up_weight.shape[1], lax.axis_size("cols"))
    wide = arrays[2].shape[1] // lax.axis_size("cols")
    good = (
        own_rows == 2 * TOK_CAM
        and own_rows == HEAD_DIM
        and tile * ups * lax.axis_size("cols") == up_weight.shape[1]
        and tile % HEAD_DIM == 0
        and depth % tile == 0
        and arrays[7].shape[1] == depth
        and wide <= tile
        and wide % HEAD_DIM == 0
    )
    return kernel_body(*arrays) if good else plain_body(*arrays)


def solution(mesh):
    in_specs = (
        P(("groups", "rows"), "cols"),
        P("cols"),
        P("cols", "rows"),
        P("cols", "rows"),
        P("cols", "rows"),
        P("rows"),
        P("rows"),
        P("rows", "cols"),
        P("cols", "rows"),
        P("rows"),
        P("rows", "cols"),
        P("cols"),
        P("cols"),
        P("cols", "rows"),
        P("cols", "rows"),
        P("cols", "rows"),
        P("rows"),
        P("rows"),
        P("rows", "cols"),
    )
    out_specs = P(("groups", "rows"), "cols")
    inner = body if fits(mesh) else plain_body
    return jax.shard_map(inner, mesh=mesh, in_specs=in_specs, out_specs=out_specs, check_vma=False)
```

```python
import functools
import math
import types

import jax
import jax.numpy as jnp
from jax import lax
from jax.experimental import pallas as pl
from jax.experimental.pallas import tpu as pltpu
from jax.sharding import PartitionSpec as P

HEAD_DIM = 128
TOK_CAM = 64
D = 6144


EPS = 1e-06


def partner_2(array, axis, bit):
    return lax.ppermute(array, axis, [(i, i ^ 1 << bit) for i in range(lax.axis_size(axis))])


def normalize(values, scales, moments):
    row_mean = moments[0] / D
    row_var = moments[1] / D - row_mean * row_mean
    return ((values - row_mean[:, None]) * lax.rsqrt(row_var[:, None] + EPS) * scales).astype(
        jnp.bfloat16
    )


def shard_moments(values):
    return lax.psum((jnp.sum(values, 1), jnp.sum(values * values, 1)), "cols")


def head_norm(values, scales):
    row_count = values.shape[0]
    grouped = values.reshape(row_count, -1, HEAD_DIM)
    row_mean = jnp.mean(grouped, -1, keepdims=True)
    row_var = jnp.mean(grouped * grouped, -1, keepdims=True) - row_mean * row_mean
    normed = (grouped - row_mean) * lax.rsqrt(row_var + EPS)
    return (normed.reshape(row_count, -1) * scales).astype(jnp.bfloat16)


def attend(queries, key_rows, val_rows):
    inv_root = 1.0 / math.sqrt(HEAD_DIM)
    scores = (
        jnp.einsum("bqhd,bkhd->bhqk", queries, key_rows, preferred_element_type=jnp.float32)
        * inv_root
    )
    row_max = jnp.max(scores, -1, keepdims=True)
    weights = jnp.exp(scores - row_max)
    row_sum = jnp.sum(weights, -1)
    blended = jnp.einsum(
        "bhqk,bkhd->bqhd",
        weights.astype(jnp.bfloat16),
        val_rows,
        preferred_element_type=jnp.float32,
    )
    return blended / jnp.transpose(row_sum, (0, 2, 1))[..., None]


def to_heads(matrix, blocks):
    return matrix.reshape(blocks, -1, matrix.shape[1] // HEAD_DIM, HEAD_DIM)


def camera_attention(queries, key_rows, val_rows):
    local_rows = queries.shape[0]
    if local_rows >= TOK_CAM:
        blocks = local_rows // TOK_CAM
        result = attend(
            to_heads(queries, blocks), to_heads(key_rows, blocks), to_heads(val_rows, blocks)
        )
    else:
        cam_span = TOK_CAM // local_rows
        position = lax.axis_index("cols")
        key_value = jnp.stack((key_rows, val_rows))
        for which_bit in range(cam_span.bit_length() - 1):
            partner = partner_2(key_value, "cols", which_bit)
            is_lower = position >> which_bit & 1 == 0
            key_value = jnp.where(
                is_lower,
                jnp.concatenate((key_value, partner), 1),
                jnp.concatenate((partner, key_value), 1),
            )
        result = attend(to_heads(queries, 1), to_heads(key_value[0], 1), to_heads(key_value[1], 1))
    return result.reshape(local_rows, -1).astype(jnp.bfloat16)


def plain_body(
    camera_tokens,
    norm_gain,
    query_weight,
    key_weight,
    value_weight,
    query_gain,
    key_gain,
    out_weight,
    up_weight,
    up_bias,
    down_weight,
    down_bias,
    join_gain,
    join_query,
    join_key,
    join_value,
    join_query_gain,
    join_key_gain,
    join_out,
):
    own_rows = camera_tokens.shape[0]
    all_rows = own_rows * lax.axis_size("rows")
    col_rows = all_rows // lax.axis_size("cols")
    attn_width = query_weight.shape[1]
    start_f32 = camera_tokens.astype(jnp.float32)
    normed_all = lax.all_gather(
        normalize(start_f32, norm_gain, shard_moments(start_f32)), "rows", axis=0, tiled=True
    )
    joint_weight = jnp.concatenate((query_weight, key_weight, value_weight, up_weight), 1)
    joint = lax.psum_scatter(
        jnp.dot(normed_all, joint_weight, preferred_element_type=jnp.float32),
        "cols",
        scatter_dimension=0,
        tiled=True,
    )
    up_sum = joint[:, 3 * attn_width :]
    hidden = jax.nn.gelu(up_sum + up_bias, approximate=False).astype(jnp.bfloat16)
    attended = camera_attention(
        head_norm(joint[:, :attn_width], query_gain),
        head_norm(joint[:, attn_width : 2 * attn_width], key_gain),
        joint[:, 2 * attn_width : 3 * attn_width].astype(jnp.bfloat16),
    )
    attn_all, hidden_all = (
        lax.all_gather(attended, "cols", axis=0, tiled=True),
        lax.all_gather(hidden, "cols", axis=0, tiled=True),
    )
    mixed = lax.psum_scatter(
        jnp.dot(attn_all, out_weight, preferred_element_type=jnp.float32)
        + jnp.dot(hidden_all, down_weight, preferred_element_type=jnp.float32),
        "rows",
        scatter_dimension=0,
        tiled=True,
    )
    layer_own = (start_f32 + mixed + down_bias).astype(jnp.bfloat16)
    layer_f32 = layer_own.astype(jnp.float32)
    join_in = lax.all_gather(
        normalize(layer_f32, join_gain, shard_moments(layer_f32)), "rows", axis=0, tiled=True
    )
    join_weight = jnp.concatenate((join_query, join_key, join_value), 1)
    join_joint = lax.psum_scatter(
        jnp.dot(join_in, join_weight, preferred_element_type=jnp.float32),
        "cols",
        scatter_dimension=0,
        tiled=True,
    )
    join_q = head_norm(join_joint[:, :attn_width], join_query_gain)
    join_k = head_norm(join_joint[:, attn_width : 2 * attn_width], join_key_gain)
    join_v = join_joint[:, 2 * attn_width :].astype(jnp.bfloat16)
    heads_here = attn_width // HEAD_DIM
    query_heads = join_q.reshape(col_rows, heads_here, HEAD_DIM)
    inv_root = 1.0 / math.sqrt(HEAD_DIM)
    run_max = jnp.full((heads_here, col_rows), -jnp.inf, jnp.float32)
    run_sum = jnp.zeros((heads_here, col_rows), jnp.float32)
    accum = jnp.zeros((col_rows, heads_here, HEAD_DIM), jnp.float32)
    key_part = lax.all_gather(join_k, "cols", axis=0, tiled=True)
    val_part = lax.all_gather(join_v, "cols", axis=0, tiled=True)
    row_count = key_part.shape[0]
    key_heads = key_part.reshape(row_count, heads_here, HEAD_DIM)
    val_heads = val_part.reshape(row_count, heads_here, HEAD_DIM)
    scores = (
        jnp.einsum("qhd,khd->hqk", query_heads, key_heads, preferred_element_type=jnp.float32)
        * inv_root
    )
    new_max = jnp.max(scores, -1)
    factor = jnp.exp(run_max - new_max)
    weights = jnp.exp(scores - new_max[..., None])
    run_sum = run_sum * factor + jnp.sum(weights, -1)
    accum = accum * jnp.transpose(factor)[..., None] + jnp.einsum(
        "hqk,khd->qhd", weights.astype(jnp.bfloat16), val_heads, preferred_element_type=jnp.float32
    )
    run_max, run_sum, accum = (new_max, run_sum, accum)
    joined_attn = (
        (accum / jnp.transpose(run_sum)[..., None])
        .reshape(col_rows, attn_width)
        .astype(jnp.bfloat16)
    )
    joined_all = lax.all_gather(joined_attn, "cols", axis=0, tiled=True)
    result = lax.psum_scatter(
        jnp.dot(joined_all, join_out, preferred_element_type=jnp.float32),
        "rows",
        scatter_dimension=0,
        tiled=True,
    )
    return (layer_own.astype(jnp.float32) + result).astype(jnp.bfloat16)


F32 = jnp.float32
BF16 = jnp.bfloat16
MESH = pl.DeviceIdType.MESH
VMEM_LIMIT = 66 * 1024 * 1024 - 3 * 1024 * 1024


def each(count, step):
    lax.fori_loop(0, count, lambda i, carry: (step(i), carry)[1], None)


def remote(src, dst, send, recv, device):
    return pltpu.make_async_remote_copy(
        src_ref=src,
        dst_ref=dst,
        send_sem=send,
        recv_sem=recv,
        device_id=device,
        device_id_type=MESH,
    )


def places():
    col = lax.axis_index("cols")
    core = lax.rem(col, 2)
    return col, col + 1 - 2 * core, lax.rem(col + 2, 4)


def greet(cols_away):
    col, row, row_count = lax.axis_index("cols"), lax.axis_index("rows"), lax.axis_size("rows")
    barrier = pltpu.get_barrier_semaphore()
    _, mate, across = places()
    others = {1: mate, 2: across}
    if cols_away == 3:
        others[3] = mate + across - col
    for other in others.values():
        pl.semaphore_signal(barrier, inc=1, device_id={"cols": other}, device_id_type=MESH)

    @pl.when(row > 0)
    def _():
        pl.semaphore_signal(barrier, inc=1, device_id={"rows": row - 1}, device_id_type=MESH)

    @pl.when(row < row_count - 1)
    def _():
        pl.semaphore_signal(barrier, inc=1, device_id={"rows": row + 1}, device_id_type=MESH)

    inner = (row > 0) & (row < row_count - 1)

    @pl.when(inner)
    def _():
        pl.semaphore_wait(barrier, len(others) + 2)

    @pl.when(jnp.logical_not(inner))
    def _():
        pl.semaphore_wait(barrier, len(others) + 1)


def norm_heads(values, scales):
    parts = []
    for start in range(0, values.shape[1], HEAD_DIM):
        part = values[:, start : start + HEAD_DIM]
        mean = jnp.mean(part, -1, keepdims=True)
        var = jnp.mean(part * part, -1, keepdims=True) - mean * mean
        parts.append((part - mean) * lax.rsqrt(var + EPS))
    return (jnp.concatenate(parts, 1) * scales).astype(BF16)


def soft_blend(query, keys, values):
    scores = lax.dot_general(
        query, keys, (((1,), (1,)), ((), ())), preferred_element_type=F32
    ) * (1.0 / math.sqrt(HEAD_DIM))
    weights = jnp.exp(scores - jnp.max(scores, -1, keepdims=True))
    total = jnp.sum(weights, -1, keepdims=True)
    blended = jnp.dot(weights.astype(BF16), values, preferred_element_type=F32)
    return (blended / total).astype(BF16)


def layer_kernel(names, width, *refs):
    r = types.SimpleNamespace(**dict(zip(names, refs)))
    normed, accum, pool, pool_sem = r.normed, r.accum, r.pool, r.pool_sem
    col, mate, across = places()
    diagonal = mate + across - col
    owners = (col, mate, across, diagonal)
    row, rows = lax.axis_index("rows"), lax.axis_size("rows")
    chunks, _, piece, depth = normed.shape
    half = chunks // 2
    ups = r.f_send1.shape[0]
    tile = pool.shape[1]
    wide = r.hid0.shape[-1]
    out_pieces = accum.shape[-1] // tile
    in_pieces = depth // tile
    slot_pieces = max(in_pieces, out_pieces)
    n_in, n_out = 3 + ups, 1 + ups
    last = chunks - 1
    ring = 2 * n_in
    mine = pl.ds(pl.multiple_of(col * wide, HEAD_DIM), wide)
    own_place, mate_place, across_place, diag_place = range(4)

    def load_in(source, slot, start, wid):
        first = slot * slot_pieces
        return pltpu.make_async_copy(
            source.at[:, :, pl.ds(pl.multiple_of(start, HEAD_DIM), wid)],
            pool.at[pl.ds(first, in_pieces), :, pl.ds(0, wid)],
            pool_sem.at[slot],
        )

    def load_out(source, slot, start, deep):
        for j in range(out_pieces):
            pltpu.make_async_copy(
                source.at[pl.ds(pl.multiple_of(start, HEAD_DIM), deep), pl.ds(j * tile, tile)],
                pool.at[slot * slot_pieces + j, pl.ds(0, deep)],
                pool_sem.at[slot],
            ).start()

    def load_camera_in(owner, slot):
        for which, source in enumerate((r.wq, r.wk, r.wv)):
            load_in(source, slot + which, owner * wide, wide).start()
        each(
            ups,
            lambda unit: load_in(
                r.w_up, slot + 3 + unit, owner * (ups * tile) + unit * tile, tile
            ).start(),
        )

    def load_join_in(owner, slot):
        for which, source in enumerate((r.jq, r.jk, r.jv)):
            load_in(source, slot + which, owner * wide, wide).start()

    def load_camera_out(owner, slot):
        load_out(r.w_out, slot, owner * wide, wide)
        each(ups, lambda unit: load_out(r.w_down, slot + 1 + unit, (owner * ups + unit) * tile, tile))

    def in_weight(slot, wid):
        return pool.at[pl.ds(slot * slot_pieces, in_pieces), :, pl.ds(0, wid)]

    def wait_in(slot, wid):
        part = in_weight(slot, wid)
        pltpu.make_async_copy(part, part, pool_sem.at[slot]).wait()

    def wait_out(slot, deep):
        part = pool.at[pl.ds(slot * slot_pieces, out_pieces), pl.ds(0, deep)]
        pltpu.make_async_copy(part, part, pool_sem.at[slot]).wait()

    def product(slot, left, wid):
        weight = in_weight(slot, wid)[...].reshape(depth, wid)
        return jnp.dot(left, weight, preferred_element_type=F32)

    def add_tile(span, value, slot, begin=False):
        start, count = span
        deep = value.shape[1]
        for j in range(out_pieces):
            part = jnp.dot(
                value, pool[slot * slot_pieces + j, pl.ds(0, deep)], preferred_element_type=F32
            ).reshape(count, rows, piece, tile)
            at = (pl.ds(start, count), slice(None), slice(None), slice(j * tile, (j + 1) * tile))
            if begin:
                accum[at] = part
            else:
                accum[at] += part

    def gather_copy(c, block, right):
        rel = lax.rem(block - row + rows, rows)
        away = lax.rem(rel + (rows - 1 if right else 1), rows)
        return remote(
            normed.at[c, rel],
            normed.at[c, away],
            r.g_send.at[int(right)],
            r.g_arrive.at[c, block],
            {"rows": row + 1 if right else row - 1},
        )

    def arrival(c, block):
        part = normed.at[c, lax.rem(block - row + rows, rows)]
        pltpu.make_async_copy(part, part, r.g_arrive.at[c, block]).wait()

    def pass_on(c, block, right):
        @pl.when((row < rows - 1) if right else (row > 0))
        def _():
            gather_copy(c, block, right).start()

    def spread(c):
        pass_on(c, row, True)
        pass_on(c, row, False)

    def take(c, away):
        @pl.when(row >= away)
        def _():
            arrival(c, row - away)
            pass_on(c, row - away, True)

        @pl.when(row + away < rows)
        def _():
            arrival(c, row + away)
            pass_on(c, row + away, False)

    def spread_done():
        for place in range(rows):

            @pl.when(row == place)
            def _():
                if place < rows - 1:
                    all_sent(normed.at[:, pl.ds(0, place + 1)], r.g_send.at[1])
                if place > 0:
                    all_sent(normed.at[:, pl.ds(0, rows - place)], r.g_send.at[0])

    f_send, f_recv, y_recv = (r.f_send0, r.f_send1), (r.f_recv0, r.f_recv1), (r.y_recv0, r.y_recv1)
    p_send, p_recv = (r.p_send0, r.p_send1), (r.p_recv0, r.p_recv1)
    first_sems = ((r.fs0, r.fr0, r.yr0), (r.fs1, r.fr1, r.yr1))
    second_recv = (r.pr0, r.pr1)
    counts, wides, offsets = (3, ups), (wide, tile), (0, 3)

    def left_of(region):
        c0, nc, r0, nr = region
        return normed[pl.ds(c0, nc), pl.ds(r0, nr)].reshape(nc * nr * piece, depth)

    def part_of(region):
        c0, nc, r0, nr = region
        return pl.ds(c0, nc), pl.ds(r0, nr)

    def shaped(value, region):
        return value.reshape(region[1], region[3], piece, value.shape[-1])

    def f_copy(group, unit, stage, region):
        at = (unit, *part_of(region))
        fs, fr, _ = first_sems[group]
        return remote(
            f_send[group].at[at], f_recv[group].at[at], fs.at[unit], fr.at[unit, stage], {"cols": mate}
        )

    def y_copy(group, unit, stage, region):
        at = (unit, *part_of(region))
        yr = first_sems[group][2]
        return remote(
            f_send[group].at[at],
            y_recv[group].at[at],
            r.ys.at[group],
            yr.at[unit, stage],
            {"cols": across},
        )

    def p_copy(group, unit, stage, span):
        at = (unit, pl.ds(*span))
        return remote(
            p_send[group].at[at],
            p_recv[group].at[at],
            r.ps.at[group],
            second_recv[group].at[unit, stage],
            {"cols": mate},
        )

    def all_sent(source, sem):
        pltpu.make_async_copy(source, source, sem).wait()

    def give(region, stage, group, base, fresh):
        wid = wides[group]

        def step(unit):
            slot = base + offsets[group] + unit
            if fresh:
                wait_in(slot, wid)
            value = product(slot, left_of(region), wid).astype(BF16)
            f_send[group][(unit, *part_of(region))] = shaped(value, region)
            f_copy(group, unit, stage, region).start()

        each(counts[group], step)

    def send(region, stage, group, base, fresh, start=True):
        wid = wides[group]

        def step(unit):
            slot = base + offsets[group] + unit
            if fresh:
                wait_in(slot, wid)
            value = shaped(product(slot, left_of(region), wid), region)
            at = (unit, *part_of(region))
            f_copy(group, unit, stage, region).wait()
            f_send[group][at] = (value + f_recv[group][at].astype(F32)).astype(BF16)
            if start:
                y_copy(group, unit, stage, region).start()

        each(counts[group], step)

    def give_second(span, stage, group, base, fresh):
        wid = wides[group]
        region = (*span, 0, rows)

        def step(unit):
            slot = base + offsets[group] + unit
            if fresh:
                wait_in(slot, wid)
            value = product(slot, left_of(region), wid).astype(BF16)
            p_send[group][unit, pl.ds(*span)] = shaped(value, region)
            p_copy(group, unit, stage, span).start()

        each(counts[group], step)

    def final(group, unit, span, slot):
        region = (*span, 0, rows)
        wid = wides[group]
        part = pl.ds(*span)
        value = product(slot, left_of(region), wid)
        height = value.shape[0]
        got = p_recv[group][unit, part].astype(F32) + y_recv[group][unit, part].astype(F32)
        return value + got.reshape(height, wid)

    def final_qkv(span, base, gains, wait):
        region = (*span, 0, rows)
        for which in range(3):
            wait(which)
            value = final(0, which, span, base + which)
            if which < 2:
                value = norm_heads(value, gains[which][mine].reshape(1, -1))
            else:
                value = value.astype(BF16)
            r.qkv[which, pl.ds(*span)] = shaped(value, region)

    def hid(place, k, span):
        if isinstance(k, int) and k == 0:
            return r.hid0.at[place, pl.ds(*span)]
        return r.hid1.at[place, k - 1, pl.ds(*span)]

    def hid_value(place, k, span):
        part = hid(place, k, span)
        return part[...].reshape(span[1] * rows * piece, part.shape[-1])

    def of(sems, phase, k, c):
        wrap = sems.shape[1]
        if phase:
            return sems.at[c // wrap, c % wrap]
        return sems.at[k, c % wrap]

    def kind(k):
        return 0 if isinstance(k, int) and k == 0 else 1

    def to_across(phase, k, c):
        return remote(
            hid(own_place, k, (c, 1)),
            hid(across_place, k, (c, 1)),
            r.a_send.at[kind(k)],
            of(r.a_recv, phase, k, c),
            {"cols": across},
        )

    def half_to_mate(k, h):
        span = (h * half, half)
        return remote(
            hid(own_place, k, span),
            hid(mate_place, k, span),
            r.b_send.at[kind(k)],
            r.b_recv.at[k, h],
            {"cols": mate},
        )

    def to_mate(c):
        return remote(
            hid(own_place, 0, (c, 1)),
            hid(mate_place, 0, (c, 1)),
            r.b_send.at[0],
            of(r.b_recv, 1, 0, c),
            {"cols": mate},
        )

    def forward(phase, k, c):
        return remote(
            hid(across_place, k, (c, 1)),
            hid(diag_place, k, (c, 1)),
            r.d_send.at[kind(k)],
            of(r.d_recv, phase, k, c),
            {"cols": mate},
        )

    def z_wait(c, place):
        part = r.z_in.at[c, place]
        pltpu.make_async_copy(part, part, r.z_arrive.at[c, place]).wait()

    def sums(c, step):
        for place, moves in enumerate(SUM_MOVES[step]):

            @pl.when(row == place)
            def _():
                for block, there in moves:
                    rel = (block - place) % rows
                    value = accum[c, rel]
                    if step > 0:
                        z_wait(c, rel)
                        value += r.z_in[c, rel].astype(F32)
                    r.z_send[c, rel - 1] = value.astype(BF16)
                    slot = (block - there) % rows
                    if step == 0 and slot == 0:
                        slot = rows
                    remote(
                        r.z_send.at[c, rel - 1],
                        r.z_in.at[c, slot],
                        r.z_sent.at[0],
                        r.z_arrive.at[c, slot],
                        {"rows": there},
                    ).start()

    def sums_end(c):
        z_wait(c, rows)
        z_wait(c, 0)
        accum[c, 0] += r.z_in[c, rows].astype(F32) + r.z_in[c, 0].astype(F32)

    others = (mate, across, diagonal)

    def pairs(flat):
        lane = lax.broadcasted_iota(jnp.int32, (flat.shape[0], HEAD_DIM), 1)
        return jnp.where(
            lane < HEAD_DIM // 2,
            jnp.sum(flat, 1, keepdims=True),
            jnp.sum(flat * flat, 1, keepdims=True),
        )

    def normal(values, mean, square, gain):
        var = square / width - mean * mean
        return ((values - mean) * lax.rsqrt(var + EPS) * gain[...].reshape(1, -1)).astype(BF16)

    def swap(c, slot):
        i = c % half
        return remote(
            r.moments.at[3, c],
            r.moments.at[slot, c],
            r.m_send.at[i, slot],
            r.m_recv.at[i, slot],
            {"cols": others[slot]},
        )

    def norm_start(c):
        sums_end(c)
        total = accum[c, 0] + r.tokens[c].astype(F32) + r.down_bias[...].reshape(1, -1)
        layer = total.astype(BF16)
        r.layer[c] = layer
        r.moments[3, c] = pairs(layer.astype(F32))
        for slot in range(3):
            swap(c, slot).start()

    def norm_end(c):
        for slot in range(3):
            swap(c, slot).wait()
        m = r.moments
        total = (m[3, c] + m[0, c]) + (m[1, c] + m[2, c])
        at = HEAD_DIM // 2
        normed[c, 0] = normal(
            r.layer[c].astype(F32), total[:, :1] / width, total[:, at : at + 1], r.join_gain
        )
        for place in range(rows):

            @pl.when(row == place)
            def _():
                for there in range(rows):
                    if abs(there - place) == 1 or (abs(there - place) == 2 and place in (0, rows - 1)):
                        cast(c, place, there, place)

    def cast(c, place, there, block):
        rel, away = (block - place) % rows, (block - there) % rows
        remote(
            normed.at[c, rel],
            normed.at[c, away],
            r.g_send.at[2],
            r.g_arrive.at[c, away],
            {"rows": there},
        ).start()

    def landed(c, rel):
        part = normed.at[c, rel]
        pltpu.make_async_copy(part, part, r.g_arrive.at[c, rel]).wait()

    def relay(c):
        for place, there, blocks in ((1, 0, (2, 3)), (2, 3, (1, 0))):

            @pl.when(row == place)
            def _():
                for block in blocks:
                    landed(c, (block - place) % rows)
                    cast(c, place, there, block)

    def gathered(c):
        for place in range(rows):

            @pl.when(row == place)
            def _():
                for block in (((1, 2, 3), (0,), (3,), (2, 1, 0))[place]):
                    landed(c, (block - place) % rows)

    load_camera_in(diagonal, 0)
    load_camera_in(across, n_in)
    load_camera_in(mate, ring)
    own = r.tokens[...].reshape(chunks * piece, depth).astype(F32)
    few = r.start.shape[1]
    begin = HEAD_DIM // 2 - few // 2
    r.start[3] = jnp.transpose(pairs(own))[begin : begin + few]
    greet(3)
    swaps = [
        remote(
            r.start.at[3],
            r.start.at[slot],
            r.m_send.at[half, slot],
            r.m_recv.at[half, slot],
            {"cols": others[slot]},
        )
        for slot in range(3)
    ]
    for move in swaps:
        move.start()
    for move in swaps:
        move.wait()
    total = (r.start[3] + r.start[0]) + (r.start[1] + r.start[2])
    total = jnp.transpose(jnp.concatenate([total] * (HEAD_DIM // few), 0))
    normed[:, 0] = normal(
        own, total[:, :1] / width, total[:, few // 2 : few // 2 + 1], r.gain
    ).reshape(chunks, piece, depth)
    first_half, second_half = (0, half), (half, half)
    each(half, spread)
    region = (0, chunks, 0, 1)
    rest = [(h * half, half, 1, rows - 1) for h in range(2)]

    def takes(h, away):
        each(half, lambda i: take(h * half + i, away))

    for group in range(2):
        give(region, 0, group, 0, True)
        send(region, 0, group, n_in, True)
    takes(0, 1)
    takes(0, 2)
    each(half, lambda i: spread(half + i))
    takes(0, 3)
    for group in range(2):
        give(rest[0], 1, group, 0, False)
        send(rest[0], 1, group, n_in, False)
        if group == 0:
            takes(1, 1)
    takes(1, 2)
    for group in range(2):
        give_second(first_half, 0, group, ring, True)
    takes(1, 3)
    for group in range(2):
        give(rest[1], 2, group, 0, False)
        send(rest[1], 2, group, n_in, False)
    load_camera_out(col, 0)
    load_camera_out(mate, n_out)
    load_camera_out(across, 2 * n_out)
    for group in range(2):
        give_second(second_half, 1, group, ring, False)
    load_camera_in(col, ring)
    spread_done()

    def finals(h):
        span = (h * half, half)

        def arrived(group, unit):
            @pl.when(h == 0)
            def _():
                wait_in(ring + offsets[group] + unit, wides[group])
                y_copy(group, unit, 0, region).wait_recv()

            p_copy(group, unit, h, span).wait_recv()
            y_copy(group, unit, 1 + h, (*span[:1], half, 1, rows - 1)).wait_recv()

        final_qkv(span, ring, (r.q_gain, r.k_gain), lambda which: arrived(0, which))

        def camera(rel):
            for start in range(0, wide, HEAD_DIM):
                head = pl.ds(start, HEAD_DIM)
                q, k, v = (
                    r.qkv[which, pl.ds(*span), rel, :, head].reshape(half * piece, HEAD_DIM)
                    for which in range(3)
                )
                r.hid0[own_place, pl.ds(*span), rel, :, head] = soft_blend(q, k, v).reshape(
                    half, piece, HEAD_DIM
                )

        each(rows, camera)
        half_to_mate(0, h).start()

        def activate(unit):
            arrived(1, unit)
            raw = final(1, unit, span, ring + 3 + unit) + r.bias[col * ups + unit]
            value = (raw * (1.0 + lax.erf(raw * math.sqrt(0.5))) * 0.5).astype(BF16)
            r.hid1[own_place, unit, pl.ds(*span)] = shaped(value, (*span, 0, rows))
            half_to_mate(unit + 1, h).start()

        each(ups, activate)

        @pl.when(h == 0)
        def _():
            def ship(c):
                to_across(0, 0, c).start()
                each(ups, lambda unit: to_across(0, unit + 1, c).start())

            each(half, ship)

        def fresh_out(slot, deep):
            @pl.when(h == 0)
            def _():
                wait_out(slot, deep)

        def near_up(place):
            def one(unit):
                slot = place * n_out + 1 + unit
                fresh_out(slot, tile)
                if place == mate_place:
                    half_to_mate(unit + 1, h).wait_recv()
                add_tile(span, hid_value(place, unit + 1, span), slot)

            return one

        fresh_out(0, wide)
        add_tile(span, hid_value(own_place, 0, span), 0, True)
        each(ups, near_up(own_place))
        fresh_out(n_out, wide)
        half_to_mate(0, h).wait_recv()
        add_tile(span, hid_value(mate_place, 0, span), n_out)
        each(ups, near_up(mate_place))

    each(2, finals)
    load_camera_out(diagonal, ring)
    load_join_in(diagonal, 0)
    load_join_in(across, 3)
    join_out_slots = (2 * n_out - 2, 2 * n_out - 1, ring + n_out, ring + n_out + 1)
    for place in range(4):
        load_out(r.w_join, join_out_slots[place], owners[place] * wide, wide)
    for group in range(2):
        all_sent(f_send[group], r.ys.at[group])
        all_sent(p_send[group], r.ps.at[group])

    def far(c, k):
        ahead = k + AHEAD
        later = c + ahead // n_out

        @pl.when((later >= half) & (later < chunks))
        def _():
            to_across(0, ahead % n_out, later).start()

        to_across(0, k, c).wait_recv()
        forward(0, k, c).start()

        @pl.when(c == 0)
        def _():
            wait_out(2 * n_out + k, wide if k == 0 else tile)

        add_tile((c, 1), hid_value(across_place, k, (c, 1)), 2 * n_out + k)

    def farther(c, k):
        @pl.when(c == 0)
        def _():
            wait_out(ring + k, wide if k == 0 else tile)

        forward(0, k, c).wait_recv()
        add_tile((c, 1), hid_value(diag_place, k, (c, 1)), ring + k)

    def steps(c, pause=lambda k: None):
        def before(back, action):
            if isinstance(c, int):
                action(c - back)
                return

            @pl.when(c >= back)
            def _():
                action(c - back)

        for k in range(n_out):
            far(c, k)
            if k > 0:
                farther(c, k - 1)
            if k == 1:
                before(2, norm_start)
            if k == 1:
                before(3, norm_end)
            if k == 1:
                before(4, relay)
            if k == 2:
                before(1, lambda b: sums(b, 1))
            pause(k)
        farther(c, n_out - 1)
        sums(c, 0)

    queue = []
    spans = ((0, 2), (2, 2), (4, 2), (6, 1), (7, 1))
    second_spans = ((0, 4), (4, 2), (6, 2))
    final_spans = (((0, 4), (0,), (0, 1)), ((4, 2), (1,), (2,)), ((6, 2), (2,), (3, 4)))

    def whole(span):
        return (*span, 0, rows)

    def ready(i):
        for c in range(spans[i][0], sum(spans[i])):
            gathered(c)
        give(whole(spans[i]), i, 0, 0, i == 0)
        send(whole(spans[i]), i, 0, 3, i == 0, False)
        for unit in range(3):
            for c in range(spans[i][0], sum(spans[i])):
                queue.append((unit, i, whole((c, 1))))

    def issue(count):
        for _ in range(count):
            if queue:
                unit, i, part = queue.pop(0)
                y_copy(0, unit, i, part).start()

    def join_second(i):
        give_second(second_spans[i], i, 0, 2 * n_out, i == 0)

    def join_final(i):
        span, p_stages, y_stages = final_spans[i]

        def arrived(which):
            if i == 0:
                wait_in(ring + which, wide)
            for stage in p_stages:
                p_copy(0, which, stage, second_spans[stage]).wait_recv()
            for stage in y_stages:
                y_copy(0, which, stage, whole(spans[stage])).wait_recv()

        final_qkv(span, ring, (r.jq_gain, r.jk_gain), arrived)

    each(last, steps)
    ready(0)
    steps(last, lambda k: issue(1 if k else 0))
    load_join_in(mate, 2 * n_out)
    load_join_in(col, ring)
    issue(1)
    norm_end(5)
    sums(7, 1)
    norm_start(6)
    issue(2)
    relay(4)
    relay(5)
    ready(1)
    norm_end(6)
    norm_start(7)
    issue(3)
    join_second(0)
    relay(6)
    issue(1)
    norm_end(7)
    issue(2)
    ready(2)
    issue(4)
    join_second(1)
    relay(7)
    ready(3)
    issue(len(queue))
    all_sent(r.z_send, r.z_sent.at[0])
    for which, buffer in enumerate((r.hid0, r.hid1)):
        all_sent(buffer.at[own_place], r.a_send.at[which])
        all_sent(buffer.at[own_place], r.b_send.at[which])
        all_sent(buffer.at[own_place], r.d_send.at[which])
    ready(4)
    issue(len(queue))
    join_second(2)
    join_final(0)
    join_final(1)
    join_final(2)

    def blend(c):
        for start in range(0, wide, HEAD_DIM):
            head = pl.ds(start, HEAD_DIM)
            q = r.qkv[0, c, :, :, head].reshape(rows * piece, HEAD_DIM)
            k, v = (
                r.qkv[which, :, :, :, head].reshape(chunks * rows * piece, HEAD_DIM)
                for which in (1, 2)
            )
            r.hid0[own_place, c, :, :, head] = soft_blend(q, k, v).reshape(rows, piece, HEAD_DIM)
        to_across(1, 0, c).start()
        to_mate(c).start()

    def hand_on(c):
        to_across(1, 0, c).wait_recv()
        forward(1, 0, c).start()

    def result_of(c):
        sums_end(c)
        r.result[c] = (accum[c, 0] + r.layer[c].astype(F32)).astype(BF16)

    blend(0)
    blend(1)
    for slot in join_out_slots:
        wait_out(slot, wide)

    def join_steps(c):
        def before(back, action):
            @pl.when(c >= back)
            def _():
                action(c - back)

        def add(place, start=False):
            add_tile((c, 1), hid_value(place, 0, (c, 1)), join_out_slots[place], start)

        add(own_place, True)
        to_mate(c).wait_recv()
        add(mate_place)

        @pl.when(c == 0)
        def _():
            hand_on(c)

        add(across_place)
        forward(1, 0, c).wait_recv()
        add(diag_place)
        sums(c, 0)

        @pl.when(c + 2 < chunks)
        def _():
            blend(c + 2)

        before(1, lambda b: sums(b, 1))

        @pl.when(c + 1 < chunks)
        def _():
            hand_on(c + 1)

        before(3, result_of)

    each(chunks, join_steps)
    sums(last, 1)
    result_of(last - 2)
    result_of(last - 1)
    result_of(last)

    all_sent(r.z_send, r.z_sent.at[0])
    all_sent(r.hid0.at[own_place], r.a_send.at[0])
    all_sent(r.hid0.at[own_place], r.b_send.at[0])
    all_sent(r.hid0.at[own_place], r.d_send.at[0])
    all_sent(f_send[0], r.ys.at[0])
    all_sent(p_send[0], r.ps.at[0])
    inner = (row > 0) & (row < rows - 1)

    @pl.when(inner)
    def _():
        all_sent(normed, r.g_send.at[2])

    @pl.when(jnp.logical_not(inner))
    def _():
        all_sent(normed.at[:, pl.ds(0, 2)], r.g_send.at[2])


AHEAD = 4
SUM_MOVES = (
    (((3, 1), (2, 1), (1, 1)), ((0, 0),), ((3, 3),), ((0, 2), (1, 2), (2, 2))),
    ((), ((3, 3), (2, 2)), ((0, 0), (1, 1)), ()),
)
CHUNKS = 8


def tile_of(depth, columns, cols):
    ups = 3
    tile = columns // cols // ups
    return ups, tile


def kernel_body(
    camera_tokens,
    norm_gain,
    query_weight,
    key_weight,
    value_weight,
    query_gain,
    key_gain,
    out_weight,
    up_weight,
    up_bias,
    down_weight,
    down_bias,
    join_gain,
    join_query,
    join_key,
    join_value,
    join_query_gain,
    join_key_gain,
    join_out,
):
    own_rows, depth = camera_tokens.shape
    rows, cols = lax.axis_size("rows"), lax.axis_size("cols")
    width = out_weight.shape[1]
    wide = query_weight.shape[1] // cols
    ups, tile = tile_of(depth, up_weight.shape[1], cols)
    chunks, piece = CHUNKS, own_rows // CHUNKS
    n_in, n_out = 3 + ups, 1 + ups
    slot_pieces = max(depth, width) // tile

    def blocked(weight):
        return weight.reshape(depth // tile, tile, weight.shape[1])

    any_spec, vmem_spec = pl.BlockSpec(memory_space=pl.ANY), pl.BlockSpec(memory_space=pltpu.VMEM)
    inputs = {
        "tokens": (camera_tokens.reshape(chunks, piece, depth), vmem_spec),
        "gain": (norm_gain, vmem_spec),
        "q_gain": (query_gain, vmem_spec),
        "k_gain": (key_gain, vmem_spec),
        "bias": (up_bias.reshape(cols * ups, 1, tile), vmem_spec),
        "down_bias": (down_bias, vmem_spec),
        "join_gain": (join_gain, vmem_spec),
        "jq_gain": (join_query_gain, vmem_spec),
        "jk_gain": (join_key_gain, vmem_spec),
        "wq": (blocked(query_weight), any_spec),
        "wk": (blocked(key_weight), any_spec),
        "wv": (blocked(value_weight), any_spec),
        "w_up": (blocked(up_weight), any_spec),
        "w_out": (out_weight, any_spec),
        "w_down": (down_weight, any_spec),
        "jq": (blocked(join_query), any_spec),
        "jk": (blocked(join_key), any_spec),
        "jv": (blocked(join_value), any_spec),
        "w_join": (join_out, any_spec),
    }
    dma, vmem = pltpu.SemaphoreType.DMA, pltpu.VMEM
    scratch = {
        "pool": vmem((3 * n_in * slot_pieces, tile, tile), BF16),
        "pool_sem": dma((3 * n_in,)),
        "normed": vmem((chunks, rows, piece, depth), BF16),
        "start": vmem((4, 16, HEAD_DIM), F32),
        "moments": vmem((4, chunks, piece, HEAD_DIM), F32),
        "m_send": dma((chunks // 2 + 1, 3)),
        "m_recv": dma((chunks // 2 + 1, 3)),
        "g_send": dma((3,)),
        "g_arrive": dma((chunks, rows)),
        "qkv": vmem((3, chunks, rows, piece, wide), BF16),
        "hid0": vmem((4, chunks, rows, piece, wide), BF16),
        "hid1": vmem((4, ups, chunks, rows, piece, tile), BF16),
        "accum": vmem((chunks, rows, piece, width), F32),
        "z_send": vmem((chunks, rows - 1, piece, width), BF16),
        "z_in": vmem((chunks, rows + 1, piece, width), BF16),
        "z_sent": dma((1,)),
        "z_arrive": dma((chunks, rows + 1)),
        "layer": vmem((chunks, piece, width), BF16),
        "a_recv": dma((n_out, chunks)),
        "b_recv": dma((n_out, 2)),
        "d_recv": dma((n_out, 2)),
        "ys": dma((2,)),
        "ps": dma((2,)),
    }
    for name in ("a_send", "b_send", "d_send"):
        scratch[name] = dma((2,))
    for group, (count, wid) in enumerate(((3, wide), (ups, tile))):
        for name in ("f_send", "f_recv", "y_recv", "p_send", "p_recv"):
            scratch[name + str(group)] = vmem((count, chunks, rows, piece, wid), BF16)
        scratch["fs" + str(group)] = dma((count,))
        for name in ("fr", "yr", "pr"):
            scratch[name + str(group)] = dma((count, 3 if group else 5))
    names = (*inputs, "result", *scratch)
    joined = pl.pallas_call(
        functools.partial(layer_kernel, names, float(depth * cols)),
        name="layer",
        out_shape=jax.ShapeDtypeStruct((chunks, piece, width), BF16),
        in_specs=[spec for _, spec in inputs.values()],
        out_specs=vmem_spec,
        scratch_shapes=list(scratch.values()),
        compiler_params=pltpu.CompilerParams(
            collective_id=0, has_side_effects=True, vmem_limit_bytes=VMEM_LIMIT
        ),
    )(*[value for value, _ in inputs.values()])
    return joined.reshape(own_rows, width)


def fits(mesh):
    cols, rows = mesh.shape["cols"], mesh.shape["rows"]
    return cols == 4 and rows == 4 and D % (rows * cols * HEAD_DIM) == 0


def body(*arrays):
    tokens, up_weight = arrays[0], arrays[8]
    own_rows, depth = tokens.shape
    ups, tile = tile_of(depth, up_weight.shape[1], lax.axis_size("cols"))
    wide = arrays[2].shape[1] // lax.axis_size("cols")
    good = (
        own_rows == 2 * TOK_CAM
        and own_rows == HEAD_DIM
        and tile * ups * lax.axis_size("cols") == up_weight.shape[1]
        and tile % HEAD_DIM == 0
        and depth % tile == 0
        and arrays[7].shape[1] == depth
        and wide <= tile
        and wide % HEAD_DIM == 0
    )
    return kernel_body(*arrays) if good else plain_body(*arrays)


def solution(mesh):
    in_specs = (
        P(("groups", "rows"), "cols"),
        P("cols"),
        P("cols", "rows"),
        P("cols", "rows"),
        P("cols", "rows"),
        P("rows"),
        P("rows"),
        P("rows", "cols"),
        P("cols", "rows"),
        P("rows"),
        P("rows", "cols"),
        P("cols"),
        P("cols"),
        P("cols", "rows"),
        P("cols", "rows"),
        P("cols", "rows"),
        P("rows"),
        P("rows"),
        P("rows", "cols"),
    )
    out_specs = P(("groups", "rows"), "cols")
    inner = body if fits(mesh) else plain_body
    return jax.shard_map(inner, mesh=mesh, in_specs=in_specs, out_specs=out_specs, check_vma=False)
```

```python
import functools
import math
import types

import jax
import jax.numpy as jnp
from jax import lax
from jax.experimental import pallas as pl
from jax.experimental.pallas import tpu as pltpu
from jax.sharding import PartitionSpec as P

HEAD_DIM = 128
TOK_CAM = 64
D = 6144


EPS = 1e-06


def partner_2(array, axis, bit):
    return lax.ppermute(array, axis, [(i, i ^ 1 << bit) for i in range(lax.axis_size(axis))])


def normalize(values, scales, moments):
    row_mean = moments[0] / D
    row_var = moments[1] / D - row_mean * row_mean
    return ((values - row_mean[:, None]) * lax.rsqrt(row_var[:, None] + EPS) * scales).astype(
        jnp.bfloat16
    )


def shard_moments(values):
    return lax.psum((jnp.sum(values, 1), jnp.sum(values * values, 1)), "cols")


def head_norm(values, scales):
    row_count = values.shape[0]
    grouped = values.reshape(row_count, -1, HEAD_DIM)
    row_mean = jnp.mean(grouped, -1, keepdims=True)
    row_var = jnp.mean(grouped * grouped, -1, keepdims=True) - row_mean * row_mean
    normed = (grouped - row_mean) * lax.rsqrt(row_var + EPS)
    return (normed.reshape(row_count, -1) * scales).astype(jnp.bfloat16)


def attend(queries, key_rows, val_rows):
    inv_root = 1.0 / math.sqrt(HEAD_DIM)
    scores = (
        jnp.einsum("bqhd,bkhd->bhqk", queries, key_rows, preferred_element_type=jnp.float32)
        * inv_root
    )
    row_max = jnp.max(scores, -1, keepdims=True)
    weights = jnp.exp(scores - row_max)
    row_sum = jnp.sum(weights, -1)
    blended = jnp.einsum(
        "bhqk,bkhd->bqhd",
        weights.astype(jnp.bfloat16),
        val_rows,
        preferred_element_type=jnp.float32,
    )
    return blended / jnp.transpose(row_sum, (0, 2, 1))[..., None]


def to_heads(matrix, blocks):
    return matrix.reshape(blocks, -1, matrix.shape[1] // HEAD_DIM, HEAD_DIM)


def camera_attention(queries, key_rows, val_rows):
    local_rows = queries.shape[0]
    if local_rows >= TOK_CAM:
        blocks = local_rows // TOK_CAM
        result = attend(
            to_heads(queries, blocks), to_heads(key_rows, blocks), to_heads(val_rows, blocks)
        )
    else:
        cam_span = TOK_CAM // local_rows
        position = lax.axis_index("cols")
        key_value = jnp.stack((key_rows, val_rows))
        for which_bit in range(cam_span.bit_length() - 1):
            partner = partner_2(key_value, "cols", which_bit)
            is_lower = position >> which_bit & 1 == 0
            key_value = jnp.where(
                is_lower,
                jnp.concatenate((key_value, partner), 1),
                jnp.concatenate((partner, key_value), 1),
            )
        result = attend(to_heads(queries, 1), to_heads(key_value[0], 1), to_heads(key_value[1], 1))
    return result.reshape(local_rows, -1).astype(jnp.bfloat16)


def plain_body(
    camera_tokens,
    norm_gain,
    query_weight,
    key_weight,
    value_weight,
    query_gain,
    key_gain,
    out_weight,
    up_weight,
    up_bias,
    down_weight,
    down_bias,
    join_gain,
    join_query,
    join_key,
    join_value,
    join_query_gain,
    join_key_gain,
    join_out,
):
    own_rows = camera_tokens.shape[0]
    all_rows = own_rows * lax.axis_size("rows")
    col_rows = all_rows // lax.axis_size("cols")
    attn_width = query_weight.shape[1]
    start_f32 = camera_tokens.astype(jnp.float32)
    normed_all = lax.all_gather(
        normalize(start_f32, norm_gain, shard_moments(start_f32)), "rows", axis=0, tiled=True
    )
    joint_weight = jnp.concatenate((query_weight, key_weight, value_weight, up_weight), 1)
    joint = lax.psum_scatter(
        jnp.dot(normed_all, joint_weight, preferred_element_type=jnp.float32),
        "cols",
        scatter_dimension=0,
        tiled=True,
    )
    up_sum = joint[:, 3 * attn_width :]
    hidden = jax.nn.gelu(up_sum + up_bias, approximate=False).astype(jnp.bfloat16)
    attended = camera_attention(
        head_norm(joint[:, :attn_width], query_gain),
        head_norm(joint[:, attn_width : 2 * attn_width], key_gain),
        joint[:, 2 * attn_width : 3 * attn_width].astype(jnp.bfloat16),
    )
    attn_all, hidden_all = (
        lax.all_gather(attended, "cols", axis=0, tiled=True),
        lax.all_gather(hidden, "cols", axis=0, tiled=True),
    )
    mixed = lax.psum_scatter(
        jnp.dot(attn_all, out_weight, preferred_element_type=jnp.float32)
        + jnp.dot(hidden_all, down_weight, preferred_element_type=jnp.float32),
        "rows",
        scatter_dimension=0,
        tiled=True,
    )
    layer_own = (start_f32 + mixed + down_bias).astype(jnp.bfloat16)
    layer_f32 = layer_own.astype(jnp.float32)
    join_in = lax.all_gather(
        normalize(layer_f32, join_gain, shard_moments(layer_f32)), "rows", axis=0, tiled=True
    )
    join_weight = jnp.concatenate((join_query, join_key, join_value), 1)
    join_joint = lax.psum_scatter(
        jnp.dot(join_in, join_weight, preferred_element_type=jnp.float32),
        "cols",
        scatter_dimension=0,
        tiled=True,
    )
    join_q = head_norm(join_joint[:, :attn_width], join_query_gain)
    join_k = head_norm(join_joint[:, attn_width : 2 * attn_width], join_key_gain)
    join_v = join_joint[:, 2 * attn_width :].astype(jnp.bfloat16)
    heads_here = attn_width // HEAD_DIM
    query_heads = join_q.reshape(col_rows, heads_here, HEAD_DIM)
    inv_root = 1.0 / math.sqrt(HEAD_DIM)
    run_max = jnp.full((heads_here, col_rows), -jnp.inf, jnp.float32)
    run_sum = jnp.zeros((heads_here, col_rows), jnp.float32)
    accum = jnp.zeros((col_rows, heads_here, HEAD_DIM), jnp.float32)
    key_part = lax.all_gather(join_k, "cols", axis=0, tiled=True)
    val_part = lax.all_gather(join_v, "cols", axis=0, tiled=True)
    row_count = key_part.shape[0]
    key_heads = key_part.reshape(row_count, heads_here, HEAD_DIM)
    val_heads = val_part.reshape(row_count, heads_here, HEAD_DIM)
    scores = (
        jnp.einsum("qhd,khd->hqk", query_heads, key_heads, preferred_element_type=jnp.float32)
        * inv_root
    )
    new_max = jnp.max(scores, -1)
    factor = jnp.exp(run_max - new_max)
    weights = jnp.exp(scores - new_max[..., None])
    run_sum = run_sum * factor + jnp.sum(weights, -1)
    accum = accum * jnp.transpose(factor)[..., None] + jnp.einsum(
        "hqk,khd->qhd", weights.astype(jnp.bfloat16), val_heads, preferred_element_type=jnp.float32
    )
    run_max, run_sum, accum = (new_max, run_sum, accum)
    joined_attn = (
        (accum / jnp.transpose(run_sum)[..., None])
        .reshape(col_rows, attn_width)
        .astype(jnp.bfloat16)
    )
    joined_all = lax.all_gather(joined_attn, "cols", axis=0, tiled=True)
    result = lax.psum_scatter(
        jnp.dot(joined_all, join_out, preferred_element_type=jnp.float32),
        "rows",
        scatter_dimension=0,
        tiled=True,
    )
    return (layer_own.astype(jnp.float32) + result).astype(jnp.bfloat16)


F32 = jnp.float32
BF16 = jnp.bfloat16
MESH = pl.DeviceIdType.MESH
VMEM_LIMIT = 66 * 1024 * 1024 - 3 * 1024 * 1024


def each(count, step):
    lax.fori_loop(0, count, lambda i, carry: (step(i), carry)[1], None)


def remote(src, dst, send, recv, device):
    return pltpu.make_async_remote_copy(
        src_ref=src,
        dst_ref=dst,
        send_sem=send,
        recv_sem=recv,
        device_id=device,
        device_id_type=MESH,
    )


def places():
    col = lax.axis_index("cols")
    core = lax.rem(col, 2)
    return col, col + 1 - 2 * core, lax.rem(col + 2, 4)


def greet(cols_away):
    col, row, row_count = lax.axis_index("cols"), lax.axis_index("rows"), lax.axis_size("rows")
    barrier = pltpu.get_barrier_semaphore()
    _, mate, across = places()
    others = {1: mate, 2: across}
    if cols_away == 3:
        others[3] = mate + across - col
    for other in others.values():
        pl.semaphore_signal(barrier, inc=1, device_id={"cols": other}, device_id_type=MESH)

    @pl.when(row > 0)
    def _():
        pl.semaphore_signal(barrier, inc=1, device_id={"rows": row - 1}, device_id_type=MESH)

    @pl.when(row < row_count - 1)
    def _():
        pl.semaphore_signal(barrier, inc=1, device_id={"rows": row + 1}, device_id_type=MESH)

    inner = (row > 0) & (row < row_count - 1)

    @pl.when(inner)
    def _():
        pl.semaphore_wait(barrier, len(others) + 2)

    @pl.when(jnp.logical_not(inner))
    def _():
        pl.semaphore_wait(barrier, len(others) + 1)


def norm_heads(values, scales):
    parts = []
    for start in range(0, values.shape[1], HEAD_DIM):
        part = values[:, start : start + HEAD_DIM]
        mean = jnp.mean(part, -1, keepdims=True)
        var = jnp.mean(part * part, -1, keepdims=True) - mean * mean
        parts.append((part - mean) * lax.rsqrt(var + EPS))
    return (jnp.concatenate(parts, 1) * scales).astype(BF16)


def soft_blend(query, keys, values):
    scores = lax.dot_general(
        query, keys, (((1,), (1,)), ((), ())), preferred_element_type=F32
    ) * (1.0 / math.sqrt(HEAD_DIM))
    weights = jnp.exp(scores - jnp.max(scores, -1, keepdims=True))
    total = jnp.sum(weights, -1, keepdims=True)
    blended = jnp.dot(weights.astype(BF16), values, preferred_element_type=F32)
    return (blended / total).astype(BF16)


def layer_kernel(names, width, *refs):
    r = types.SimpleNamespace(**dict(zip(names, refs)))
    normed, accum, pool, pool_sem = r.normed, r.accum, r.pool, r.pool_sem
    col, mate, across = places()
    diagonal = mate + across - col
    owners = (col, mate, across, diagonal)
    row, rows = lax.axis_index("rows"), lax.axis_size("rows")
    chunks, _, piece, depth = normed.shape
    half = chunks // 2
    ups = r.f_send1.shape[0]
    tile = pool.shape[1]
    wide = r.hid0.shape[-1]
    out_pieces = accum.shape[-1] // tile
    in_pieces = depth // tile
    slot_pieces = max(in_pieces, out_pieces)
    n_in, n_out = 3 + ups, 1 + ups
    last = chunks - 1
    ring = 2 * n_in
    mine = pl.ds(pl.multiple_of(col * wide, HEAD_DIM), wide)
    own_place, mate_place, across_place, diag_place = range(4)

    def load_in(source, slot, start, wid):
        first = slot * slot_pieces
        return pltpu.make_async_copy(
            source.at[:, :, pl.ds(pl.multiple_of(start, HEAD_DIM), wid)],
            pool.at[pl.ds(first, in_pieces), :, pl.ds(0, wid)],
            pool_sem.at[slot],
        )

    def load_out(source, slot, start, deep):
        for j in range(out_pieces):
            pltpu.make_async_copy(
                source.at[pl.ds(pl.multiple_of(start, HEAD_DIM), deep), pl.ds(j * tile, tile)],
                pool.at[slot * slot_pieces + j, pl.ds(0, deep)],
                pool_sem.at[slot],
            ).start()

    def load_camera_in(owner, slot):
        for which, source in enumerate((r.wq, r.wk, r.wv)):
            load_in(source, slot + which, owner * wide, wide).start()
        each(
            ups,
            lambda unit: load_in(
                r.w_up, slot + 3 + unit, owner * (ups * tile) + unit * tile, tile
            ).start(),
        )

    def load_join_in(owner, slot):
        for which, source in enumerate((r.jq, r.jk, r.jv)):
            load_in(source, slot + which, owner * wide, wide).start()

    def load_camera_out(owner, slot):
        load_out(r.w_out, slot, owner * wide, wide)
        each(ups, lambda unit: load_out(r.w_down, slot + 1 + unit, (owner * ups + unit) * tile, tile))

    def in_weight(slot, wid):
        return pool.at[pl.ds(slot * slot_pieces, in_pieces), :, pl.ds(0, wid)]

    def wait_in(slot, wid):
        part = in_weight(slot, wid)
        pltpu.make_async_copy(part, part, pool_sem.at[slot]).wait()

    def wait_out(slot, deep):
        part = pool.at[pl.ds(slot * slot_pieces, out_pieces), pl.ds(0, deep)]
        pltpu.make_async_copy(part, part, pool_sem.at[slot]).wait()

    def product(slot, left, wid):
        weight = in_weight(slot, wid)[...].reshape(depth, wid)
        return jnp.dot(left, weight, preferred_element_type=F32)

    def add_tile(span, value, slot, begin=False):
        start, count = span
        deep = value.shape[1]
        for j in range(out_pieces):
            part = jnp.dot(
                value, pool[slot * slot_pieces + j, pl.ds(0, deep)], preferred_element_type=F32
            ).reshape(count, rows, piece, tile)
            at = (pl.ds(start, count), slice(None), slice(None), slice(j * tile, (j + 1) * tile))
            if begin:
                accum[at] = part
            else:
                accum[at] += part

    def gather_copy(c, block, right):
        rel = lax.rem(block - row + rows, rows)
        away = lax.rem(rel + (rows - 1 if right else 1), rows)
        return remote(
            normed.at[c, rel],
            normed.at[c, away],
            r.g_send.at[int(right)],
            r.g_arrive.at[c, block],
            {"rows": row + 1 if right else row - 1},
        )

    def arrival(c, block):
        part = normed.at[c, lax.rem(block - row + rows, rows)]
        pltpu.make_async_copy(part, part, r.g_arrive.at[c, block]).wait()

    def pass_on(c, block, right):
        @pl.when((row < rows - 1) if right else (row > 0))
        def _():
            gather_copy(c, block, right).start()

    def spread(c):
        pass_on(c, row, True)
        pass_on(c, row, False)

    def take(c, away):
        @pl.when(row >= away)
        def _():
            arrival(c, row - away)
            pass_on(c, row - away, True)

        @pl.when(row + away < rows)
        def _():
            arrival(c, row + away)
            pass_on(c, row + away, False)

    def spread_done():
        for place in range(rows):

            @pl.when(row == place)
            def _():
                if place < rows - 1:
                    all_sent(normed.at[:, pl.ds(0, place + 1)], r.g_send.at[1])
                if place > 0:
                    all_sent(normed.at[:, pl.ds(0, rows - place)], r.g_send.at[0])

    f_send, f_recv, y_recv = (r.f_send0, r.f_send1), (r.f_recv0, r.f_recv1), (r.y_recv0, r.y_recv1)
    p_send, p_recv = (r.p_send0, r.p_send1), (r.p_recv0, r.p_recv1)
    first_sems = ((r.fs0, r.fr0, r.yr0), (r.fs1, r.fr1, r.yr1))
    second_recv = (r.pr0, r.pr1)
    counts, wides, offsets = (3, ups), (wide, tile), (0, 3)

    def left_of(region):
        c0, nc, r0, nr = region
        return normed[pl.ds(c0, nc), pl.ds(r0, nr)].reshape(nc * nr * piece, depth)

    def part_of(region):
        c0, nc, r0, nr = region
        return pl.ds(c0, nc), pl.ds(r0, nr)

    def shaped(value, region):
        return value.reshape(region[1], region[3], piece, value.shape[-1])

    def f_copy(group, unit, stage, region):
        at = (unit, *part_of(region))
        fs, fr, _ = first_sems[group]
        return remote(
            f_send[group].at[at], f_recv[group].at[at], fs.at[unit], fr.at[unit, stage], {"cols": mate}
        )

    def y_copy(group, unit, stage, region):
        at = (unit, *part_of(region))
        yr = first_sems[group][2]
        return remote(
            f_send[group].at[at],
            y_recv[group].at[at],
            r.ys.at[group],
            yr.at[unit, stage],
            {"cols": across},
        )

    def p_copy(group, unit, stage, span):
        at = (unit, pl.ds(*span))
        return remote(
            p_send[group].at[at],
            p_recv[group].at[at],
            r.ps.at[group],
            second_recv[group].at[unit, stage],
            {"cols": mate},
        )

    def all_sent(source, sem):
        pltpu.make_async_copy(source, source, sem).wait()

    def give(region, stage, group, base, fresh):
        wid = wides[group]

        def step(unit):
            slot = base + offsets[group] + unit
            if fresh:
                wait_in(slot, wid)
            value = product(slot, left_of(region), wid).astype(BF16)
            f_send[group][(unit, *part_of(region))] = shaped(value, region)
            f_copy(group, unit, stage, region).start()

        each(counts[group], step)

    def send(region, stage, group, base, fresh, start=True):
        wid = wides[group]

        def step(unit):
            slot = base + offsets[group] + unit
            if fresh:
                wait_in(slot, wid)
            value = shaped(product(slot, left_of(region), wid), region)
            at = (unit, *part_of(region))
            f_copy(group, unit, stage, region).wait()
            f_send[group][at] = (value + f_recv[group][at].astype(F32)).astype(BF16)
            if start:
                y_copy(group, unit, stage, region).start()

        each(counts[group], step)

    def give_second(span, stage, group, base, fresh):
        wid = wides[group]
        region = (*span, 0, rows)

        def step(unit):
            slot = base + offsets[group] + unit
            if fresh:
                wait_in(slot, wid)
            value = product(slot, left_of(region), wid).astype(BF16)
            p_send[group][unit, pl.ds(*span)] = shaped(value, region)
            p_copy(group, unit, stage, span).start()

        each(counts[group], step)

    def final(group, unit, span, slot):
        region = (*span, 0, rows)
        wid = wides[group]
        part = pl.ds(*span)
        value = product(slot, left_of(region), wid)
        height = value.shape[0]
        got = p_recv[group][unit, part].astype(F32) + y_recv[group][unit, part].astype(F32)
        return value + got.reshape(height, wid)

    def final_qkv(span, base, gains, wait):
        region = (*span, 0, rows)
        for which in range(3):
            wait(which)
            value = final(0, which, span, base + which)
            if which < 2:
                value = norm_heads(value, gains[which][mine].reshape(1, -1))
            else:
                value = value.astype(BF16)
            r.qkv[which, pl.ds(*span)] = shaped(value, region)

    def hid(place, k, span):
        if isinstance(k, int) and k == 0:
            return r.hid0.at[place, pl.ds(*span)]
        return r.hid1.at[place, k - 1, pl.ds(*span)]

    def hid_value(place, k, span):
        part = hid(place, k, span)
        return part[...].reshape(span[1] * rows * piece, part.shape[-1])

    def of(sems, phase, k, c):
        wrap = sems.shape[1]
        if phase:
            return sems.at[c // wrap, c % wrap]
        return sems.at[k, c % wrap]

    def kind(k):
        return 0 if isinstance(k, int) and k == 0 else 1

    def to_across(phase, k, c):
        return remote(
            hid(own_place, k, (c, 1)),
            hid(across_place, k, (c, 1)),
            r.a_send.at[kind(k)],
            of(r.a_recv, phase, k, c),
            {"cols": across},
        )

    def half_to_mate(k, h):
        span = (h * half, half)
        return remote(
            hid(own_place, k, span),
            hid(mate_place, k, span),
            r.b_send.at[kind(k)],
            r.b_recv.at[k, h],
            {"cols": mate},
        )

    def to_mate(c):
        return remote(
            hid(own_place, 0, (c, 1)),
            hid(mate_place, 0, (c, 1)),
            r.b_send.at[0],
            of(r.b_recv, 1, 0, c),
            {"cols": mate},
        )

    def forward(phase, k, c):
        return remote(
            hid(across_place, k, (c, 1)),
            hid(diag_place, k, (c, 1)),
            r.d_send.at[kind(k)],
            of(r.d_recv, phase, k, c),
            {"cols": mate},
        )

    def z_wait(c, place):
        part = r.z_in.at[c, place]
        pltpu.make_async_copy(part, part, r.z_arrive.at[c, place]).wait()

    def sums(c, step):
        for place, moves in enumerate(SUM_MOVES[step]):

            @pl.when(row == place)
            def _():
                for block, there in moves:
                    rel = (block - place) % rows
                    value = accum[c, rel]
                    if step > 0:
                        z_wait(c, rel)
                        value += r.z_in[c, rel].astype(F32)
                    r.z_send[c, rel - 1] = value.astype(BF16)
                    slot = (block - there) % rows
                    if step == 0 and slot == 0:
                        slot = rows
                    remote(
                        r.z_send.at[c, rel - 1],
                        r.z_in.at[c, slot],
                        r.z_sent.at[0],
                        r.z_arrive.at[c, slot],
                        {"rows": there},
                    ).start()

    def sums_end(c):
        z_wait(c, rows)
        z_wait(c, 0)
        accum[c, 0] += r.z_in[c, rows].astype(F32) + r.z_in[c, 0].astype(F32)

    others = (mate, across, diagonal)

    def pairs(flat):
        lane = lax.broadcasted_iota(jnp.int32, (flat.shape[0], HEAD_DIM), 1)
        return jnp.where(
            lane < HEAD_DIM // 2,
            jnp.sum(flat, 1, keepdims=True),
            jnp.sum(flat * flat, 1, keepdims=True),
        )

    def normal(values, mean, square, gain):
        var = square / width - mean * mean
        return ((values - mean) * lax.rsqrt(var + EPS) * gain[...].reshape(1, -1)).astype(BF16)

    def swap(c, slot):
        i = c % half
        return remote(
            r.moments.at[3, c],
            r.moments.at[slot, c],
            r.m_send.at[i, slot],
            r.m_recv.at[i, slot],
            {"cols": others[slot]},
        )

    def norm_start(c):
        sums_end(c)
        total = accum[c, 0] + r.tokens[c].astype(F32) + r.down_bias[...].reshape(1, -1)
        layer = total.astype(BF16)
        r.layer[c] = layer
        r.moments[3, c] = pairs(layer.astype(F32))
        for slot in range(3):
            swap(c, slot).start()

    def norm_end(c):
        for slot in range(3):
            swap(c, slot).wait()
        m = r.moments
        total = (m[3, c] + m[0, c]) + (m[1, c] + m[2, c])
        at = HEAD_DIM // 2
        normed[c, 0] = normal(
            r.layer[c].astype(F32), total[:, :1] / width, total[:, at : at + 1], r.join_gain
        )
        for place in range(rows):

            @pl.when(row == place)
            def _():
                for there in range(rows):
                    if abs(there - place) == 1 or (abs(there - place) == 2 and place in (0, rows - 1)):
                        cast(c, place, there, place)

    def cast(c, place, there, block):
        rel, away = (block - place) % rows, (block - there) % rows
        remote(
            normed.at[c, rel],
            normed.at[c, away],
            r.g_send.at[2],
            r.g_arrive.at[c, away],
            {"rows": there},
        ).start()

    def landed(c, rel):
        part = normed.at[c, rel]
        pltpu.make_async_copy(part, part, r.g_arrive.at[c, rel]).wait()

    def relay(c):
        for place, there, blocks in ((1, 0, (2, 3)), (2, 3, (1, 0))):

            @pl.when(row == place)
            def _():
                for block in blocks:
                    landed(c, (block - place) % rows)
                    cast(c, place, there, block)

    def gathered(c):
        for place in range(rows):

            @pl.when(row == place)
            def _():
                for block in (((1, 2, 3), (0,), (3,), (2, 1, 0))[place]):
                    landed(c, (block - place) % rows)

    load_camera_in(diagonal, 0)
    load_camera_in(across, n_in)
    load_camera_in(mate, ring)
    own = r.tokens[...].reshape(chunks * piece, depth).astype(F32)
    few = r.start.shape[1]
    begin = HEAD_DIM // 2 - few // 2
    r.start[3] = jnp.transpose(pairs(own))[begin : begin + few]
    greet(3)
    swaps = [
        remote(
            r.start.at[3],
            r.start.at[slot],
            r.m_send.at[half, slot],
            r.m_recv.at[half, slot],
            {"cols": others[slot]},
        )
        for slot in range(3)
    ]
    for move in swaps:
        move.start()
    for move in swaps:
        move.wait()
    total = (r.start[3] + r.start[0]) + (r.start[1] + r.start[2])
    total = jnp.transpose(jnp.concatenate([total] * (HEAD_DIM // few), 0))
    normed[:, 0] = normal(
        own, total[:, :1] / width, total[:, few // 2 : few // 2 + 1], r.gain
    ).reshape(chunks, piece, depth)
    first_half, second_half = (0, half), (half, half)
    each(half, spread)
    region = (0, chunks, 0, 1)
    rest = [(h * half, half, 1, rows - 1) for h in range(2)]

    def takes(h, away):
        each(half, lambda i: take(h * half + i, away))

    for group in range(2):
        give(region, 0, group, 0, True)
        send(region, 0, group, n_in, True)
    takes(0, 1)
    takes(0, 2)
    each(half, lambda i: spread(half + i))
    takes(0, 3)
    for group in range(2):
        give(rest[0], 1, group, 0, False)
        send(rest[0], 1, group, n_in, False)
        if group == 0:
            takes(1, 1)
    takes(1, 2)
    for group in range(2):
        give_second(first_half, 0, group, ring, True)
    takes(1, 3)
    for group in range(2):
        give(rest[1], 2, group, 0, False)
        send(rest[1], 2, group, n_in, False)
    load_camera_out(col, 0)
    load_camera_out(mate, n_out)
    load_camera_out(across, 2 * n_out)
    for group in range(2):
        give_second(second_half, 1, group, ring, False)
    load_camera_in(col, ring)
    spread_done()

    def finals(h):
        span = (h * half, half)

        def arrived(group, unit):
            @pl.when(h == 0)
            def _():
                wait_in(ring + offsets[group] + unit, wides[group])
                y_copy(group, unit, 0, region).wait_recv()

            p_copy(group, unit, h, span).wait_recv()
            y_copy(group, unit, 1 + h, (*span[:1], half, 1, rows - 1)).wait_recv()

        final_qkv(span, ring, (r.q_gain, r.k_gain), lambda which: arrived(0, which))

        def camera(rel):
            for start in range(0, wide, HEAD_DIM):
                head = pl.ds(start, HEAD_DIM)
                q, k, v = (
                    r.qkv[which, pl.ds(*span), rel, :, head].reshape(half * piece, HEAD_DIM)
                    for which in range(3)
                )
                r.hid0[own_place, pl.ds(*span), rel, :, head] = soft_blend(q, k, v).reshape(
                    half, piece, HEAD_DIM
                )

        each(rows, camera)
        half_to_mate(0, h).start()

        def activate(unit):
            arrived(1, unit)
            raw = final(1, unit, span, ring + 3 + unit) + r.bias[col * ups + unit]
            value = (raw * (1.0 + lax.erf(raw * math.sqrt(0.5))) * 0.5).astype(BF16)
            r.hid1[own_place, unit, pl.ds(*span)] = shaped(value, (*span, 0, rows))
            half_to_mate(unit + 1, h).start()

        each(ups, activate)

        @pl.when(h == 0)
        def _():
            def ship(c):
                to_across(0, 0, c).start()
                each(ups, lambda unit: to_across(0, unit + 1, c).start())

            each(half, ship)

        def fresh_out(slot, deep):
            @pl.when(h == 0)
            def _():
                wait_out(slot, deep)

        def near_up(place):
            def one(unit):
                slot = place * n_out + 1 + unit
                fresh_out(slot, tile)
                if place == mate_place:
                    half_to_mate(unit + 1, h).wait_recv()
                add_tile(span, hid_value(place, unit + 1, span), slot)

            return one

        fresh_out(0, wide)
        add_tile(span, hid_value(own_place, 0, span), 0, True)
        each(ups, near_up(own_place))
        fresh_out(n_out, wide)
        half_to_mate(0, h).wait_recv()
        add_tile(span, hid_value(mate_place, 0, span), n_out)
        each(ups, near_up(mate_place))

    each(2, finals)
    load_camera_out(diagonal, ring)
    load_join_in(diagonal, 0)
    load_join_in(across, 3)
    join_out_slots = (2 * n_out - 2, 2 * n_out - 1, ring + n_out, ring + n_out + 1)
    for place in range(4):
        load_out(r.w_join, join_out_slots[place], owners[place] * wide, wide)
    for group in range(2):
        all_sent(f_send[group], r.ys.at[group])
        all_sent(p_send[group], r.ps.at[group])

    def far(c, k):
        ahead = k + AHEAD
        later = c + ahead // n_out

        @pl.when((later >= half) & (later < chunks))
        def _():
            to_across(0, ahead % n_out, later).start()

        to_across(0, k, c).wait_recv()
        forward(0, k, c).start()

        @pl.when(c == 0)
        def _():
            wait_out(2 * n_out + k, wide if k == 0 else tile)

        add_tile((c, 1), hid_value(across_place, k, (c, 1)), 2 * n_out + k)

    def farther(c, k):
        @pl.when(c == 0)
        def _():
            wait_out(ring + k, wide if k == 0 else tile)

        forward(0, k, c).wait_recv()
        add_tile((c, 1), hid_value(diag_place, k, (c, 1)), ring + k)

    def steps(c, pause=lambda k: None):
        def before(back, action):
            if isinstance(c, int):
                action(c - back)
                return

            @pl.when(c >= back)
            def _():
                action(c - back)

        for k in range(n_out):
            far(c, k)
            if k > 0:
                farther(c, k - 1)
            if k == 1:
                before(2, norm_start)
            if k == 1:
                before(3, norm_end)
            if k == 1:
                before(4, relay)
            if k == 2:
                before(1, lambda b: sums(b, 1))
            pause(k)
        farther(c, n_out - 1)
        sums(c, 0)

    queue = []
    spans = ((0, 2), (2, 2), (4, 2), (6, 1), (7, 1))
    second_spans = ((0, 4), (4, 2), (6, 2))
    final_spans = (((0, 4), (0,), (0, 1)), ((4, 2), (1,), (2,)), ((6, 2), (2,), (3, 4)))

    def whole(span):
        return (*span, 0, rows)

    def ready(i):
        for c in range(spans[i][0], sum(spans[i])):
            gathered(c)
        give(whole(spans[i]), i, 0, 0, i == 0)
        send(whole(spans[i]), i, 0, 3, i == 0, False)
        for unit in range(3):
            for c in range(spans[i][0], sum(spans[i])):
                queue.append((unit, i, whole((c, 1))))

    def issue(count):
        for _ in range(count):
            if queue:
                unit, i, part = queue.pop(0)
                y_copy(0, unit, i, part).start()

    def join_second(i):
        give_second(second_spans[i], i, 0, 2 * n_out, i == 0)

    def join_final(i):
        span, p_stages, y_stages = final_spans[i]

        def arrived(which):
            if i == 0:
                wait_in(ring + which, wide)
            for stage in p_stages:
                p_copy(0, which, stage, second_spans[stage]).wait_recv()
            for stage in y_stages:
                y_copy(0, which, stage, whole(spans[stage])).wait_recv()

        final_qkv(span, ring, (r.jq_gain, r.jk_gain), arrived)

    each(last, steps)
    ready(0)
    steps(last, lambda k: issue(1 if k else 0))
    load_join_in(mate, 2 * n_out)
    load_join_in(col, ring)
    issue(1)
    norm_end(5)
    issue(1)
    ready(1)
    sums(7, 1)
    issue(2)
    norm_start(6)
    issue(2)
    relay(4)
    relay(5)
    norm_end(6)
    norm_start(7)
    issue(3)
    join_second(0)
    relay(6)
    issue(1)
    norm_end(7)
    issue(2)
    ready(2)
    issue(4)
    join_second(1)
    relay(7)
    ready(3)
    issue(len(queue))
    all_sent(r.z_send, r.z_sent.at[0])
    for which, buffer in enumerate((r.hid0, r.hid1)):
        all_sent(buffer.at[own_place], r.a_send.at[which])
        all_sent(buffer.at[own_place], r.b_send.at[which])
        all_sent(buffer.at[own_place], r.d_send.at[which])
    ready(4)
    issue(len(queue))
    join_second(2)
    join_final(0)
    join_final(1)
    join_final(2)

    def blend(c):
        for start in range(0, wide, HEAD_DIM):
            head = pl.ds(start, HEAD_DIM)
            q = r.qkv[0, c, :, :, head].reshape(rows * piece, HEAD_DIM)
            k, v = (
                r.qkv[which, :, :, :, head].reshape(chunks * rows * piece, HEAD_DIM)
                for which in (1, 2)
            )
            r.hid0[own_place, c, :, :, head] = soft_blend(q, k, v).reshape(rows, piece, HEAD_DIM)
        to_across(1, 0, c).start()
        to_mate(c).start()

    def hand_on(c):
        to_across(1, 0, c).wait_recv()
        forward(1, 0, c).start()

    def result_of(c):
        sums_end(c)
        r.result[c] = (accum[c, 0] + r.layer[c].astype(F32)).astype(BF16)

    blend(0)
    blend(1)
    for slot in join_out_slots:
        wait_out(slot, wide)

    def join_steps(c):
        def before(back, action):
            @pl.when(c >= back)
            def _():
                action(c - back)

        def add(place, start=False):
            add_tile((c, 1), hid_value(place, 0, (c, 1)), join_out_slots[place], start)

        add(own_place, True)
        to_mate(c).wait_recv()
        add(mate_place)

        @pl.when(c == 0)
        def _():
            hand_on(c)

        add(across_place)
        forward(1, 0, c).wait_recv()
        add(diag_place)
        sums(c, 0)

        @pl.when(c + 2 < chunks)
        def _():
            blend(c + 2)

        before(1, lambda b: sums(b, 1))

        @pl.when(c + 1 < chunks)
        def _():
            hand_on(c + 1)

        before(3, result_of)

    each(chunks, join_steps)
    sums(last, 1)
    result_of(last - 2)
    result_of(last - 1)
    result_of(last)

    all_sent(r.z_send, r.z_sent.at[0])
    all_sent(r.hid0.at[own_place], r.a_send.at[0])
    all_sent(r.hid0.at[own_place], r.b_send.at[0])
    all_sent(r.hid0.at[own_place], r.d_send.at[0])
    all_sent(f_send[0], r.ys.at[0])
    all_sent(p_send[0], r.ps.at[0])
    inner = (row > 0) & (row < rows - 1)

    @pl.when(inner)
    def _():
        all_sent(normed, r.g_send.at[2])

    @pl.when(jnp.logical_not(inner))
    def _():
        all_sent(normed.at[:, pl.ds(0, 2)], r.g_send.at[2])


AHEAD = 4
SUM_MOVES = (
    (((3, 1), (2, 1), (1, 1)), ((0, 0),), ((3, 3),), ((0, 2), (1, 2), (2, 2))),
    ((), ((3, 3), (2, 2)), ((0, 0), (1, 1)), ()),
)
CHUNKS = 8


def tile_of(depth, columns, cols):
    ups = 3
    tile = columns // cols // ups
    return ups, tile


def kernel_body(
    camera_tokens,
    norm_gain,
    query_weight,
    key_weight,
    value_weight,
    query_gain,
    key_gain,
    out_weight,
    up_weight,
    up_bias,
    down_weight,
    down_bias,
    join_gain,
    join_query,
    join_key,
    join_value,
    join_query_gain,
    join_key_gain,
    join_out,
):
    own_rows, depth = camera_tokens.shape
    rows, cols = lax.axis_size("rows"), lax.axis_size("cols")
    width = out_weight.shape[1]
    wide = query_weight.shape[1] // cols
    ups, tile = tile_of(depth, up_weight.shape[1], cols)
    chunks, piece = CHUNKS, own_rows // CHUNKS
    n_in, n_out = 3 + ups, 1 + ups
    slot_pieces = max(depth, width) // tile

    def blocked(weight):
        return weight.reshape(depth // tile, tile, weight.shape[1])

    any_spec, vmem_spec = pl.BlockSpec(memory_space=pl.ANY), pl.BlockSpec(memory_space=pltpu.VMEM)
    inputs = {
        "tokens": (camera_tokens.reshape(chunks, piece, depth), vmem_spec),
        "gain": (norm_gain, vmem_spec),
        "q_gain": (query_gain, vmem_spec),
        "k_gain": (key_gain, vmem_spec),
        "bias": (up_bias.reshape(cols * ups, 1, tile), vmem_spec),
        "down_bias": (down_bias, vmem_spec),
        "join_gain": (join_gain, vmem_spec),
        "jq_gain": (join_query_gain, vmem_spec),
        "jk_gain": (join_key_gain, vmem_spec),
        "wq": (blocked(query_weight), any_spec),
        "wk": (blocked(key_weight), any_spec),
        "wv": (blocked(value_weight), any_spec),
        "w_up": (blocked(up_weight), any_spec),
        "w_out": (out_weight, any_spec),
        "w_down": (down_weight, any_spec),
        "jq": (blocked(join_query), any_spec),
        "jk": (blocked(join_key), any_spec),
        "jv": (blocked(join_value), any_spec),
        "w_join": (join_out, any_spec),
    }
    dma, vmem = pltpu.SemaphoreType.DMA, pltpu.VMEM
    scratch = {
        "pool": vmem((3 * n_in * slot_pieces, tile, tile), BF16),
        "pool_sem": dma((3 * n_in,)),
        "normed": vmem((chunks, rows, piece, depth), BF16),
        "start": vmem((4, 16, HEAD_DIM), F32),
        "moments": vmem((4, chunks, piece, HEAD_DIM), F32),
        "m_send": dma((chunks // 2 + 1, 3)),
        "m_recv": dma((chunks // 2 + 1, 3)),
        "g_send": dma((3,)),
        "g_arrive": dma((chunks, rows)),
        "qkv": vmem((3, chunks, rows, piece, wide), BF16),
        "hid0": vmem((4, chunks, rows, piece, wide), BF16),
        "hid1": vmem((4, ups, chunks, rows, piece, tile), BF16),
        "accum": vmem((chunks, rows, piece, width), F32),
        "z_send": vmem((chunks, rows - 1, piece, width), BF16),
        "z_in": vmem((chunks, rows + 1, piece, width), BF16),
        "z_sent": dma((1,)),
        "z_arrive": dma((chunks, rows + 1)),
        "layer": vmem((chunks, piece, width), BF16),
        "a_recv": dma((n_out, chunks)),
        "b_recv": dma((n_out, 2)),
        "d_recv": dma((n_out, 2)),
        "ys": dma((2,)),
        "ps": dma((2,)),
    }
    for name in ("a_send", "b_send", "d_send"):
        scratch[name] = dma((2,))
    for group, (count, wid) in enumerate(((3, wide), (ups, tile))):
        for name in ("f_send", "f_recv", "y_recv", "p_send", "p_recv"):
            scratch[name + str(group)] = vmem((count, chunks, rows, piece, wid), BF16)
        scratch["fs" + str(group)] = dma((count,))
        for name in ("fr", "yr", "pr"):
            scratch[name + str(group)] = dma((count, 3 if group else 5))
    names = (*inputs, "result", *scratch)
    joined = pl.pallas_call(
        functools.partial(layer_kernel, names, float(depth * cols)),
        name="layer",
        out_shape=jax.ShapeDtypeStruct((chunks, piece, width), BF16),
        in_specs=[spec for _, spec in inputs.values()],
        out_specs=vmem_spec,
        scratch_shapes=list(scratch.values()),
        compiler_params=pltpu.CompilerParams(
            collective_id=0, has_side_effects=True, vmem_limit_bytes=VMEM_LIMIT
        ),
    )(*[value for value, _ in inputs.values()])
    return joined.reshape(own_rows, width)


def fits(mesh):
    cols, rows = mesh.shape["cols"], mesh.shape["rows"]
    return cols == 4 and rows == 4 and D % (rows * cols * HEAD_DIM) == 0


def body(*arrays):
    tokens, up_weight = arrays[0], arrays[8]
    own_rows, depth = tokens.shape
    ups, tile = tile_of(depth, up_weight.shape[1], lax.axis_size("cols"))
    wide = arrays[2].shape[1] // lax.axis_size("cols")
    good = (
        own_rows == 2 * TOK_CAM
        and own_rows == HEAD_DIM
        and tile * ups * lax.axis_size("cols") == up_weight.shape[1]
        and tile % HEAD_DIM == 0
        and depth % tile == 0
        and arrays[7].shape[1] == depth
        and wide <= tile
        and wide % HEAD_DIM == 0
    )
    return kernel_body(*arrays) if good else plain_body(*arrays)


def solution(mesh):
    in_specs = (
        P(("groups", "rows"), "cols"),
        P("cols"),
        P("cols", "rows"),
        P("cols", "rows"),
        P("cols", "rows"),
        P("rows"),
        P("rows"),
        P("rows", "cols"),
        P("cols", "rows"),
        P("rows"),
        P("rows", "cols"),
        P("cols"),
        P("cols"),
        P("cols", "rows"),
        P("cols", "rows"),
        P("cols", "rows"),
        P("rows"),
        P("rows"),
        P("rows", "cols"),
    )
    out_specs = P(("groups", "rows"), "cols")
    inner = body if fits(mesh) else plain_body
    return jax.shard_map(inner, mesh=mesh, in_specs=in_specs, out_specs=out_specs, check_vma=False)
```

```python
import functools
import math
import types

import jax
import jax.numpy as jnp
from jax import lax
from jax.experimental import pallas as pl
from jax.experimental.pallas import tpu as pltpu
from jax.sharding import PartitionSpec as P

HEAD_DIM = 128
TOK_CAM = 64
D = 6144


EPS = 1e-06


def partner_2(array, axis, bit):
    return lax.ppermute(array, axis, [(i, i ^ 1 << bit) for i in range(lax.axis_size(axis))])


def normalize(values, scales, moments):
    row_mean = moments[0] / D
    row_var = moments[1] / D - row_mean * row_mean
    return ((values - row_mean[:, None]) * lax.rsqrt(row_var[:, None] + EPS) * scales).astype(
        jnp.bfloat16
    )


def shard_moments(values):
    return lax.psum((jnp.sum(values, 1), jnp.sum(values * values, 1)), "cols")


def head_norm(values, scales):
    row_count = values.shape[0]
    grouped = values.reshape(row_count, -1, HEAD_DIM)
    row_mean = jnp.mean(grouped, -1, keepdims=True)
    row_var = jnp.mean(grouped * grouped, -1, keepdims=True) - row_mean * row_mean
    normed = (grouped - row_mean) * lax.rsqrt(row_var + EPS)
    return (normed.reshape(row_count, -1) * scales).astype(jnp.bfloat16)


def attend(queries, key_rows, val_rows):
    inv_root = 1.0 / math.sqrt(HEAD_DIM)
    scores = (
        jnp.einsum("bqhd,bkhd->bhqk", queries, key_rows, preferred_element_type=jnp.float32)
        * inv_root
    )
    row_max = jnp.max(scores, -1, keepdims=True)
    weights = jnp.exp(scores - row_max)
    row_sum = jnp.sum(weights, -1)
    blended = jnp.einsum(
        "bhqk,bkhd->bqhd",
        weights.astype(jnp.bfloat16),
        val_rows,
        preferred_element_type=jnp.float32,
    )
    return blended / jnp.transpose(row_sum, (0, 2, 1))[..., None]


def to_heads(matrix, blocks):
    return matrix.reshape(blocks, -1, matrix.shape[1] // HEAD_DIM, HEAD_DIM)


def camera_attention(queries, key_rows, val_rows):
    local_rows = queries.shape[0]
    if local_rows >= TOK_CAM:
        blocks = local_rows // TOK_CAM
        result = attend(
            to_heads(queries, blocks), to_heads(key_rows, blocks), to_heads(val_rows, blocks)
        )
    else:
        cam_span = TOK_CAM // local_rows
        position = lax.axis_index("cols")
        key_value = jnp.stack((key_rows, val_rows))
        for which_bit in range(cam_span.bit_length() - 1):
            partner = partner_2(key_value, "cols", which_bit)
            is_lower = position >> which_bit & 1 == 0
            key_value = jnp.where(
                is_lower,
                jnp.concatenate((key_value, partner), 1),
                jnp.concatenate((partner, key_value), 1),
            )
        result = attend(to_heads(queries, 1), to_heads(key_value[0], 1), to_heads(key_value[1], 1))
    return result.reshape(local_rows, -1).astype(jnp.bfloat16)


def plain_body(
    camera_tokens,
    norm_gain,
    query_weight,
    key_weight,
    value_weight,
    query_gain,
    key_gain,
    out_weight,
    up_weight,
    up_bias,
    down_weight,
    down_bias,
    join_gain,
    join_query,
    join_key,
    join_value,
    join_query_gain,
    join_key_gain,
    join_out,
):
    own_rows = camera_tokens.shape[0]
    all_rows = own_rows * lax.axis_size("rows")
    col_rows = all_rows // lax.axis_size("cols")
    attn_width = query_weight.shape[1]
    start_f32 = camera_tokens.astype(jnp.float32)
    normed_all = lax.all_gather(
        normalize(start_f32, norm_gain, shard_moments(start_f32)), "rows", axis=0, tiled=True
    )
    joint_weight = jnp.concatenate((query_weight, key_weight, value_weight, up_weight), 1)
    joint = lax.psum_scatter(
        jnp.dot(normed_all, joint_weight, preferred_element_type=jnp.float32),
        "cols",
        scatter_dimension=0,
        tiled=True,
    )
    up_sum = joint[:, 3 * attn_width :]
    hidden = jax.nn.gelu(up_sum + up_bias, approximate=False).astype(jnp.bfloat16)
    attended = camera_attention(
        head_norm(joint[:, :attn_width], query_gain),
        head_norm(joint[:, attn_width : 2 * attn_width], key_gain),
        joint[:, 2 * attn_width : 3 * attn_width].astype(jnp.bfloat16),
    )
    attn_all, hidden_all = (
        lax.all_gather(attended, "cols", axis=0, tiled=True),
        lax.all_gather(hidden, "cols", axis=0, tiled=True),
    )
    mixed = lax.psum_scatter(
        jnp.dot(attn_all, out_weight, preferred_element_type=jnp.float32)
        + jnp.dot(hidden_all, down_weight, preferred_element_type=jnp.float32),
        "rows",
        scatter_dimension=0,
        tiled=True,
    )
    layer_own = (start_f32 + mixed + down_bias).astype(jnp.bfloat16)
    layer_f32 = layer_own.astype(jnp.float32)
    join_in = lax.all_gather(
        normalize(layer_f32, join_gain, shard_moments(layer_f32)), "rows", axis=0, tiled=True
    )
    join_weight = jnp.concatenate((join_query, join_key, join_value), 1)
    join_joint = lax.psum_scatter(
        jnp.dot(join_in, join_weight, preferred_element_type=jnp.float32),
        "cols",
        scatter_dimension=0,
        tiled=True,
    )
    join_q = head_norm(join_joint[:, :attn_width], join_query_gain)
    join_k = head_norm(join_joint[:, attn_width : 2 * attn_width], join_key_gain)
    join_v = join_joint[:, 2 * attn_width :].astype(jnp.bfloat16)
    heads_here = attn_width // HEAD_DIM
    query_heads = join_q.reshape(col_rows, heads_here, HEAD_DIM)
    inv_root = 1.0 / math.sqrt(HEAD_DIM)
    run_max = jnp.full((heads_here, col_rows), -jnp.inf, jnp.float32)
    run_sum = jnp.zeros((heads_here, col_rows), jnp.float32)
    accum = jnp.zeros((col_rows, heads_here, HEAD_DIM), jnp.float32)
    key_part = lax.all_gather(join_k, "cols", axis=0, tiled=True)
    val_part = lax.all_gather(join_v, "cols", axis=0, tiled=True)
    row_count = key_part.shape[0]
    key_heads = key_part.reshape(row_count, heads_here, HEAD_DIM)
    val_heads = val_part.reshape(row_count, heads_here, HEAD_DIM)
    scores = (
        jnp.einsum("qhd,khd->hqk", query_heads, key_heads, preferred_element_type=jnp.float32)
        * inv_root
    )
    new_max = jnp.max(scores, -1)
    factor = jnp.exp(run_max - new_max)
    weights = jnp.exp(scores - new_max[..., None])
    run_sum = run_sum * factor + jnp.sum(weights, -1)
    accum = accum * jnp.transpose(factor)[..., None] + jnp.einsum(
        "hqk,khd->qhd", weights.astype(jnp.bfloat16), val_heads, preferred_element_type=jnp.float32
    )
    run_max, run_sum, accum = (new_max, run_sum, accum)
    joined_attn = (
        (accum / jnp.transpose(run_sum)[..., None])
        .reshape(col_rows, attn_width)
        .astype(jnp.bfloat16)
    )
    joined_all = lax.all_gather(joined_attn, "cols", axis=0, tiled=True)
    result = lax.psum_scatter(
        jnp.dot(joined_all, join_out, preferred_element_type=jnp.float32),
        "rows",
        scatter_dimension=0,
        tiled=True,
    )
    return (layer_own.astype(jnp.float32) + result).astype(jnp.bfloat16)


F32 = jnp.float32
BF16 = jnp.bfloat16
MESH = pl.DeviceIdType.MESH
VMEM_LIMIT = 66 * 1024 * 1024 - 3 * 1024 * 1024


def each(count, step):
    lax.fori_loop(0, count, lambda i, carry: (step(i), carry)[1], None)


def remote(src, dst, send, recv, device):
    return pltpu.make_async_remote_copy(
        src_ref=src,
        dst_ref=dst,
        send_sem=send,
        recv_sem=recv,
        device_id=device,
        device_id_type=MESH,
    )


def places():
    col = lax.axis_index("cols")
    core = lax.rem(col, 2)
    return col, col + 1 - 2 * core, lax.rem(col + 2, 4)


def greet(cols_away):
    col, row, row_count = lax.axis_index("cols"), lax.axis_index("rows"), lax.axis_size("rows")
    barrier = pltpu.get_barrier_semaphore()
    _, mate, across = places()
    others = {1: mate, 2: across}
    if cols_away == 3:
        others[3] = mate + across - col
    for other in others.values():
        pl.semaphore_signal(barrier, inc=1, device_id={"cols": other}, device_id_type=MESH)

    @pl.when(row > 0)
    def _():
        pl.semaphore_signal(barrier, inc=1, device_id={"rows": row - 1}, device_id_type=MESH)

    @pl.when(row < row_count - 1)
    def _():
        pl.semaphore_signal(barrier, inc=1, device_id={"rows": row + 1}, device_id_type=MESH)

    inner = (row > 0) & (row < row_count - 1)

    @pl.when(inner)
    def _():
        pl.semaphore_wait(barrier, len(others) + 2)

    @pl.when(jnp.logical_not(inner))
    def _():
        pl.semaphore_wait(barrier, len(others) + 1)


def norm_heads(values, scales):
    parts = []
    for start in range(0, values.shape[1], HEAD_DIM):
        part = values[:, start : start + HEAD_DIM]
        mean = jnp.mean(part, -1, keepdims=True)
        var = jnp.mean(part * part, -1, keepdims=True) - mean * mean
        parts.append((part - mean) * lax.rsqrt(var + EPS))
    return (jnp.concatenate(parts, 1) * scales).astype(BF16)


def soft_blend(query, keys, values):
    scores = lax.dot_general(
        query, keys, (((1,), (1,)), ((), ())), preferred_element_type=F32
    ) * (1.0 / math.sqrt(HEAD_DIM))
    weights = jnp.exp(scores - jnp.max(scores, -1, keepdims=True))
    total = jnp.sum(weights, -1, keepdims=True)
    blended = jnp.dot(weights.astype(BF16), values, preferred_element_type=F32)
    return (blended / total).astype(BF16)


def layer_kernel(names, width, *refs):
    r = types.SimpleNamespace(**dict(zip(names, refs)))
    normed, accum, pool, pool_sem = r.normed, r.accum, r.pool, r.pool_sem
    col, mate, across = places()
    diagonal = mate + across - col
    owners = (col, mate, across, diagonal)
    row, rows = lax.axis_index("rows"), lax.axis_size("rows")
    chunks, _, piece, depth = normed.shape
    half = chunks // 2
    ups = r.f_send1.shape[0]
    tile = pool.shape[1]
    wide = r.hid0.shape[-1]
    out_pieces = accum.shape[-1] // tile
    in_pieces = depth // tile
    slot_pieces = max(in_pieces, out_pieces)
    n_in, n_out = 3 + ups, 1 + ups
    last = chunks - 1
    ring = 2 * n_in
    mine = pl.ds(pl.multiple_of(col * wide, HEAD_DIM), wide)
    own_place, mate_place, across_place, diag_place = range(4)

    def load_in(source, slot, start, wid):
        first = slot * slot_pieces
        return pltpu.make_async_copy(
            source.at[:, :, pl.ds(pl.multiple_of(start, HEAD_DIM), wid)],
            pool.at[pl.ds(first, in_pieces), :, pl.ds(0, wid)],
            pool_sem.at[slot],
        )

    def load_out(source, slot, start, deep):
        for j in range(out_pieces):
            pltpu.make_async_copy(
                source.at[pl.ds(pl.multiple_of(start, HEAD_DIM), deep), pl.ds(j * tile, tile)],
                pool.at[slot * slot_pieces + j, pl.ds(0, deep)],
                pool_sem.at[slot],
            ).start()

    def load_camera_in(owner, slot):
        for which, source in enumerate((r.wq, r.wk, r.wv)):
            load_in(source, slot + which, owner * wide, wide).start()
        each(
            ups,
            lambda unit: load_in(
                r.w_up, slot + 3 + unit, owner * (ups * tile) + unit * tile, tile
            ).start(),
        )

    def load_join_in(owner, slot):
        for which, source in enumerate((r.jq, r.jk, r.jv)):
            load_in(source, slot + which, owner * wide, wide).start()

    def load_camera_out(owner, slot):
        load_out(r.w_out, slot, owner * wide, wide)
        each(ups, lambda unit: load_out(r.w_down, slot + 1 + unit, (owner * ups + unit) * tile, tile))

    def in_weight(slot, wid):
        return pool.at[pl.ds(slot * slot_pieces, in_pieces), :, pl.ds(0, wid)]

    def wait_in(slot, wid):
        part = in_weight(slot, wid)
        pltpu.make_async_copy(part, part, pool_sem.at[slot]).wait()

    def wait_out(slot, deep):
        part = pool.at[pl.ds(slot * slot_pieces, out_pieces), pl.ds(0, deep)]
        pltpu.make_async_copy(part, part, pool_sem.at[slot]).wait()

    def product(slot, left, wid):
        weight = in_weight(slot, wid)[...].reshape(depth, wid)
        return jnp.dot(left, weight, preferred_element_type=F32)

    def add_tile(span, value, slot, begin=False):
        start, count = span
        deep = value.shape[1]
        for j in range(out_pieces):
            part = jnp.dot(
                value, pool[slot * slot_pieces + j, pl.ds(0, deep)], preferred_element_type=F32
            ).reshape(count, rows, piece, tile)
            at = (pl.ds(start, count), slice(None), slice(None), slice(j * tile, (j + 1) * tile))
            if begin:
                accum[at] = part
            else:
                accum[at] += part

    def gather_copy(c, block, right):
        rel = lax.rem(block - row + rows, rows)
        away = lax.rem(rel + (rows - 1 if right else 1), rows)
        return remote(
            normed.at[c, rel],
            normed.at[c, away],
            r.g_send.at[int(right)],
            r.g_arrive.at[c, block],
            {"rows": row + 1 if right else row - 1},
        )

    def arrival(c, block):
        part = normed.at[c, lax.rem(block - row + rows, rows)]
        pltpu.make_async_copy(part, part, r.g_arrive.at[c, block]).wait()

    def pass_on(c, block, right):
        @pl.when((row < rows - 1) if right else (row > 0))
        def _():
            gather_copy(c, block, right).start()

    def spread(c):
        pass_on(c, row, True)
        pass_on(c, row, False)

    def take(c, away):
        @pl.when(row >= away)
        def _():
            arrival(c, row - away)
            pass_on(c, row - away, True)

        @pl.when(row + away < rows)
        def _():
            arrival(c, row + away)
            pass_on(c, row + away, False)

    def spread_done():
        for place in range(rows):

            @pl.when(row == place)
            def _():
                if place < rows - 1:
                    all_sent(normed.at[:, pl.ds(0, place + 1)], r.g_send.at[1])
                if place > 0:
                    all_sent(normed.at[:, pl.ds(0, rows - place)], r.g_send.at[0])

    f_send, f_recv, y_recv = (r.f_send0, r.f_send1), (r.f_recv0, r.f_recv1), (r.y_recv0, r.y_recv1)
    p_send, p_recv = (r.p_send0, r.p_send1), (r.p_recv0, r.p_recv1)
    first_sems = ((r.fs0, r.fr0, r.yr0), (r.fs1, r.fr1, r.yr1))
    second_recv = (r.pr0, r.pr1)
    counts, wides, offsets = (3, ups), (wide, tile), (0, 3)

    def left_of(region):
        c0, nc, r0, nr = region
        return normed[pl.ds(c0, nc), pl.ds(r0, nr)].reshape(nc * nr * piece, depth)

    def part_of(region):
        c0, nc, r0, nr = region
        return pl.ds(c0, nc), pl.ds(r0, nr)

    def shaped(value, region):
        return value.reshape(region[1], region[3], piece, value.shape[-1])

    def f_copy(group, unit, stage, region):
        at = (unit, *part_of(region))
        fs, fr, _ = first_sems[group]
        return remote(
            f_send[group].at[at], f_recv[group].at[at], fs.at[unit], fr.at[unit, stage], {"cols": mate}
        )

    def y_copy(group, unit, stage, region):
        at = (unit, *part_of(region))
        yr = first_sems[group][2]
        return remote(
            f_send[group].at[at],
            y_recv[group].at[at],
            r.ys.at[group],
            yr.at[unit, stage],
            {"cols": across},
        )

    def p_copy(group, unit, stage, span):
        at = (unit, pl.ds(*span))
        return remote(
            p_send[group].at[at],
            p_recv[group].at[at],
            r.ps.at[group],
            second_recv[group].at[unit, stage],
            {"cols": mate},
        )

    def all_sent(source, sem):
        pltpu.make_async_copy(source, source, sem).wait()

    def give(region, stage, group, base, fresh):
        wid = wides[group]

        def step(unit):
            slot = base + offsets[group] + unit
            if fresh:
                wait_in(slot, wid)
            value = product(slot, left_of(region), wid).astype(BF16)
            f_send[group][(unit, *part_of(region))] = shaped(value, region)
            f_copy(group, unit, stage, region).start()

        each(counts[group], step)

    def send(region, stage, group, base, fresh, start=True):
        wid = wides[group]

        def step(unit):
            slot = base + offsets[group] + unit
            if fresh:
                wait_in(slot, wid)
            value = shaped(product(slot, left_of(region), wid), region)
            at = (unit, *part_of(region))
            f_copy(group, unit, stage, region).wait()
            f_send[group][at] = (value + f_recv[group][at].astype(F32)).astype(BF16)
            if start:
                y_copy(group, unit, stage, region).start()

        each(counts[group], step)

    def give_second(span, stage, group, base, fresh):
        wid = wides[group]
        region = (*span, 0, rows)

        def step(unit):
            slot = base + offsets[group] + unit
            if fresh:
                wait_in(slot, wid)
            value = product(slot, left_of(region), wid).astype(BF16)
            p_send[group][unit, pl.ds(*span)] = shaped(value, region)
            p_copy(group, unit, stage, span).start()

        each(counts[group], step)

    def final(group, unit, span, slot):
        region = (*span, 0, rows)
        wid = wides[group]
        part = pl.ds(*span)
        value = product(slot, left_of(region), wid)
        height = value.shape[0]
        got = p_recv[group][unit, part].astype(F32) + y_recv[group][unit, part].astype(F32)
        return value + got.reshape(height, wid)

    def final_qkv(span, base, gains, wait):
        region = (*span, 0, rows)
        for which in range(3):
            wait(which)
            value = final(0, which, span, base + which)
            if which < 2:
                value = norm_heads(value, gains[which][mine].reshape(1, -1))
            else:
                value = value.astype(BF16)
            r.qkv[which, pl.ds(*span)] = shaped(value, region)

    def hid(place, k, span):
        if isinstance(k, int) and k == 0:
            return r.hid0.at[place, pl.ds(*span)]
        return r.hid1.at[place, k - 1, pl.ds(*span)]

    def hid_value(place, k, span):
        part = hid(place, k, span)
        return part[...].reshape(span[1] * rows * piece, part.shape[-1])

    def of(sems, phase, k, c):
        wrap = sems.shape[1]
        if phase:
            return sems.at[c // wrap, c % wrap]
        return sems.at[k, c % wrap]

    def kind(k):
        return 0 if isinstance(k, int) and k == 0 else 1

    def to_across(phase, k, c):
        return remote(
            hid(own_place, k, (c, 1)),
            hid(across_place, k, (c, 1)),
            r.a_send.at[kind(k)],
            of(r.a_recv, phase, k, c),
            {"cols": across},
        )

    def half_to_mate(k, h):
        span = (h * half, half)
        return remote(
            hid(own_place, k, span),
            hid(mate_place, k, span),
            r.b_send.at[kind(k)],
            r.b_recv.at[k, h],
            {"cols": mate},
        )

    def to_mate(c):
        return remote(
            hid(own_place, 0, (c, 1)),
            hid(mate_place, 0, (c, 1)),
            r.b_send.at[0],
            of(r.b_recv, 1, 0, c),
            {"cols": mate},
        )

    def forward(phase, k, c):
        return remote(
            hid(across_place, k, (c, 1)),
            hid(diag_place, k, (c, 1)),
            r.d_send.at[kind(k)],
            of(r.d_recv, phase, k, c),
            {"cols": mate},
        )

    def z_wait(c, place):
        part = r.z_in.at[c, place]
        pltpu.make_async_copy(part, part, r.z_arrive.at[c, place]).wait()

    def sums(c, step):
        for place, moves in enumerate(SUM_MOVES[step]):

            @pl.when(row == place)
            def _():
                for block, there in moves:
                    rel = (block - place) % rows
                    value = accum[c, rel]
                    if step > 0:
                        z_wait(c, rel)
                        value += r.z_in[c, rel].astype(F32)
                    r.z_send[c, rel - 1] = value.astype(BF16)
                    slot = (block - there) % rows
                    if step == 0 and slot == 0:
                        slot = rows
                    remote(
                        r.z_send.at[c, rel - 1],
                        r.z_in.at[c, slot],
                        r.z_sent.at[0],
                        r.z_arrive.at[c, slot],
                        {"rows": there},
                    ).start()

    def sums_end(c):
        z_wait(c, rows)
        z_wait(c, 0)
        accum[c, 0] += r.z_in[c, rows].astype(F32) + r.z_in[c, 0].astype(F32)

    others = (mate, across, diagonal)

    def pairs(flat):
        lane = lax.broadcasted_iota(jnp.int32, (flat.shape[0], HEAD_DIM), 1)
        return jnp.where(
            lane < HEAD_DIM // 2,
            jnp.sum(flat, 1, keepdims=True),
            jnp.sum(flat * flat, 1, keepdims=True),
        )

    def normal(values, mean, square, gain):
        var = square / width - mean * mean
        return ((values - mean) * lax.rsqrt(var + EPS) * gain[...].reshape(1, -1)).astype(BF16)

    def swap(c, slot):
        i = c % half
        return remote(
            r.moments.at[3, c],
            r.moments.at[slot, c],
            r.m_send.at[i, slot],
            r.m_recv.at[i, slot],
            {"cols": others[slot]},
        )

    def norm_start(c):
        sums_end(c)
        total = accum[c, 0] + r.tokens[c].astype(F32) + r.down_bias[...].reshape(1, -1)
        layer = total.astype(BF16)
        r.layer[c] = layer
        r.moments[3, c] = pairs(layer.astype(F32))
        for slot in range(3):
            swap(c, slot).start()

    def norm_end(c):
        for slot in range(3):
            swap(c, slot).wait()
        m = r.moments
        total = (m[3, c] + m[0, c]) + (m[1, c] + m[2, c])
        at = HEAD_DIM // 2
        normed[c, 0] = normal(
            r.layer[c].astype(F32), total[:, :1] / width, total[:, at : at + 1], r.join_gain
        )
        for place in range(rows):

            @pl.when(row == place)
            def _():
                for there in range(rows):
                    if abs(there - place) == 1 or (abs(there - place) == 2 and place in (0, rows - 1)):
                        cast(c, place, there, place)

    def cast(c, place, there, block):
        rel, away = (block - place) % rows, (block - there) % rows
        remote(
            normed.at[c, rel],
            normed.at[c, away],
            r.g_send.at[2],
            r.g_arrive.at[c, away],
            {"rows": there},
        ).start()

    def landed(c, rel):
        part = normed.at[c, rel]
        pltpu.make_async_copy(part, part, r.g_arrive.at[c, rel]).wait()

    def relay(c):
        for place, there, blocks in ((1, 0, (2, 3)), (2, 3, (1, 0))):

            @pl.when(row == place)
            def _():
                for block in blocks:
                    landed(c, (block - place) % rows)
                    cast(c, place, there, block)

    def gathered(c):
        for place in range(rows):

            @pl.when(row == place)
            def _():
                for block in (((1, 2, 3), (0,), (3,), (2, 1, 0))[place]):
                    landed(c, (block - place) % rows)

    load_camera_in(diagonal, 0)
    load_camera_in(across, n_in)
    load_camera_in(mate, ring)
    own = r.tokens[...].reshape(chunks * piece, depth).astype(F32)
    few = r.start.shape[1]
    begin = HEAD_DIM // 2 - few // 2
    r.start[3] = jnp.transpose(pairs(own))[begin : begin + few]
    greet(3)
    swaps = [
        remote(
            r.start.at[3],
            r.start.at[slot],
            r.m_send.at[half, slot],
            r.m_recv.at[half, slot],
            {"cols": others[slot]},
        )
        for slot in range(3)
    ]
    for move in swaps:
        move.start()
    for move in swaps:
        move.wait()
    total = (r.start[3] + r.start[0]) + (r.start[1] + r.start[2])
    total = jnp.transpose(jnp.concatenate([total] * (HEAD_DIM // few), 0))
    normed[:, 0] = normal(
        own, total[:, :1] / width, total[:, few // 2 : few // 2 + 1], r.gain
    ).reshape(chunks, piece, depth)
    first_half, second_half = (0, half), (half, half)
    each(half, spread)
    region = (0, chunks, 0, 1)
    rest = [(h * half, half, 1, rows - 1) for h in range(2)]

    def takes(h, away):
        each(half, lambda i: take(h * half + i, away))

    for group in range(2):
        give(region, 0, group, 0, True)
        send(region, 0, group, n_in, True)
    takes(0, 1)
    takes(0, 2)
    each(half, lambda i: spread(half + i))
    takes(0, 3)
    for group in range(2):
        give(rest[0], 1, group, 0, False)
        send(rest[0], 1, group, n_in, False)
        if group == 0:
            takes(1, 1)
    takes(1, 2)
    for group in range(2):
        give_second(first_half, 0, group, ring, True)
    takes(1, 3)
    for group in range(2):
        give(rest[1], 2, group, 0, False)
        send(rest[1], 2, group, n_in, False)
    load_camera_out(col, 0)
    load_camera_out(mate, n_out)
    load_camera_out(across, 2 * n_out)
    for group in range(2):
        give_second(second_half, 1, group, ring, False)
    load_camera_in(col, ring)
    spread_done()

    def finals(h):
        span = (h * half, half)

        def arrived(group, unit):
            @pl.when(h == 0)
            def _():
                wait_in(ring + offsets[group] + unit, wides[group])
                y_copy(group, unit, 0, region).wait_recv()

            p_copy(group, unit, h, span).wait_recv()
            y_copy(group, unit, 1 + h, (*span[:1], half, 1, rows - 1)).wait_recv()

        final_qkv(span, ring, (r.q_gain, r.k_gain), lambda which: arrived(0, which))

        def camera(rel):
            for start in range(0, wide, HEAD_DIM):
                head = pl.ds(start, HEAD_DIM)
                q, k, v = (
                    r.qkv[which, pl.ds(*span), rel, :, head].reshape(half * piece, HEAD_DIM)
                    for which in range(3)
                )
                r.hid0[own_place, pl.ds(*span), rel, :, head] = soft_blend(q, k, v).reshape(
                    half, piece, HEAD_DIM
                )

        each(rows, camera)
        half_to_mate(0, h).start()

        def activate(unit):
            arrived(1, unit)
            raw = final(1, unit, span, ring + 3 + unit) + r.bias[col * ups + unit]
            value = (raw * (1.0 + lax.erf(raw * math.sqrt(0.5))) * 0.5).astype(BF16)
            r.hid1[own_place, unit, pl.ds(*span)] = shaped(value, (*span, 0, rows))
            half_to_mate(unit + 1, h).start()

        each(ups, activate)

        @pl.when(h == 0)
        def _():
            def ship(c):
                to_across(0, 0, c).start()
                each(ups, lambda unit: to_across(0, unit + 1, c).start())

            each(half, ship)

        def fresh_out(slot, deep):
            @pl.when(h == 0)
            def _():
                wait_out(slot, deep)

        def near_up(place):
            def one(unit):
                slot = place * n_out + 1 + unit
                fresh_out(slot, tile)
                if place == mate_place:
                    half_to_mate(unit + 1, h).wait_recv()
                add_tile(span, hid_value(place, unit + 1, span), slot)

            return one

        fresh_out(0, wide)
        add_tile(span, hid_value(own_place, 0, span), 0, True)
        each(ups, near_up(own_place))
        fresh_out(n_out, wide)
        half_to_mate(0, h).wait_recv()
        add_tile(span, hid_value(mate_place, 0, span), n_out)
        each(ups, near_up(mate_place))

    each(2, finals)
    load_camera_out(diagonal, ring)
    load_join_in(diagonal, 0)
    load_join_in(across, 3)
    join_out_slots = (2 * n_out - 2, 2 * n_out - 1, ring + n_out, ring + n_out + 1)
    for place in range(4):
        load_out(r.w_join, join_out_slots[place], owners[place] * wide, wide)
    for group in range(2):
        all_sent(f_send[group], r.ys.at[group])
        all_sent(p_send[group], r.ps.at[group])

    def far(c, k):
        ahead = k + AHEAD
        later = c + ahead // n_out

        @pl.when((later >= half) & (later < chunks))
        def _():
            to_across(0, ahead % n_out, later).start()

        to_across(0, k, c).wait_recv()
        forward(0, k, c).start()

        @pl.when(c == 0)
        def _():
            wait_out(2 * n_out + k, wide if k == 0 else tile)

        add_tile((c, 1), hid_value(across_place, k, (c, 1)), 2 * n_out + k)

    def farther(c, k):
        @pl.when(c == 0)
        def _():
            wait_out(ring + k, wide if k == 0 else tile)

        forward(0, k, c).wait_recv()
        add_tile((c, 1), hid_value(diag_place, k, (c, 1)), ring + k)

    def steps(c, pause=lambda k: None):
        def before(back, action):
            if isinstance(c, int):
                action(c - back)
                return

            @pl.when(c >= back)
            def _():
                action(c - back)

        for k in range(n_out):
            far(c, k)
            if k > 0:
                farther(c, k - 1)
            if k == 1:
                before(2, norm_start)
            if k == 1:
                before(3, norm_end)
            if k == 1:
                before(4, relay)
            if k == 2:
                before(1, lambda b: sums(b, 1))
            pause(k)
        farther(c, n_out - 1)
        sums(c, 0)

    queue = []
    spans = ((0, 2), (2, 2), (4, 2), (6, 1), (7, 1))
    second_spans = ((0, 4), (4, 2), (6, 2))
    final_spans = (((0, 4), (0,), (0, 1)), ((4, 2), (1,), (2,)), ((6, 2), (2,), (3, 4)))

    def whole(span):
        return (*span, 0, rows)

    def ready(i):
        for c in range(spans[i][0], sum(spans[i])):
            gathered(c)
        give(whole(spans[i]), i, 0, 0, i == 0)
        send(whole(spans[i]), i, 0, 3, i == 0, False)
        for unit in range(3):
            for c in range(spans[i][0], sum(spans[i])):
                queue.append((unit, i, whole((c, 1))))

    def issue(count):
        for _ in range(count):
            if queue:
                unit, i, part = queue.pop(0)
                y_copy(0, unit, i, part).start()

    def join_second(i):
        give_second(second_spans[i], i, 0, 2 * n_out, i == 0)

    def join_final(i):
        span, p_stages, y_stages = final_spans[i]

        def arrived(which):
            if i == 0:
                wait_in(ring + which, wide)
            for stage in p_stages:
                p_copy(0, which, stage, second_spans[stage]).wait_recv()
            for stage in y_stages:
                y_copy(0, which, stage, whole(spans[stage])).wait_recv()

        final_qkv(span, ring, (r.jq_gain, r.jk_gain), arrived)

    each(last, steps)
    ready(0)
    steps(last, lambda k: issue(1 if k else 0))
    load_join_in(mate, 2 * n_out)
    load_join_in(col, ring)
    issue(1)
    norm_end(5)
    sums(7, 1)
    norm_start(6)
    issue(2)
    relay(4)
    ready(1)
    relay(5)
    norm_end(6)
    norm_start(7)
    issue(3)
    join_second(0)
    relay(6)
    issue(1)
    norm_end(7)
    issue(2)
    ready(2)
    issue(4)
    join_second(1)
    relay(7)
    ready(3)
    issue(len(queue))
    all_sent(r.z_send, r.z_sent.at[0])
    for which, buffer in enumerate((r.hid0, r.hid1)):
        all_sent(buffer.at[own_place], r.a_send.at[which])
        all_sent(buffer.at[own_place], r.b_send.at[which])
        all_sent(buffer.at[own_place], r.d_send.at[which])
    ready(4)
    issue(len(queue))
    join_second(2)
    join_final(0)
    join_final(1)
    join_final(2)

    def blend(c):
        for start in range(0, wide, HEAD_DIM):
            head = pl.ds(start, HEAD_DIM)
            q = r.qkv[0, c, :, :, head].reshape(rows * piece, HEAD_DIM)
            k, v = (
                r.qkv[which, :, :, :, head].reshape(chunks * rows * piece, HEAD_DIM)
                for which in (1, 2)
            )
            r.hid0[own_place, c, :, :, head] = soft_blend(q, k, v).reshape(rows, piece, HEAD_DIM)
        to_across(1, 0, c).start()
        to_mate(c).start()

    def hand_on(c):
        to_across(1, 0, c).wait_recv()
        forward(1, 0, c).start()

    def result_of(c):
        sums_end(c)
        r.result[c] = (accum[c, 0] + r.layer[c].astype(F32)).astype(BF16)

    blend(0)
    blend(1)
    for slot in join_out_slots:
        wait_out(slot, wide)

    def join_steps(c):
        def before(back, action):
            @pl.when(c >= back)
            def _():
                action(c - back)

        def add(place, start=False):
            add_tile((c, 1), hid_value(place, 0, (c, 1)), join_out_slots[place], start)

        add(own_place, True)
        to_mate(c).wait_recv()
        add(mate_place)

        @pl.when(c == 0)
        def _():
            hand_on(c)

        add(across_place)
        forward(1, 0, c).wait_recv()
        add(diag_place)
        sums(c, 0)

        @pl.when(c + 2 < chunks)
        def _():
            blend(c + 2)

        before(1, lambda b: sums(b, 1))

        @pl.when(c + 1 < chunks)
        def _():
            hand_on(c + 1)

        before(3, result_of)

    each(chunks, join_steps)
    sums(last, 1)
    result_of(last - 2)
    result_of(last - 1)
    result_of(last)

    all_sent(r.z_send, r.z_sent.at[0])
    all_sent(r.hid0.at[own_place], r.a_send.at[0])
    all_sent(r.hid0.at[own_place], r.b_send.at[0])
    all_sent(r.hid0.at[own_place], r.d_send.at[0])
    all_sent(f_send[0], r.ys.at[0])
    all_sent(p_send[0], r.ps.at[0])
    inner = (row > 0) & (row < rows - 1)

    @pl.when(inner)
    def _():
        all_sent(normed, r.g_send.at[2])

    @pl.when(jnp.logical_not(inner))
    def _():
        all_sent(normed.at[:, pl.ds(0, 2)], r.g_send.at[2])


AHEAD = 4
SUM_MOVES = (
    (((3, 1), (2, 1), (1, 1)), ((0, 0),), ((3, 3),), ((0, 2), (1, 2), (2, 2))),
    ((), ((3, 3), (2, 2)), ((0, 0), (1, 1)), ()),
)
CHUNKS = 8


def tile_of(depth, columns, cols):
    ups = 3
    tile = columns // cols // ups
    return ups, tile


def kernel_body(
    camera_tokens,
    norm_gain,
    query_weight,
    key_weight,
    value_weight,
    query_gain,
    key_gain,
    out_weight,
    up_weight,
    up_bias,
    down_weight,
    down_bias,
    join_gain,
    join_query,
    join_key,
    join_value,
    join_query_gain,
    join_key_gain,
    join_out,
):
    own_rows, depth = camera_tokens.shape
    rows, cols = lax.axis_size("rows"), lax.axis_size("cols")
    width = out_weight.shape[1]
    wide = query_weight.shape[1] // cols
    ups, tile = tile_of(depth, up_weight.shape[1], cols)
    chunks, piece = CHUNKS, own_rows // CHUNKS
    n_in, n_out = 3 + ups, 1 + ups
    slot_pieces = max(depth, width) // tile

    def blocked(weight):
        return weight.reshape(depth // tile, tile, weight.shape[1])

    any_spec, vmem_spec = pl.BlockSpec(memory_space=pl.ANY), pl.BlockSpec(memory_space=pltpu.VMEM)
    inputs = {
        "tokens": (camera_tokens.reshape(chunks, piece, depth), vmem_spec),
        "gain": (norm_gain, vmem_spec),
        "q_gain": (query_gain, vmem_spec),
        "k_gain": (key_gain, vmem_spec),
        "bias": (up_bias.reshape(cols * ups, 1, tile), vmem_spec),
        "down_bias": (down_bias, vmem_spec),
        "join_gain": (join_gain, vmem_spec),
        "jq_gain": (join_query_gain, vmem_spec),
        "jk_gain": (join_key_gain, vmem_spec),
        "wq": (blocked(query_weight), any_spec),
        "wk": (blocked(key_weight), any_spec),
        "wv": (blocked(value_weight), any_spec),
        "w_up": (blocked(up_weight), any_spec),
        "w_out": (out_weight, any_spec),
        "w_down": (down_weight, any_spec),
        "jq": (blocked(join_query), any_spec),
        "jk": (blocked(join_key), any_spec),
        "jv": (blocked(join_value), any_spec),
        "w_join": (join_out, any_spec),
    }
    dma, vmem = pltpu.SemaphoreType.DMA, pltpu.VMEM
    scratch = {
        "pool": vmem((3 * n_in * slot_pieces, tile, tile), BF16),
        "pool_sem": dma((3 * n_in,)),
        "normed": vmem((chunks, rows, piece, depth), BF16),
        "start": vmem((4, 16, HEAD_DIM), F32),
        "moments": vmem((4, chunks, piece, HEAD_DIM), F32),
        "m_send": dma((chunks // 2 + 1, 3)),
        "m_recv": dma((chunks // 2 + 1, 3)),
        "g_send": dma((3,)),
        "g_arrive": dma((chunks, rows)),
        "qkv": vmem((3, chunks, rows, piece, wide), BF16),
        "hid0": vmem((4, chunks, rows, piece, wide), BF16),
        "hid1": vmem((4, ups, chunks, rows, piece, tile), BF16),
        "accum": vmem((chunks, rows, piece, width), F32),
        "z_send": vmem((chunks, rows - 1, piece, width), BF16),
        "z_in": vmem((chunks, rows + 1, piece, width), BF16),
        "z_sent": dma((1,)),
        "z_arrive": dma((chunks, rows + 1)),
        "layer": vmem((chunks, piece, width), BF16),
        "a_recv": dma((n_out, chunks)),
        "b_recv": dma((n_out, 2)),
        "d_recv": dma((n_out, 2)),
        "ys": dma((2,)),
        "ps": dma((2,)),
    }
    for name in ("a_send", "b_send", "d_send"):
        scratch[name] = dma((2,))
    for group, (count, wid) in enumerate(((3, wide), (ups, tile))):
        for name in ("f_send", "f_recv", "y_recv", "p_send", "p_recv"):
            scratch[name + str(group)] = vmem((count, chunks, rows, piece, wid), BF16)
        scratch["fs" + str(group)] = dma((count,))
        for name in ("fr", "yr", "pr"):
            scratch[name + str(group)] = dma((count, 3 if group else 5))
    names = (*inputs, "result", *scratch)
    joined = pl.pallas_call(
        functools.partial(layer_kernel, names, float(depth * cols)),
        name="layer",
        out_shape=jax.ShapeDtypeStruct((chunks, piece, width), BF16),
        in_specs=[spec for _, spec in inputs.values()],
        out_specs=vmem_spec,
        scratch_shapes=list(scratch.values()),
        compiler_params=pltpu.CompilerParams(
            collective_id=0, has_side_effects=True, vmem_limit_bytes=VMEM_LIMIT
        ),
    )(*[value for value, _ in inputs.values()])
    return joined.reshape(own_rows, width)


def fits(mesh):
    cols, rows = mesh.shape["cols"], mesh.shape["rows"]
    return cols == 4 and rows == 4 and D % (rows * cols * HEAD_DIM) == 0


def body(*arrays):
    tokens, up_weight = arrays[0], arrays[8]
    own_rows, depth = tokens.shape
    ups, tile = tile_of(depth, up_weight.shape[1], lax.axis_size("cols"))
    wide = arrays[2].shape[1] // lax.axis_size("cols")
    good = (
        own_rows == 2 * TOK_CAM
        and own_rows == HEAD_DIM
        and tile * ups * lax.axis_size("cols") == up_weight.shape[1]
        and tile % HEAD_DIM == 0
        and depth % tile == 0
        and arrays[7].shape[1] == depth
        and wide <= tile
        and wide % HEAD_DIM == 0
    )
    return kernel_body(*arrays) if good else plain_body(*arrays)


def solution(mesh):
    in_specs = (
        P(("groups", "rows"), "cols"),
        P("cols"),
        P("cols", "rows"),
        P("cols", "rows"),
        P("cols", "rows"),
        P("rows"),
        P("rows"),
        P("rows", "cols"),
        P("cols", "rows"),
        P("rows"),
        P("rows", "cols"),
        P("cols"),
        P("cols"),
        P("cols", "rows"),
        P("cols", "rows"),
        P("cols", "rows"),
        P("rows"),
        P("rows"),
        P("rows", "cols"),
    )
    out_specs = P(("groups", "rows"), "cols")
    inner = body if fits(mesh) else plain_body
    return jax.shard_map(inner, mesh=mesh, in_specs=in_specs, out_specs=out_specs, check_vma=False)
```
